256 devices in a mesh: gx: 8 (over x, core), gy: 8 (over z), gz: 4 (over y).
Axes of the slice: x: 4, y: 4, z: 8, core: 2. Of those that a mesh axis runs over, the one named last changes fastest.
Arguments:
- fields: float32 [1, 256, 256, 512], P(None, 'gx', 'gy', 'gz'), may hold values from -13 to 13
- exponents: int32 [5], replicated, may hold values from -5 to -1
Outputs:
- coefficients: float32 [1, 256, 256, 512], P(None, 'gx', 'gy', 'gz')
- statistics: float32 [2, 1, 5], replicated
The draws below stay inside these ranges and needn't reach their ends.
All inputs are finite; a program needn't handle non-finite values.
Results may differ from the reference program's by a relative error of at most 0.0003.
Values sent between devices are 32-bit elements; how exact they have to be, the bound alone decides.
No kernel may reach another device: no remote copies, remote signals or barrier semaphores. Data moves between devices by JAX's collectives and lax.ppermute only.
A program may use at most 64 MiB of HBM per device.

```python
import jax
import jax.numpy as jnp
from jax import lax

FIELDS = 1
FINE = 3
COARSE = 2
LEVELS = 5
NX = 256
NY = 256
NZ = 512


def coarse_rough(key):
    block = 2 ** FINE
    values = jax.random.uniform(jax.random.fold_in(key, 23), (FIELDS, NX // block, NY // block, NZ // block), jnp.float32, -3.0, 3.0)
    values = jnp.repeat(values, block, axis=1)
    values = jnp.repeat(values, block, axis=2)
    return jnp.repeat(values, block, axis=3)


def draw_fields(key, part):
    shape = (FIELDS, NX, NY, NZ)
    coord_x = jnp.arange(NX, dtype=jnp.float32)[None, :, None, None] / NX
    coord_y = jnp.arange(NY, dtype=jnp.float32)[None, None, :, None] / NY
    coord_z = jnp.arange(NZ, dtype=jnp.float32)[None, None, None, :] / NZ
    rising = 0.5 + 1.5 * (coord_x + coord_y + coord_z) / 3.0
    rough = coarse_rough(key)
    noise = jax.random.truncated_normal(jax.random.fold_in(key, 7), -5.0, 5.0, shape, jnp.float32)
    return (rising * noise + rough).astype(jnp.float32)


def touch_ends(array, key, smallest, largest):
    spot = [jax.random.randint(jax.random.fold_in(key, axis), (), 0, length) for axis, length in enumerate(array.shape)]
    widest = array.shape.index(max(array.shape))
    next_to = spot[:widest] + [(spot[widest] + 1) % array.shape[widest]] + spot[widest + 1:]
    return array.at[tuple(spot)].set(smallest).at[tuple(next_to)].set(largest)


def setup_inputs(seed: int = 0) -> dict:
    seeds = jax.random.split(jax.random.key(seed), 3)
    return {
        "fields": draw_fields(jax.random.fold_in(seeds[2], 71), 0),
        "exponents": touch_ends(jax.random.randint(seeds[1], (LEVELS,), -5, 0), jax.random.fold_in(seeds[1], 1), -5, -1).astype(jnp.int32),
    }


def split_pair(values, axis_dim):
    length = values.shape[axis_dim]
    even_part = lax.slice_in_dim(values, 0, length, 2, axis_dim)
    odd_part = lax.slice_in_dim(values, 1, length, 2, axis_dim)
    return even_part, odd_part


def lift_whole(values, axis_dim):
    even_part, odd_part = split_pair(values, axis_dim)
    detail = odd_part - 0.5 * (even_part + jnp.roll(even_part, -1, axis_dim))
    smooth = even_part + 0.25 * (jnp.roll(detail, 1, axis_dim) + detail)
    return jnp.stack((smooth, detail), axis_dim + 1).reshape(values.shape)


def detail_mask(shape):
    parity_flags = [(jnp.arange(shape[index_dim]) % 2) == 0 for index_dim in (1, 2, 3)]
    smooth_cells = parity_flags[0][:, None, None] & parity_flags[1][None, :, None] & parity_flags[2][None, None, :]
    return jnp.where(smooth_cells, 0.0, 1.0).astype(jnp.float32)[None]


def shrink(values, exponent):
    thresh = jnp.exp2(exponent.astype(jnp.float32))
    return jnp.sign(values) * jnp.maximum(jnp.abs(values) - thresh, 0.0)


def reference(fields, exponents):
    current = fields
    layers = []
    energies = []
    retained = []
    cell_total = NX * NY * NZ
    for layer_index in range(FINE + COARSE):
        for axis_dim in (1, 2, 3):
            current = lift_whole(current, axis_dim)
        masking = detail_mask(current.shape)
        shrunk = shrink(current, exponents[layer_index])
        level_count = 7.0 * cell_total / 8 ** (layer_index + 1)
        energies.append(jnp.sum(current * current * masking, axis=(1, 2, 3)) / level_count)
        retained.append(jnp.sum(jnp.abs(shrunk) * masking, axis=(1, 2, 3)) / level_count)
        layers.append(shrunk)
        current = current[:, ::2, ::2, ::2]
    result = current
    for shrunk in reversed(layers):
        result = shrunk.at[:, ::2, ::2, ::2].set(result)
    statistics = jnp.stack((jnp.stack(energies, 1), jnp.stack(retained, 1)))
    return result, statistics
```

```python
import functools

import jax
import jax.numpy as jnp
import numpy as np
from jax import lax
from jax.experimental import pallas as pl
from jax.experimental.pallas import tpu as pltpu
from jax.sharding import PartitionSpec as P

NEAR = 4
LEVELS = 5
LANES = 128
SIDE = 32
EXT = 2 * NEAR
PITCH = SIDE + EXT
F32 = jnp.float32


def cascade(cells, ahead, behind):
    details, firsts = [], []
    for level in range(NEAR):
        half = len(cells) // 2
        following = cells[2::2] + [ahead[level]]
        detail = [cells[2 * k + 1] - 0.5 * (cells[2 * k] + following[k]) for k in range(half)]
        details.append(detail[-1])
        firsts.append(cells[0])
        before = [behind[level]] + detail[:-1]
        cells = [cells[2 * k] + 0.25 * (before[k] + detail[k]) for k in range(half)]
    return details, firsts


def end_weights(length):
    none = [np.zeros(length)] * NEAR
    details, firsts = cascade(list(np.eye(length)), none, none)
    return np.stack(details + firsts)


def seam_weights():
    zero = [np.zeros(1)] * NEAR
    flat = [np.zeros(1)] * SIDE
    alpha = np.zeros((NEAR, NEAR))
    beta = np.zeros((NEAR, NEAR))
    for j in range(NEAR):
        unit = [np.ones(1) * (k == j) for k in range(NEAR)]
        alpha[:, j] = [d[0] for d in cascade(flat, unit, zero)[0]]
        beta[:, j] = [f[0] for f in cascade(flat, zero, unit)[1]]
    lasts, firsts = [], []
    for level in range(NEAR):
        first = np.eye(EXT)[NEAR + level]
        for j in range(level):
            first = first + beta[level, j] * lasts[j]
        firsts.append(first)
        last = np.eye(EXT)[level]
        for j in range(level + 1):
            last = last + alpha[level, j] * firsts[j]
        lasts.append(last)
    return np.stack(lasts), np.stack(firsts)


W = end_weights(SIDE)
WZ = end_weights(LANES)
LAST, FIRST = seam_weights()
GROUP = LANES // EXT


def constant_tables():
    tables = np.zeros((7, LANES, LANES), np.float32)
    left = np.zeros((EXT, EXT))
    right = np.zeros((EXT, EXT))
    left[:, :NEAR] = LAST.T
    right[:, NEAR:] = FIRST.T
    tables[0] = np.tile(WZ.T, (1, GROUP))
    tables[1] = np.kron(np.eye(GROUP), left)
    tables[2] = np.kron(np.eye(GROUP), right)
    for half in range(2):
        tables[3 + half, :, : EXT * EXT] = np.kron(W[:, half * GROUP : (half + 1) * GROUP].T, np.eye(EXT))
    tables[5, : EXT * EXT, : EXT * EXT] = np.kron(left, np.eye(EXT))
    tables[6, : EXT * EXT, : EXT * EXT] = np.kron(right, np.eye(EXT))
    return tables


def dot(a, b):
    return jnp.dot(a, b, precision=lax.Precision.HIGHEST, preferred_element_type=F32)


def lanes_of(rows):
    return lax.broadcasted_iota(jnp.int32, (rows, LANES), 1)


def rows_of(rows):
    return lax.broadcasted_iota(jnp.int32, (rows, LANES), 0)


def roll(v, shift):
    return pltpu.roll(v, shift % LANES, 1)


def weighted(rows, load):
    sums = [None] * EXT
    for i in range(SIDE):
        block = load(i)
        for g in range(EXT):
            if W[g, i] != 0.0:
                term = float(W[g, i]) * block
                sums[g] = term if sums[g] is None else sums[g] + term
    return sums


def mix(weights, blocks):
    total = None
    for w, block in zip(weights, blocks):
        if w != 0.0:
            term = float(w) * block
            total = term if total is None else total + term
    return total


def ends_kernel(f, table, pz, fx, fy):
    lane = lanes_of(SIDE)
    packed = [jnp.zeros((SIDE, LANES), F32)] * 2
    for x in range(SIDE):
        out = dot(f[pl.ds(x * SIDE, SIDE), :], table[...])
        packed[x // GROUP] = jnp.where(lane // EXT == x % GROUP, out, packed[x // GROUP])
    for half in range(2):
        pz[pl.ds(half * SIDE, SIDE), :] = packed[half]
    for c in range(SIDE // 8):
        for g, block in enumerate(weighted(8, lambda x: f[pl.ds(x * SIDE + 8 * c, 8), :])):
            fx[pl.ds(g * SIDE + 8 * c, 8), :] = block
    for c in range(SIDE // 8):
        for g, block in enumerate(weighted(8, lambda y: f[pl.ds(8 * c * SIDE + y, 8, stride=SIDE), :])):
            fy[pl.ds(g * SIDE + 8 * c, 8), :] = block


def depth_kernel(pz, before, after, fx, tables, ez, up, down):
    slot = lanes_of(SIDE) % EXT
    fxe = None
    for half in range(2):
        rows = pl.ds(half * SIDE, SIDE)
        own = pz[rows, :]
        full = dot(jnp.where(slot < NEAR, before[rows, :], own), tables[1]) + dot(
            jnp.where(slot < NEAR, own, after[rows, :]), tables[2]
        )
        ez[rows, :] = full
        part = dot(full, tables[3 + half])
        fxe = part if fxe is None else fxe + part
    for g in range(NEAR):
        up[pl.ds(g * SIDE, SIDE), :] = fx[pl.ds(g * SIDE, SIDE), :]
        down[pl.ds(g * SIDE, SIDE), :] = fx[pl.ds((NEAR + g) * SIDE, SIDE), :]
    up[pl.ds(NEAR * SIDE, SIDE), :] = fxe
    down[pl.ds(NEAR * SIDE, SIDE), :] = fxe


def width_kernel(up, down, before, after, fy, ez, wy, tables, xe, xee, yup, ydown):
    for c in range(SIDE // 8):
        rows = [pl.ds(g * SIDE + 8 * c, 8) for g in range(NEAR)]
        own_last = [up[r, :] for r in rows]
        own_first = [down[r, :] for r in rows]
        seam_before = [before[r, :] for r in rows] + own_first
        seam_after = own_last + [after[r, :] for r in rows]
        for level in range(NEAR):
            xe[pl.ds(level * SIDE + 8 * c, 8), :] = mix(LAST[level], seam_before)
            xe[pl.ds((NEAR + level) * SIDE + 8 * c, 8), :] = mix(FIRST[level], seam_after)
    slot = lanes_of(SIDE) // EXT
    rows = pl.ds(NEAR * SIDE, SIDE)
    own = up[rows, :]
    corner = dot(jnp.where(slot < NEAR, before[rows, :], own), tables[5]) + dot(
        jnp.where(slot < NEAR, own, after[rows, :]), tables[6]
    )
    xee[...] = corner
    sums = weighted(EXT, lambda y: xe[pl.ds(y, EXT, stride=SIDE), :])
    for g in range(EXT):
        target = yup if g < NEAR else ydown
        base = (g % NEAR) * PITCH
        target[pl.ds(base, SIDE), :] = fy[pl.ds(g * SIDE, SIDE), :]
        target[pl.ds(base + SIDE, EXT), :] = sums[g]
    for i, block in enumerate((ez[pl.ds(0, SIDE), :], ez[pl.ds(SIDE, SIDE), :], corner)):
        part = dot(wy[...], block)
        yup[pl.ds(NEAR * PITCH + i * EXT, EXT), :] = part
        ydown[pl.ds(NEAR * PITCH + i * EXT, EXT), :] = part


def lift_chunk(ref, at, level, masked):
    step = 1 << level
    pairs = SIDE // (2 * step)
    masked = masked and level > 0
    behind = ref[at(SIDE + level), :]
    even = ref[at(0), :]
    for k in range(pairs):
        odd = ref[at(step * (2 * k + 1)), :]
        ahead = ref[at(step * (2 * k + 2)), :] if k < pairs - 1 else ref[at(SIDE + NEAR + level), :]
        detail = odd - 0.5 * (even + ahead)
        smooth = even + 0.25 * (behind + detail)
        if masked:
            live = (lanes_of(odd.shape[0]) & (step - 1)) == 0
            detail, smooth = jnp.where(live, detail, odd), jnp.where(live, smooth, even)
        ref[at(step * (2 * k + 1)), :] = detail
        ref[at(2 * step * k), :] = smooth
        behind, even = detail, ahead


def chunks(level):
    step = 1 << level
    count = SIDE // step
    own = [(8 * step * c, min(8, count), step) for c in range(max(1, count // 8))]
    return own + ([(SIDE, EXT, 1)] if level < NEAR else [])


def levels_kernel(f, ez, xe, xee, yup, ydown, before, after, th, coef, send, v, q):
    for x in range(SIDE):
        v[pl.ds(x * PITCH, SIDE), :] = f[pl.ds(x * SIDE, SIDE), :]
    for g in range(EXT):
        v[pl.ds((SIDE + g) * PITCH, SIDE), :] = xe[pl.ds(g * SIDE, SIDE), :]
    for c in range(PITCH // 8):
        rows = [pl.ds(g * PITCH + 8 * c, 8) for g in range(NEAR)]
        seam_before = [before[r, :] for r in rows] + [ydown[r, :] for r in rows]
        seam_after = [yup[r, :] for r in rows] + [after[r, :] for r in rows]
        for level in range(NEAR):
            v[pl.ds(8 * c * PITCH + SIDE + level, 8, stride=PITCH), :] = mix(LAST[level], seam_before)
            v[pl.ds(8 * c * PITCH + SIDE + NEAR + level, 8, stride=PITCH), :] = mix(FIRST[level], seam_after)
    row8 = rows_of(EXT)
    for i in range(3):
        first = NEAR * PITCH + i * EXT
        own = [yup[pl.ds(first + j, 1), :] for j in range(EXT)]
        seam_before = [before[pl.ds(first + j, 1), :] for j in range(NEAR)] + own[NEAR:]
        seam_after = own[:NEAR] + [after[pl.ds(first + NEAR + j, 1), :] for j in range(NEAR)]
        extra = jnp.zeros((EXT, LANES), F32)
        for level in range(NEAR):
            extra = jnp.where(row8 == level, mix(LAST[level], seam_before), extra)
            extra = jnp.where(row8 == NEAR + level, mix(FIRST[level], seam_after), extra)
        block = ez[pl.ds(i * SIDE, SIDE), :] if i < 2 else xee[...]
        for j in range(GROUP if i < 2 else EXT):
            x = i * GROUP + j
            q[pl.ds(x * PITCH, SIDE), :] = roll(block, -EXT * j)
            q[pl.ds(x * PITCH + SIDE, EXT), :] = roll(extra, -EXT * j)

    for level in range(NEAR):
        step = 1 << level
        for ref in (v, q):
            for first, count, stride in chunks(level):
                lift_chunk(ref, lambda i: pl.ds(i * PITCH + first, count, stride=stride), level, ref is v)
            for first, count, stride in chunks(level):
                lift_chunk(ref, lambda i: pl.ds(first * PITCH + i, count, stride=stride * PITCH), level, ref is v)
        planes = list(range(0, SIDE, step)) + (list(range(SIDE, PITCH)) if level < NEAR - 1 else [])
        for x in planes:
            for first, count, stride in chunks(level):
                if first == SIDE and level == NEAR - 1:
                    continue
                at = pl.ds(x * PITCH + first, count, stride=stride)
                lane = lanes_of(count)
                cells, ends = v[at, :], q[at, :]
                ahead = jnp.where(lane == 0, roll(ends, -(NEAR + level)), cells)
                detail = cells - 0.5 * (roll(cells, step) + roll(ahead, -step))
                behind = jnp.where(lane == LANES - step, roll(ends, -step - level), detail)
                smooth = cells + 0.25 * (roll(behind, step) + roll(detail, -step))
                place = lane & (2 * step - 1)
                v[at, :] = jnp.where(place == 0, smooth, jnp.where(place == step, detail, cells))

    energy = [jnp.zeros((8, LANES), F32)] * NEAR
    kept = [jnp.zeros((8, LANES), F32)] * NEAR
    for c in range(SIDE // 8):
        bits = (rows_of(8) + 8 * c) | lanes_of(8)
        own = [(bits & ((2 << level) - 1)) == (1 << level) for level in range(NEAR)]
        rest = [(bits & ((1 << level) - 1)) == 0 for level in range(NEAR)]
        bounds = []
        for depth in range(NEAR + 1):
            bound = jnp.broadcast_to(th[pl.ds(min(depth, NEAR - 1), 1), :], (8, LANES))
            for level in range(min(depth, NEAR - 1) - 1, -1, -1):
                bound = jnp.where(own[level], th[pl.ds(level, 1), :], bound)
            bounds.append(bound)
        squares = [None] * (NEAR + 1)
        sizes = [None] * (NEAR + 1)
        for x in range(SIDE):
            depth = NEAR if x == 0 else min(NEAR, (x & -x).bit_length() - 1)
            cells = v[pl.ds(x * PITCH + 8 * c, 8), :]
            shrunk = cells - jnp.minimum(jnp.maximum(cells, -bounds[depth]), bounds[depth])
            coef[pl.ds(x * SIDE + 8 * c, 8), :] = shrunk
            square, size = cells * cells, jnp.abs(shrunk)
            squares[depth] = square if squares[depth] is None else squares[depth] + square
            sizes[depth] = size if sizes[depth] is None else sizes[depth] + size
        for sums, target in ((squares, energy), (sizes, kept)):
            for level in range(NEAR):
                deeper = functools.reduce(lambda a, b: a + b, sums[level + 1 :])
                part = jnp.where(rest[level], sums[level], 0.0) + jnp.where(own[level], deeper, 0.0)
                target[level] = target[level] + part

    lane8 = lanes_of(8)
    corners = [v[pl.ds(a * 16 * PITCH + b * 16, 1), :] for a in range(2) for b in range(2)]
    block = jnp.zeros((8, LANES), F32)
    for i, corner in enumerate(corners):
        block = jnp.where(row8 == i, corner, block)
    source, target = rows_of(LANES), lanes_of(LANES)
    pick = jnp.where((source == 16 * (target % 8)) & (target < 32), 1.0, 0.0).astype(F32)
    block = jnp.where(lane8 // 8 == row8, dot(block, pick), 0.0)
    for i, part in enumerate(energy + kept):
        block = jnp.where((lane8 == 32 + i) & (row8 == 0), jnp.sum(part), block)
    send[...] = jnp.broadcast_to(jnp.sum(block, axis=0, keepdims=True), send.shape)


def last_kernel(got, spot, coef, th, out, stats, grid, *, sizes, counts):
    nx, ny, nz = sizes
    plane = ny * nz
    lane, row = lanes_of(plane), rows_of(plane)
    turn = pl.program_id(0)

    @pl.when(turn == 0)
    def _():
        v = [got[pl.ds(i * plane, plane), :] for i in range(nx)]
        sums = functools.reduce(lambda a, b: a + b, v)
        sums = jnp.sum(sums, axis=0, keepdims=True)

        def down(a, shift):
            return pltpu.roll(a, shift % plane, 0)

        odd = (lane & 16) != 0
        d = [v[i] - 0.5 * roll(v[i] + v[(i + 1) % nx], 16) for i in range(nx)]
        v = [jnp.where(odd, d[i], v[i] + 0.25 * roll(d[i] + d[i - 1], -16)) for i in range(nx)]
        odd = (lane & 8) != 0
        d = [a - 0.5 * roll(a + down(a, -nz), 8) for a in v]
        v = [jnp.where(odd, b, a + 0.25 * roll(b + down(b, nz), -8)) for a, b in zip(v, d)]
        odd = (lane & 1) != 0
        top, low = (lane & 7) == 7, (lane & 7) == 0
        far = row % nz == nz - 1
        near = row % nz == 0
        result = []
        for a in v:
            following = jnp.where(far, down(a, nz - 1), down(a, -1))
            d = a - 0.5 * (roll(a, 1) + jnp.where(top, roll(following, 7), roll(a, -1)))
            previous = jnp.where(near, down(d, 1 - nz), down(d, 1))
            s = a + 0.25 * (jnp.where(low, roll(previous, -7), roll(d, 1)) + roll(d, -1))
            result.append(jnp.where(odd, d, s))
        bound = th[pl.ds(LEVELS - 1, 1), :]
        detail = (lane < 32) & ((lane & 25) != 0)
        energy = kept = None
        for i, a in enumerate(result):
            shrunk = a - jnp.minimum(jnp.maximum(a, -bound), bound)
            grid[pl.ds(i * plane, plane), :] = jnp.where(detail, shrunk, a)
            square, size = jnp.where(detail, a * a, 0.0), jnp.where(detail, jnp.abs(shrunk), 0.0)
            energy = square if energy is None else energy + square
            kept = size if kept is None else kept + size
        lane1 = lanes_of(1)
        for i, (part, base) in enumerate(((energy, 32), (kept, 36))):
            totals = jnp.where(lane1 == NEAR, jnp.sum(part), roll(sums, -base))
            scale = jnp.zeros((1, LANES), F32)
            for level in range(LEVELS):
                scale = jnp.where(lane1 == level, 1.0 / counts[level], scale)
            stats[i] = (totals * scale)[:, :LEVELS]

    own = grid[pl.ds(spot[0], 1), :]
    row8, lane8 = rows_of(8), lanes_of(8)
    block = jnp.where((lane8 < 32) & (lane8 // 8 == 2 * turn + row8) & (row8 < 2), own, 0.0)
    source, target = rows_of(LANES), lanes_of(LANES)
    pick = jnp.where((target == 16 * (source % 8)) & (source < 32), 1.0, 0.0).astype(F32)
    block = dot(block, pick)
    out[...] = coef[...]
    start = (lane8[:1] % 16) == 0
    for b in range(2):
        at = pl.ds(16 * b, 1)
        out[at, :] = jnp.where(start, block[b : b + 1, :], coef[at, :])


def shape(*dims):
    return jax.ShapeDtypeStruct(dims, F32)


def shards(fields, exponents):
    sizes = tuple(lax.axis_size(a) for a in ("gx", "gy", "gz"))
    devices = sizes[0] * sizes[1] * sizes[2]
    cells = fields.size * devices
    counts = [7.0 * cells / 8 ** (level + 1) for level in range(LEVELS)]
    f = fields.reshape(SIDE * SIDE, LANES)
    th = jnp.broadcast_to(jnp.pad(jnp.exp2(exponents.astype(F32)), (0, 3))[:, None], (8, LANES))
    tables = jnp.asarray(constant_tables())
    wy = jnp.asarray(W.astype(np.float32))

    def swap(up, down, axis):
        n = lax.axis_size(axis)
        before = lax.ppermute(up, axis, [(i, (i + 1) % n) for i in range(n)])
        after = lax.ppermute(down, axis, [((i + 1) % n, i) for i in range(n)])
        return before, after

    pz, fx, fy = pl.pallas_call(
        ends_kernel,
        out_shape=(shape(2 * SIDE, LANES), shape(EXT * SIDE, LANES), shape(EXT * SIDE, LANES)),
        name="ends",
    )(f, tables[0])
    before, after = swap(pz, pz, "gz")
    message = shape((NEAR + 1) * SIDE, LANES)
    ez, up, down = pl.pallas_call(
        depth_kernel, out_shape=(shape(2 * SIDE, LANES), message, message), name="depth"
    )(pz, before, after, fx, tables)
    before, after = swap(up, down, "gx")
    message = shape(NEAR * PITCH + 3 * EXT, LANES)
    xe, xee, yup, ydown = pl.pallas_call(
        width_kernel,
        out_shape=(shape(EXT * SIDE, LANES), shape(SIDE, LANES), message, message),
        name="width",
    )(up, down, before, after, fy, ez, wy, tables)
    before, after = swap(yup, ydown, "gy")
    coef, send = pl.pallas_call(
        levels_kernel,
        out_shape=(shape(SIDE * SIDE, LANES), shape(devices, LANES)),
        scratch_shapes=[pltpu.VMEM((PITCH * PITCH, LANES), F32)] * 2,
        name="levels",
    )(f, ez, xe, xee, yup, ydown, before, after, th)
    got = lax.all_to_all(send.reshape(devices, 1, LANES), ("gx", "gy", "gz"), 0, 0).reshape(devices, LANES)
    spot = lax.axis_index(("gx", "gy", "gz")).astype(jnp.int32).reshape(1)
    whole = lambda *dims: pl.BlockSpec(dims, lambda i: (0,) * len(dims))
    out, stats = pl.pallas_call(
        functools.partial(last_kernel, sizes=sizes, counts=counts),
        grid=(2,),
        in_specs=[
            whole(devices, LANES),
            pl.BlockSpec(memory_space=pltpu.SMEM),
            pl.BlockSpec((SIDE, LANES), lambda i: (16 * i, 0)),
            whole(8, LANES),
        ],
        out_specs=[pl.BlockSpec((SIDE, LANES), lambda i: (16 * i, 0)), whole(2, 1, LEVELS)],
        out_shape=(shape(SIDE * SIDE, LANES), shape(2, 1, LEVELS)),
        scratch_shapes=[pltpu.VMEM((devices, LANES), F32)],
        input_output_aliases={2: 0},
        name="last",
    )(got, spot, coef, th)
    return out.reshape(fields.shape), stats


def solution(mesh):
    placed = (P(None, "gx", "gy", "gz"), P())
    return jax.shard_map(shards, mesh=mesh, in_specs=placed, out_specs=placed, check_vma=False)
```

```python
import functools

import jax
import jax.numpy as jnp
import numpy as np
from jax import lax
from jax.experimental import pallas as pl
from jax.experimental.pallas import tpu as pltpu
from jax.sharding import PartitionSpec as P

NEAR = 4
LEVELS = 5
LANES = 128
SIDE = 32
EXT = 2 * NEAR
PITCH = SIDE + EXT
F32 = jnp.float32


def cascade(cells, ahead, behind):
    details, firsts = [], []
    for level in range(NEAR):
        half = len(cells) // 2
        following = cells[2::2] + [ahead[level]]
        detail = [cells[2 * k + 1] - 0.5 * (cells[2 * k] + following[k]) for k in range(half)]
        details.append(detail[-1])
        firsts.append(cells[0])
        before = [behind[level]] + detail[:-1]
        cells = [cells[2 * k] + 0.25 * (before[k] + detail[k]) for k in range(half)]
    return details, firsts


def end_weights(length):
    none = [np.zeros(length)] * NEAR
    details, firsts = cascade(list(np.eye(length)), none, none)
    return np.stack(details + firsts)


def seam_weights():
    zero = [np.zeros(1)] * NEAR
    flat = [np.zeros(1)] * SIDE
    alpha = np.zeros((NEAR, NEAR))
    beta = np.zeros((NEAR, NEAR))
    for j in range(NEAR):
        unit = [np.ones(1) * (k == j) for k in range(NEAR)]
        alpha[:, j] = [d[0] for d in cascade(flat, unit, zero)[0]]
        beta[:, j] = [f[0] for f in cascade(flat, zero, unit)[1]]
    lasts, firsts = [], []
    for level in range(NEAR):
        first = np.eye(EXT)[NEAR + level]
        for j in range(level):
            first = first + beta[level, j] * lasts[j]
        firsts.append(first)
        last = np.eye(EXT)[level]
        for j in range(level + 1):
            last = last + alpha[level, j] * firsts[j]
        lasts.append(last)
    return np.stack(lasts), np.stack(firsts)


W = end_weights(SIDE)
WZ = end_weights(LANES)
LAST, FIRST = seam_weights()
GROUP = LANES // EXT


def constant_tables():
    tables = np.zeros((9, LANES, LANES), np.float32)
    left = np.zeros((EXT, EXT))
    right = np.zeros((EXT, EXT))
    left[:, :NEAR] = LAST.T
    right[:, NEAR:] = FIRST.T
    spread = np.zeros((2, EXT, EXT))
    for level in range(NEAR):
        spread[0, level, EXT - (1 << level)] = 1.0
        spread[1, NEAR + level, EXT - (1 << level)] = 1.0
    tables[0] = np.tile(WZ.T, (1, GROUP))
    tables[1] = np.kron(np.eye(GROUP), left)
    tables[2] = np.kron(np.eye(GROUP), right)
    for half in range(2):
        tables[3 + half, :, : EXT * EXT] = np.kron(W[:, half * GROUP : (half + 1) * GROUP].T, np.eye(EXT))
    tables[5, : EXT * EXT, : EXT * EXT] = np.kron(left, np.eye(EXT))
    tables[6, : EXT * EXT, : EXT * EXT] = np.kron(right, np.eye(EXT))
    tables[7] = np.kron(np.eye(GROUP), spread[0])
    tables[8] = np.kron(np.eye(GROUP), spread[1])
    return tables


def dot(a, b):
    return jnp.dot(a, b, precision=lax.Precision.HIGHEST, preferred_element_type=F32)


def lanes_of(rows):
    return lax.broadcasted_iota(jnp.int32, (rows, LANES), 1)


def rows_of(rows):
    return lax.broadcasted_iota(jnp.int32, (rows, LANES), 0)


def roll(v, shift):
    return pltpu.roll(v, shift % LANES, 1)


def weighted(rows, load):
    sums = [None] * EXT
    for i in range(SIDE):
        block = load(i)
        for g in range(EXT):
            if W[g, i] != 0.0:
                term = float(W[g, i]) * block
                sums[g] = term if sums[g] is None else sums[g] + term
    return sums


def mix(weights, blocks):
    total = None
    for w, block in zip(weights, blocks):
        if w != 0.0:
            term = float(w) * block
            total = term if total is None else total + term
    return total


def ends_kernel(f, table, pz, fx, fy):
    lane = lanes_of(SIDE)
    packed = [jnp.zeros((SIDE, LANES), F32)] * 2
    for x in range(SIDE):
        out = dot(f[pl.ds(x * SIDE, SIDE), :], table[...])
        packed[x // GROUP] = jnp.where(lane // EXT == x % GROUP, out, packed[x // GROUP])
    for half in range(2):
        pz[pl.ds(half * SIDE, SIDE), :] = packed[half]
    for c in range(SIDE // 8):
        for g, block in enumerate(weighted(8, lambda x: f[pl.ds(x * SIDE + 8 * c, 8), :])):
            fx[pl.ds(g * SIDE + 8 * c, 8), :] = block
    for c in range(SIDE // 8):
        for g, block in enumerate(weighted(8, lambda y: f[pl.ds(8 * c * SIDE + y, 8, stride=SIDE), :])):
            fy[pl.ds(g * SIDE + 8 * c, 8), :] = block


def depth_kernel(pz, before, after, fx, tables, ez, up, down):
    slot = lanes_of(SIDE) % EXT
    fxe = None
    for half in range(2):
        rows = pl.ds(half * SIDE, SIDE)
        own = pz[rows, :]
        full = dot(jnp.where(slot < NEAR, before[rows, :], own), tables[1]) + dot(
            jnp.where(slot < NEAR, own, after[rows, :]), tables[2]
        )
        ez[rows, :] = full
        part = dot(full, tables[3 + half])
        fxe = part if fxe is None else fxe + part
    for g in range(NEAR):
        up[pl.ds(g * SIDE, SIDE), :] = fx[pl.ds(g * SIDE, SIDE), :]
        down[pl.ds(g * SIDE, SIDE), :] = fx[pl.ds((NEAR + g) * SIDE, SIDE), :]
    up[pl.ds(NEAR * SIDE, SIDE), :] = fxe
    down[pl.ds(NEAR * SIDE, SIDE), :] = fxe


def width_kernel(up, down, before, after, fy, ez, wy, tables, xe, xee, yup, ydown):
    for c in range(SIDE // 8):
        rows = [pl.ds(g * SIDE + 8 * c, 8) for g in range(NEAR)]
        own_last = [up[r, :] for r in rows]
        own_first = [down[r, :] for r in rows]
        seam_before = [before[r, :] for r in rows] + own_first
        seam_after = own_last + [after[r, :] for r in rows]
        for level in range(NEAR):
            xe[pl.ds(level * SIDE + 8 * c, 8), :] = mix(LAST[level], seam_before)
            xe[pl.ds((NEAR + level) * SIDE + 8 * c, 8), :] = mix(FIRST[level], seam_after)
    slot = lanes_of(SIDE) // EXT
    rows = pl.ds(NEAR * SIDE, SIDE)
    own = up[rows, :]
    corner = dot(jnp.where(slot < NEAR, before[rows, :], own), tables[5]) + dot(
        jnp.where(slot < NEAR, own, after[rows, :]), tables[6]
    )
    xee[...] = corner
    sums = weighted(EXT, lambda y: xe[pl.ds(y, EXT, stride=SIDE), :])
    for g in range(EXT):
        target = yup if g < NEAR else ydown
        base = (g % NEAR) * PITCH
        target[pl.ds(base, SIDE), :] = fy[pl.ds(g * SIDE, SIDE), :]
        target[pl.ds(base + SIDE, EXT), :] = sums[g]
    for i, block in enumerate((ez[pl.ds(0, SIDE), :], ez[pl.ds(SIDE, SIDE), :], corner)):
        part = dot(wy[...], block)
        yup[pl.ds(NEAR * PITCH + i * EXT, EXT), :] = part
        ydown[pl.ds(NEAR * PITCH + i * EXT, EXT), :] = part


def lift_chunk(ref, at, level, masked):
    step = 1 << level
    pairs = SIDE // (2 * step)
    masked = masked and level > 0
    behind = ref[at(SIDE + level), :]
    even = ref[at(0), :]
    for k in range(pairs):
        odd = ref[at(step * (2 * k + 1)), :]
        ahead = ref[at(step * (2 * k + 2)), :] if k < pairs - 1 else ref[at(SIDE + NEAR + level), :]
        detail = odd - 0.5 * (even + ahead)
        smooth = even + 0.25 * (behind + detail)
        if masked:
            live = (lanes_of(odd.shape[0]) & (step - 1)) == 0
            detail, smooth = jnp.where(live, detail, odd), jnp.where(live, smooth, even)
        ref[at(step * (2 * k + 1)), :] = detail
        ref[at(2 * step * k), :] = smooth
        behind, even = detail, ahead


def chunks(level):
    step = 1 << level
    count = SIDE // step
    own = [(8 * step * c, min(8, count), step) for c in range(max(1, count // 8))]
    return own + ([(SIDE, EXT, 1)] if level < NEAR else [])


def lift_lanes(level, v, qa, qb, t, d):
    step = 1 << level
    own = SIDE // step
    parts = [c for c in chunks(level) if c[0] < SIDE or level < NEAR - 1]
    total = own + (EXT if level < NEAR - 1 else 0)

    def sweep(work):
        def body(half, carry):
            for k in range(total // 2):
                j = half * (total // 2) + k
                x = j if step == 1 else jnp.where(j < own, j * step, j + (SIDE - own))
                for first, count, stride in parts:
                    work(pl.ds(x * PITCH + first, count, stride=stride), lanes_of(count))
            return carry

        lax.fori_loop(0, 2, body, 0)

    def left(at, lane):
        t[at, :] = roll(v[at, :], step)

    def detail(at, lane):
        cells = v[at, :]
        ahead = jnp.where(lane == LANES - step, qb[at, :], roll(cells, -step))
        d[at, :] = cells - 0.5 * (t[at, :] + ahead)

    def behind(at, lane):
        t[at, :] = roll(jnp.where(lane == LANES - step, qa[at, :], d[at, :]), step)

    def smooth(at, lane):
        cells, mid = v[at, :], d[at, :]
        even = cells + 0.25 * (t[at, :] + roll(mid, -step))
        place = lane & (2 * step - 1)
        v[at, :] = jnp.where(place == 0, even, jnp.where(place == step, mid, cells))

    for work in (left, detail, behind, smooth):
        sweep(work)


def levels_kernel(f, ez, xe, xee, yup, ydown, before, after, th, tables, coef, send, v, qa, qb, t, d):
    for x in range(SIDE):
        v[pl.ds(x * PITCH, SIDE), :] = f[pl.ds(x * SIDE, SIDE), :]
    for g in range(EXT):
        v[pl.ds((SIDE + g) * PITCH, SIDE), :] = xe[pl.ds(g * SIDE, SIDE), :]
    for c in range(PITCH // 8):
        rows = [pl.ds(g * PITCH + 8 * c, 8) for g in range(NEAR)]
        seam_before = [before[r, :] for r in rows] + [ydown[r, :] for r in rows]
        seam_after = [yup[r, :] for r in rows] + [after[r, :] for r in rows]
        for level in range(NEAR):
            v[pl.ds(8 * c * PITCH + SIDE + level, 8, stride=PITCH), :] = mix(LAST[level], seam_before)
            v[pl.ds(8 * c * PITCH + SIDE + NEAR + level, 8, stride=PITCH), :] = mix(FIRST[level], seam_after)
    row8 = rows_of(EXT)
    for i in range(3):
        first = NEAR * PITCH + i * EXT
        own = [yup[pl.ds(first + j, 1), :] for j in range(EXT)]
        seam_before = [before[pl.ds(first + j, 1), :] for j in range(NEAR)] + own[NEAR:]
        seam_after = own[:NEAR] + [after[pl.ds(first + NEAR + j, 1), :] for j in range(NEAR)]
        extra = jnp.zeros((EXT, LANES), F32)
        for level in range(NEAR):
            extra = jnp.where(row8 == level, mix(LAST[level], seam_before), extra)
            extra = jnp.where(row8 == NEAR + level, mix(FIRST[level], seam_after), extra)
        block = ez[pl.ds(i * SIDE, SIDE), :] if i < 2 else xee[...]
        parts = [(dot(block, tables[7 + k]), dot(extra, tables[7 + k])) for k in range(2)]
        for j in range(GROUP if i < 2 else EXT):
            x = i * GROUP + j
            for ref, (main, rest) in zip((qa, qb), parts):
                ref[pl.ds(x * PITCH, SIDE), :] = roll(main, -EXT * (j + 1))
                ref[pl.ds(x * PITCH + SIDE, EXT), :] = roll(rest, -EXT * (j + 1))

    for level in range(NEAR):
        step = 1 << level
        for ref in (v, qa, qb):
            for first, count, stride in chunks(level):
                lift_chunk(ref, lambda i: pl.ds(i * PITCH + first, count, stride=stride), level, ref is v)
            for first, count, stride in chunks(level):
                lift_chunk(ref, lambda i: pl.ds(first * PITCH + i, count, stride=stride * PITCH), level, ref is v)
        lift_lanes(level, v, qa, qb, t, d)

    energy = [jnp.zeros((8, LANES), F32)] * NEAR
    kept = [jnp.zeros((8, LANES), F32)] * NEAR
    for c in range(SIDE // 8):
        bits = (rows_of(8) + 8 * c) | lanes_of(8)
        own = [(bits & ((2 << level) - 1)) == (1 << level) for level in range(NEAR)]
        rest = [(bits & ((1 << level) - 1)) == 0 for level in range(NEAR)]
        bounds = []
        for depth in range(NEAR + 1):
            bound = jnp.broadcast_to(th[pl.ds(min(depth, NEAR - 1), 1), :], (8, LANES))
            for level in range(min(depth, NEAR - 1) - 1, -1, -1):
                bound = jnp.where(own[level], th[pl.ds(level, 1), :], bound)
            bounds.append(bound)
        squares = [None] * (NEAR + 1)
        sizes = [None] * (NEAR + 1)
        for x in range(SIDE):
            depth = NEAR if x == 0 else min(NEAR, (x & -x).bit_length() - 1)
            cells = v[pl.ds(x * PITCH + 8 * c, 8), :]
            shrunk = cells - jnp.minimum(jnp.maximum(cells, -bounds[depth]), bounds[depth])
            coef[pl.ds(x * SIDE + 8 * c, 8), :] = shrunk
            square, size = cells * cells, jnp.abs(shrunk)
            squares[depth] = square if squares[depth] is None else squares[depth] + square
            sizes[depth] = size if sizes[depth] is None else sizes[depth] + size
        for sums, target in ((squares, energy), (sizes, kept)):
            for level in range(NEAR):
                deeper = functools.reduce(lambda a, b: a + b, sums[level + 1 :])
                part = jnp.where(rest[level], sums[level], 0.0) + jnp.where(own[level], deeper, 0.0)
                target[level] = target[level] + part

    lane8 = lanes_of(8)
    corners = [v[pl.ds(a * 16 * PITCH + b * 16, 1), :] for a in range(2) for b in range(2)]
    block = jnp.zeros((8, LANES), F32)
    for i, corner in enumerate(corners):
        block = jnp.where(row8 == i, corner, block)
    source, target = rows_of(LANES), lanes_of(LANES)
    pick = jnp.where((source == 16 * (target % 8)) & (target < 32), 1.0, 0.0).astype(F32)
    block = jnp.where(lane8 // 8 == row8, dot(block, pick), 0.0)
    for i, part in enumerate(energy + kept):
        block = jnp.where((lane8 == 32 + i) & (row8 == 0), jnp.sum(part), block)
    send[...] = jnp.broadcast_to(jnp.sum(block, axis=0, keepdims=True), send.shape)


def last_kernel(got, spot, coef, th, out, stats, grid, *, sizes, counts):
    nx, ny, nz = sizes
    plane = ny * nz
    lane, row = lanes_of(plane), rows_of(plane)
    turn = pl.program_id(0)

    @pl.when(turn == 0)
    def _():
        v = [got[pl.ds(i * plane, plane), :] for i in range(nx)]
        sums = functools.reduce(lambda a, b: a + b, v)
        sums = jnp.sum(sums, axis=0, keepdims=True)

        def down(a, shift):
            return pltpu.roll(a, shift % plane, 0)

        odd = (lane & 16) != 0
        d = [v[i] - 0.5 * roll(v[i] + v[(i + 1) % nx], 16) for i in range(nx)]
        v = [jnp.where(odd, d[i], v[i] + 0.25 * roll(d[i] + d[i - 1], -16)) for i in range(nx)]
        odd = (lane & 8) != 0
        d = [a - 0.5 * roll(a + down(a, -nz), 8) for a in v]
        v = [jnp.where(odd, b, a + 0.25 * roll(b + down(b, nz), -8)) for a, b in zip(v, d)]
        odd = (lane & 1) != 0
        top, low = (lane & 7) == 7, (lane & 7) == 0
        far = row % nz == nz - 1
        near = row % nz == 0
        result = []
        for a in v:
            following = jnp.where(far, down(a, nz - 1), down(a, -1))
            d = a - 0.5 * (roll(a, 1) + jnp.where(top, roll(following, 7), roll(a, -1)))
            previous = jnp.where(near, down(d, 1 - nz), down(d, 1))
            s = a + 0.25 * (jnp.where(low, roll(previous, -7), roll(d, 1)) + roll(d, -1))
            result.append(jnp.where(odd, d, s))
        bound = th[pl.ds(LEVELS - 1, 1), :]
        detail = (lane < 32) & ((lane & 25) != 0)
        energy = kept = None
        for i, a in enumerate(result):
            shrunk = a - jnp.minimum(jnp.maximum(a, -bound), bound)
            grid[pl.ds(i * plane, plane), :] = jnp.where(detail, shrunk, a)
            square, size = jnp.where(detail, a * a, 0.0), jnp.where(detail, jnp.abs(shrunk), 0.0)
            energy = square if energy is None else energy + square
            kept = size if kept is None else kept + size
        lane1 = lanes_of(1)
        for i, (part, base) in enumerate(((energy, 32), (kept, 36))):
            totals = jnp.where(lane1 == NEAR, jnp.sum(part), roll(sums, -base))
            scale = jnp.zeros((1, LANES), F32)
            for level in range(LEVELS):
                scale = jnp.where(lane1 == level, 1.0 / counts[level], scale)
            stats[i] = (totals * scale)[:, :LEVELS]

    own = grid[pl.ds(spot[0], 1), :]
    row8, lane8 = rows_of(8), lanes_of(8)
    block = jnp.where((lane8 < 32) & (lane8 // 8 == 2 * turn + row8) & (row8 < 2), own, 0.0)
    source, target = rows_of(LANES), lanes_of(LANES)
    pick = jnp.where((target == 16 * (source % 8)) & (source < 32), 1.0, 0.0).astype(F32)
    block = dot(block, pick)
    out[...] = coef[...]
    start = (lane8[:1] % 16) == 0
    for b in range(2):
        at = pl.ds(16 * b, 1)
        out[at, :] = jnp.where(start, block[b : b + 1, :], coef[at, :])


def shape(*dims):
    return jax.ShapeDtypeStruct(dims, F32)


def shards(fields, exponents):
    sizes = tuple(lax.axis_size(a) for a in ("gx", "gy", "gz"))
    devices = sizes[0] * sizes[1] * sizes[2]
    cells = fields.size * devices
    counts = [7.0 * cells / 8 ** (level + 1) for level in range(LEVELS)]
    f = fields.reshape(SIDE * SIDE, LANES)
    th = jnp.broadcast_to(jnp.pad(jnp.exp2(exponents.astype(F32)), (0, 3))[:, None], (8, LANES))
    tables = jnp.asarray(constant_tables())
    wy = jnp.asarray(W.astype(np.float32))

    def swap(up, down, axis):
        n = lax.axis_size(axis)
        before = lax.ppermute(up, axis, [(i, (i + 1) % n) for i in range(n)])
        after = lax.ppermute(down, axis, [((i + 1) % n, i) for i in range(n)])
        return before, after

    here = pl.BlockSpec(memory_space=pltpu.VMEM)

    def pinned(a):
        return pltpu.with_memory_space_constraint(a, pltpu.VMEM)

    def local(kernel, name, outs, *args, scratch=()):
        args = [pinned(a) for a in args]
        return pl.pallas_call(
            kernel,
            in_specs=[here] * len(args),
            out_specs=[here] * len(outs),
            out_shape=[pltpu.VMEM((rows, LANES), F32) for rows in outs],
            scratch_shapes=[pltpu.VMEM((rows, LANES), F32) for rows in scratch],
            name=name,
        )(*args)

    pz, fx, fy = local(ends_kernel, "ends", (2 * SIDE, EXT * SIDE, EXT * SIDE), f, tables[0])
    before, after = swap(pz, pz, "gz")
    message = (NEAR + 1) * SIDE
    ez, up, down = local(
        depth_kernel, "depth", (2 * SIDE, message, message), pz, before, after, fx, tables
    )
    before, after = swap(up, down, "gx")
    message = NEAR * PITCH + 3 * EXT
    xe, xee, yup, ydown = local(
        width_kernel, "width", (EXT * SIDE, SIDE, message, message), up, down, before, after, fy, ez, wy, tables
    )
    before, after = swap(yup, ydown, "gy")
    coef, send = local(
        levels_kernel,
        "levels",
        (SIDE * SIDE, devices),
        *(f, ez, xe, xee, yup, ydown, before, after, th, tables),
        scratch=[PITCH * PITCH] * 5,
    )
    got = lax.all_to_all(send.reshape(devices, 1, LANES), ("gx", "gy", "gz"), 0, 0).reshape(devices, LANES)
    spot = lax.axis_index(("gx", "gy", "gz")).astype(jnp.int32).reshape(1)
    whole = lambda *dims: pl.BlockSpec(dims, lambda i: (0,) * len(dims))
    out, stats = pl.pallas_call(
        functools.partial(last_kernel, sizes=sizes, counts=counts),
        grid=(2,),
        in_specs=[
            here,
            pl.BlockSpec(memory_space=pltpu.SMEM),
            pl.BlockSpec((SIDE, LANES), lambda i: (16 * i, 0)),
            here,
        ],
        out_specs=[pl.BlockSpec((SIDE, LANES), lambda i: (16 * i, 0)), whole(2, 1, LEVELS)],
        out_shape=(shape(SIDE * SIDE, LANES), shape(2, 1, LEVELS)),
        scratch_shapes=[pltpu.VMEM((devices, LANES), F32)],
        input_output_aliases={2: 0},
        name="last",
    )(pinned(got), spot, coef, pinned(th))
    return out.reshape(fields.shape), stats


def solution(mesh):
    placed = (P(None, "gx", "gy", "gz"), P())
    return jax.shard_map(shards, mesh=mesh, in_specs=placed, out_specs=placed, check_vma=False)
```

```python
import functools

import jax
import jax.numpy as jnp
import numpy as np
from jax import lax
from jax.experimental import pallas as pl
from jax.experimental.pallas import tpu as pltpu
from jax.sharding import PartitionSpec as P

NEAR = 4
LEVELS = 5
LANES = 128
SIDE = 32
EXT = 2 * NEAR
PITCH = SIDE + EXT
F32 = jnp.float32


def cascade(cells, ahead, behind):
    details, firsts = [], []
    for level in range(NEAR):
        half = len(cells) // 2
        following = cells[2::2] + [ahead[level]]
        detail = [cells[2 * k + 1] - 0.5 * (cells[2 * k] + following[k]) for k in range(half)]
        details.append(detail[-1])
        firsts.append(cells[0])
        before = [behind[level]] + detail[:-1]
        cells = [cells[2 * k] + 0.25 * (before[k] + detail[k]) for k in range(half)]
    return details, firsts


def end_weights(length):
    none = [np.zeros(length)] * NEAR
    details, firsts = cascade(list(np.eye(length)), none, none)
    return np.stack(details + firsts)


def seam_weights():
    zero = [np.zeros(1)] * NEAR
    flat = [np.zeros(1)] * SIDE
    alpha = np.zeros((NEAR, NEAR))
    beta = np.zeros((NEAR, NEAR))
    for j in range(NEAR):
        unit = [np.ones(1) * (k == j) for k in range(NEAR)]
        alpha[:, j] = [d[0] for d in cascade(flat, unit, zero)[0]]
        beta[:, j] = [f[0] for f in cascade(flat, zero, unit)[1]]
    lasts, firsts = [], []
    for level in range(NEAR):
        first = np.eye(EXT)[NEAR + level]
        for j in range(level):
            first = first + beta[level, j] * lasts[j]
        firsts.append(first)
        last = np.eye(EXT)[level]
        for j in range(level + 1):
            last = last + alpha[level, j] * firsts[j]
        lasts.append(last)
    return np.stack(lasts), np.stack(firsts)


W = end_weights(SIDE)
WZ = end_weights(LANES)
LAST, FIRST = seam_weights()
GROUP = LANES // EXT


def constant_tables():
    tables = np.zeros((9, LANES, LANES), np.float32)
    left = np.zeros((EXT, EXT))
    right = np.zeros((EXT, EXT))
    left[:, :NEAR] = LAST.T
    right[:, NEAR:] = FIRST.T
    spread = np.zeros((2, EXT, EXT))
    for level in range(NEAR):
        spread[0, level, EXT - (1 << level)] = 1.0
        spread[1, NEAR + level, EXT - (1 << level)] = 1.0
    tables[0] = np.tile(WZ.T, (1, GROUP))
    tables[1] = np.kron(np.eye(GROUP), left)
    tables[2] = np.kron(np.eye(GROUP), right)
    for half in range(2):
        tables[3 + half, :, : EXT * EXT] = np.kron(W[:, half * GROUP : (half + 1) * GROUP].T, np.eye(EXT))
    tables[5, : EXT * EXT, : EXT * EXT] = np.kron(left, np.eye(EXT))
    tables[6, : EXT * EXT, : EXT * EXT] = np.kron(right, np.eye(EXT))
    tables[7] = np.kron(np.eye(GROUP), spread[0])
    tables[8] = np.kron(np.eye(GROUP), spread[1])
    return tables


def dot(a, b):
    return jnp.dot(a, b, precision=lax.Precision.HIGHEST, preferred_element_type=F32)


def lanes_of(rows):
    return lax.broadcasted_iota(jnp.int32, (rows, LANES), 1)


def rows_of(rows):
    return lax.broadcasted_iota(jnp.int32, (rows, LANES), 0)


def roll(v, shift):
    return pltpu.roll(v, shift % LANES, 1)


def weighted(rows, load):
    sums = [None] * EXT
    for i in range(SIDE):
        block = load(i)
        for g in range(EXT):
            if W[g, i] != 0.0:
                term = float(W[g, i]) * block
                sums[g] = term if sums[g] is None else sums[g] + term
    return sums


def mix(weights, blocks):
    total = None
    for w, block in zip(weights, blocks):
        if w != 0.0:
            term = float(w) * block
            total = term if total is None else total + term
    return total


def ends_kernel(f, table, pz):
    turn = pl.program_id(0)
    rows = pl.ds(turn // 2 * SIDE, SIDE)
    group = lanes_of(SIDE) // EXT
    packed = jnp.where(turn % 2 == 0, jnp.zeros((SIDE, LANES), F32), pz[rows, :])
    for j in range(GROUP // 2):
        out = dot(f[pl.ds(j * SIDE, SIDE), :], table[...])
        packed = jnp.where(group == turn % 2 * (GROUP // 2) + j, out, packed)
    pz[rows, :] = packed


def faces_kernel(f, fx, fy):
    for c in range(SIDE // 8):
        for g, block in enumerate(weighted(8, lambda x: f[pl.ds(x * SIDE + 8 * c, 8), :])):
            fx[pl.ds(g * SIDE + 8 * c, 8), :] = block
    for c in range(SIDE // 8):
        for g, block in enumerate(weighted(8, lambda y: f[pl.ds(8 * c * SIDE + y, 8, stride=SIDE), :])):
            fy[pl.ds(g * SIDE + 8 * c, 8), :] = block


def depth_kernel(pz, before, after, fx, tables, ez, up, down):
    slot = lanes_of(SIDE) % EXT
    fxe = None
    for half in range(2):
        rows = pl.ds(half * SIDE, SIDE)
        own = pz[rows, :]
        full = dot(jnp.where(slot < NEAR, before[rows, :], own), tables[1]) + dot(
            jnp.where(slot < NEAR, own, after[rows, :]), tables[2]
        )
        ez[rows, :] = full
        part = dot(full, tables[3 + half])
        fxe = part if fxe is None else fxe + part
    for g in range(NEAR):
        up[pl.ds(g * SIDE, SIDE), :] = fx[pl.ds(g * SIDE, SIDE), :]
        down[pl.ds(g * SIDE, SIDE), :] = fx[pl.ds((NEAR + g) * SIDE, SIDE), :]
    up[pl.ds(NEAR * SIDE, SIDE), :] = fxe
    down[pl.ds(NEAR * SIDE, SIDE), :] = fxe


def width_kernel(up, down, before, after, fy, ez, wy, tables, xe, xee, yup, ydown):
    for c in range(SIDE // 8):
        rows = [pl.ds(g * SIDE + 8 * c, 8) for g in range(NEAR)]
        own_last = [up[r, :] for r in rows]
        own_first = [down[r, :] for r in rows]
        seam_before = [before[r, :] for r in rows] + own_first
        seam_after = own_last + [after[r, :] for r in rows]
        for level in range(NEAR):
            xe[pl.ds(level * SIDE + 8 * c, 8), :] = mix(LAST[level], seam_before)
            xe[pl.ds((NEAR + level) * SIDE + 8 * c, 8), :] = mix(FIRST[level], seam_after)
    slot = lanes_of(SIDE) // EXT
    rows = pl.ds(NEAR * SIDE, SIDE)
    own = up[rows, :]
    corner = dot(jnp.where(slot < NEAR, before[rows, :], own), tables[5]) + dot(
        jnp.where(slot < NEAR, own, after[rows, :]), tables[6]
    )
    xee[...] = corner
    sums = weighted(EXT, lambda y: xe[pl.ds(y, EXT, stride=SIDE), :])
    for g in range(EXT):
        target = yup if g < NEAR else ydown
        base = (g % NEAR) * PITCH
        target[pl.ds(base, SIDE), :] = fy[pl.ds(g * SIDE, SIDE), :]
        target[pl.ds(base + SIDE, EXT), :] = sums[g]
    for i, block in enumerate((ez[pl.ds(0, SIDE), :], ez[pl.ds(SIDE, SIDE), :], corner)):
        part = dot(wy[...], block)
        yup[pl.ds(NEAR * PITCH + i * EXT, EXT), :] = part
        ydown[pl.ds(NEAR * PITCH + i * EXT, EXT), :] = part


def lift_chunk(ref, at, level, masked):
    step = 1 << level
    pairs = SIDE // (2 * step)
    masked = masked and level > 0
    behind = ref[at(SIDE + level), :]
    even = ref[at(0), :]
    for k in range(pairs):
        odd = ref[at(step * (2 * k + 1)), :]
        ahead = ref[at(step * (2 * k + 2)), :] if k < pairs - 1 else ref[at(SIDE + NEAR + level), :]
        detail = odd - 0.5 * (even + ahead)
        smooth = even + 0.25 * (behind + detail)
        if masked:
            live = (lanes_of(odd.shape[0]) & (step - 1)) == 0
            detail, smooth = jnp.where(live, detail, odd), jnp.where(live, smooth, even)
        ref[at(step * (2 * k + 1)), :] = detail
        ref[at(2 * step * k), :] = smooth
        behind, even = detail, ahead


def chunks(level):
    step = 1 << level
    count = SIDE // step
    own = [(8 * step * c, min(8, count), step) for c in range(max(1, count // 8))]
    return own + ([(SIDE, EXT, 1)] if level < NEAR else [])


def lift_lanes(level, go, v, qa, qb, d):
    step = 1 << level
    rows = [
        (pl.ds(x * PITCH + first, count, stride=stride), count)
        for x in list(range(0, SIDE, step)) + (list(range(SIDE, PITCH)) if level < NEAR - 1 else [])
        for first, count, stride in chunks(level)
        if first < SIDE or level < NEAR - 1
    ]

    @pl.when(go)
    def _():
        for at, count in rows:
            cells = v[at, :]
            odd = roll(cells, -step)
            ahead = roll(jnp.where(lanes_of(count) == LANES - step, qb[at, :], odd), -step)
            d[at, :] = odd - 0.5 * (cells + ahead)

    @pl.when(go)
    def _():
        for at, count in rows:
            lane = lanes_of(count)
            cells, mid = v[at, :], d[at, :]
            odd = roll(mid, step)
            behind = roll(jnp.where(lane == LANES - step, qa[at, :], odd), step)
            even = cells + 0.25 * (mid + behind)
            place = lane & (2 * step - 1)
            v[at, :] = jnp.where(place == 0, even, jnp.where(place == step, odd, cells))


def lift_width(ref, level, masked, pieces):
    for first, count, stride in pieces:
        lift_chunk(ref, lambda i: pl.ds(i * PITCH + first, count, stride=stride), level, masked)


def prepare_kernel(f, ez, xe, xee, tables, v, qa, qb):
    for x in range(SIDE):
        v[pl.ds(x * PITCH, SIDE), :] = f[pl.ds(x * SIDE, SIDE), :]
    for g in range(EXT):
        v[pl.ds((SIDE + g) * PITCH, SIDE), :] = xe[pl.ds(g * SIDE, SIDE), :]
    for i in range(3):
        block = ez[pl.ds(i * SIDE, SIDE), :] if i < 2 else xee[...]
        parts = [dot(block, tables[7 + k]) for k in range(2)]
        for j in range(GROUP if i < 2 else EXT):
            for ref, part in zip((qa, qb), parts):
                ref[pl.ds((i * GROUP + j) * PITCH, SIDE), :] = roll(part, -EXT * (j + 1))
    for ref in (v, qa, qb):
        lift_width(ref, 0, False, chunks(0)[:-1])


def levels_kernel(
    spot, yup, ydown, before, after, th, tables, v_in, qa_in, qb_in, coef, send, v, qa, qb, d
):
    del v_in, qa_in, qb_in
    go = spot[0] >= 0
    for c in range(PITCH // 8):
        rows = [pl.ds(g * PITCH + 8 * c, 8) for g in range(NEAR)]
        seam_before = [before[r, :] for r in rows] + [ydown[r, :] for r in rows]
        seam_after = [yup[r, :] for r in rows] + [after[r, :] for r in rows]
        for level in range(NEAR):
            v[pl.ds(8 * c * PITCH + SIDE + level, 8, stride=PITCH), :] = mix(LAST[level], seam_before)
            v[pl.ds(8 * c * PITCH + SIDE + NEAR + level, 8, stride=PITCH), :] = mix(FIRST[level], seam_after)
    row8 = rows_of(EXT)
    for i in range(3):
        first = NEAR * PITCH + i * EXT
        own = [yup[pl.ds(first + j, 1), :] for j in range(EXT)]
        seam_before = [before[pl.ds(first + j, 1), :] for j in range(NEAR)] + own[NEAR:]
        seam_after = own[:NEAR] + [after[pl.ds(first + NEAR + j, 1), :] for j in range(NEAR)]
        extra = jnp.zeros((EXT, LANES), F32)
        for level in range(NEAR):
            extra = jnp.where(row8 == level, mix(LAST[level], seam_before), extra)
            extra = jnp.where(row8 == NEAR + level, mix(FIRST[level], seam_after), extra)
        parts = [dot(extra, tables[7 + k]) for k in range(2)]
        for j in range(GROUP if i < 2 else EXT):
            for ref, part in zip((qa, qb), parts):
                ref[pl.ds((i * GROUP + j) * PITCH + SIDE, EXT), :] = roll(part, -EXT * (j + 1))

    for level in range(NEAR):
        for ref in (v, qa, qb):
            lift_width(ref, level, ref is v, chunks(level)[-1:] if level == 0 else chunks(level))
            for first, count, stride in chunks(level):
                lift_chunk(
                    ref,
                    lambda i: pl.ds(first * PITCH + i, count, stride=stride * PITCH),
                    level,
                    ref is v,
                )
        lift_lanes(level, go, v, qa, qb, d)

    energy = [jnp.zeros((8, LANES), F32)] * NEAR
    kept = [jnp.zeros((8, LANES), F32)] * NEAR
    for c in range(SIDE // 8):
        bits = (rows_of(8) + 8 * c) | lanes_of(8)
        own = [(bits & ((2 << level) - 1)) == (1 << level) for level in range(NEAR)]
        rest = [(bits & ((1 << level) - 1)) == 0 for level in range(NEAR)]
        bounds = []
        for depth in range(NEAR + 1):
            bound = jnp.broadcast_to(th[pl.ds(min(depth, NEAR - 1), 1), :], (8, LANES))
            for level in range(min(depth, NEAR - 1) - 1, -1, -1):
                bound = jnp.where(own[level], th[pl.ds(level, 1), :], bound)
            bounds.append(bound)
        squares = [None] * (NEAR + 1)
        sizes = [None] * (NEAR + 1)
        for x in range(SIDE):
            depth = NEAR if x == 0 else min(NEAR, (x & -x).bit_length() - 1)
            cells = v[pl.ds(x * PITCH + 8 * c, 8), :]
            shrunk = cells - jnp.minimum(jnp.maximum(cells, -bounds[depth]), bounds[depth])
            coef[pl.ds(x * SIDE + 8 * c, 8), :] = shrunk
            square, size = cells * cells, jnp.abs(shrunk)
            squares[depth] = square if squares[depth] is None else squares[depth] + square
            sizes[depth] = size if sizes[depth] is None else sizes[depth] + size
        for sums, target in ((squares, energy), (sizes, kept)):
            for level in range(NEAR):
                deeper = functools.reduce(lambda a, b: a + b, sums[level + 1 :])
                part = jnp.where(rest[level], sums[level], 0.0) + jnp.where(own[level], deeper, 0.0)
                target[level] = target[level] + part

    lane8 = lanes_of(8)
    corners = [v[pl.ds(a * 16 * PITCH + b * 16, 1), :] for a in range(2) for b in range(2)]
    block = jnp.zeros((8, LANES), F32)
    for i, corner in enumerate(corners):
        block = jnp.where(row8 == i, corner, block)
    source, target = rows_of(LANES), lanes_of(LANES)
    pick = jnp.where((source == 16 * (target % 8)) & (target < 32), 1.0, 0.0).astype(F32)
    block = jnp.where(lane8 // 8 == row8, dot(block, pick), 0.0)
    for i, part in enumerate(energy + kept):
        block = jnp.where((lane8 == 32 + i) & (row8 == 0), jnp.sum(part), block)
    send[...] = jnp.broadcast_to(jnp.sum(block, axis=0, keepdims=True), send.shape)


def last_kernel(got, spot, coef, th, out, stats, grid, *, sizes, counts):
    nx, ny, nz = sizes
    plane = ny * nz
    lane, row = lanes_of(plane), rows_of(plane)
    turn = pl.program_id(0)

    @pl.when(turn == 0)
    def _():
        v = [got[pl.ds(i * plane, plane), :] for i in range(nx)]
        sums = functools.reduce(lambda a, b: a + b, v)
        sums = jnp.sum(sums, axis=0, keepdims=True)

        def down(a, shift):
            return pltpu.roll(a, shift % plane, 0)

        odd = (lane & 16) != 0
        d = [v[i] - 0.5 * roll(v[i] + v[(i + 1) % nx], 16) for i in range(nx)]
        v = [jnp.where(odd, d[i], v[i] + 0.25 * roll(d[i] + d[i - 1], -16)) for i in range(nx)]
        odd = (lane & 8) != 0
        d = [a - 0.5 * roll(a + down(a, -nz), 8) for a in v]
        v = [jnp.where(odd, b, a + 0.25 * roll(b + down(b, nz), -8)) for a, b in zip(v, d)]
        odd = (lane & 1) != 0
        top, low = (lane & 7) == 7, (lane & 7) == 0
        far = row % nz == nz - 1
        near = row % nz == 0
        result = []
        for a in v:
            following = jnp.where(far, down(a, nz - 1), down(a, -1))
            d = a - 0.5 * (roll(a, 1) + jnp.where(top, roll(following, 7), roll(a, -1)))
            previous = jnp.where(near, down(d, 1 - nz), down(d, 1))
            s = a + 0.25 * (jnp.where(low, roll(previous, -7), roll(d, 1)) + roll(d, -1))
            result.append(jnp.where(odd, d, s))
        bound = th[pl.ds(LEVELS - 1, 1), :]
        detail = (lane < 32) & ((lane & 25) != 0)
        energy = kept = None
        for i, a in enumerate(result):
            shrunk = a - jnp.minimum(jnp.maximum(a, -bound), bound)
            grid[pl.ds(i * plane, plane), :] = jnp.where(detail, shrunk, a)
            square, size = jnp.where(detail, a * a, 0.0), jnp.where(detail, jnp.abs(shrunk), 0.0)
            energy = square if energy is None else energy + square
            kept = size if kept is None else kept + size
        lane1 = lanes_of(1)
        for i, (part, base) in enumerate(((energy, 32), (kept, 36))):
            totals = jnp.where(lane1 == NEAR, jnp.sum(part), roll(sums, -base))
            scale = jnp.zeros((1, LANES), F32)
            for level in range(LEVELS):
                scale = jnp.where(lane1 == level, 1.0 / counts[level], scale)
            stats[i] = (totals * scale)[:, :LEVELS]

    own = grid[pl.ds(spot[0], 1), :]
    row8, lane8 = rows_of(8), lanes_of(8)
    block = jnp.where((lane8 < 32) & (lane8 // 8 == 2 * turn + row8) & (row8 < 2), own, 0.0)
    source, target = rows_of(LANES), lanes_of(LANES)
    pick = jnp.where((target == 16 * (source % 8)) & (source < 32), 1.0, 0.0).astype(F32)
    block = dot(block, pick)
    out[...] = coef[...]
    start = (lane8[:1] % 16) == 0
    for b in range(2):
        at = pl.ds(16 * b, 1)
        out[at, :] = jnp.where(start, block[b : b + 1, :], coef[at, :])


def shape(*dims):
    return jax.ShapeDtypeStruct(dims, F32)


def shards(fields, exponents):
    sizes = tuple(lax.axis_size(a) for a in ("gx", "gy", "gz"))
    devices = sizes[0] * sizes[1] * sizes[2]
    cells = fields.size * devices
    counts = [7.0 * cells / 8 ** (level + 1) for level in range(LEVELS)]
    f = fields.reshape(SIDE * SIDE, LANES)
    th = jnp.broadcast_to(jnp.pad(jnp.exp2(exponents.astype(F32)), (0, 3))[:, None], (8, LANES))
    tables = jnp.asarray(constant_tables())
    wy = jnp.asarray(W.astype(np.float32))

    def swap(up, down, axis):
        n = lax.axis_size(axis)
        before = lax.ppermute(up, axis, [(i, (i + 1) % n) for i in range(n)])
        after = lax.ppermute(down, axis, [((i + 1) % n, i) for i in range(n)])
        return before, after

    here = pl.BlockSpec(memory_space=pltpu.VMEM)

    def pinned(a):
        return pltpu.with_memory_space_constraint(a, pltpu.VMEM)

    def local(kernel, name, outs, *args, scalars=(), scratch=(), aliases={}):
        args = [pinned(a) for a in args]
        return pl.pallas_call(
            kernel,
            in_specs=[pl.BlockSpec(memory_space=pltpu.SMEM)] * len(scalars) + [here] * len(args),
            out_specs=[here] * len(outs),
            out_shape=[pltpu.VMEM((rows, LANES), F32) for rows in outs],
            scratch_shapes=[pltpu.VMEM((rows, LANES), F32) for rows in scratch],
            input_output_aliases=aliases,
            compiler_params=pltpu.CompilerParams(vmem_limit_bytes=8 << 20),
            name=name,
        )(*scalars, *args)

    spot = lax.axis_index(("gx", "gy", "gz")).astype(jnp.int32).reshape(1)
    whole = lambda *dims: pl.BlockSpec(dims, lambda i: (0,) * len(dims))
    pz = pl.pallas_call(
        ends_kernel,
        grid=(4,),
        in_specs=[pl.BlockSpec((SIDE * SIDE // 4, LANES), lambda i: (i, 0)), whole(LANES, LANES)],
        out_specs=here,
        out_shape=pltpu.VMEM((2 * SIDE, LANES), F32),
        name="ends",
    )(f, tables[0])
    before, after = swap(pz, pz, "gz")
    fx, fy = local(faces_kernel, "faces", (EXT * SIDE, EXT * SIDE), f)
    message = (NEAR + 1) * SIDE
    ez, up, down = local(
        depth_kernel, "depth", (2 * SIDE, message, message), pz, before, after, fx, tables
    )
    before, after = swap(up, down, "gx")
    message = NEAR * PITCH + 3 * EXT
    xe, xee, yup, ydown = local(
        width_kernel, "width", (EXT * SIDE, SIDE, message, message), up, down, before, after, fy, ez, wy, tables
    )
    before, after = swap(yup, ydown, "gy")
    block = PITCH * PITCH
    v, qa, qb = local(prepare_kernel, "prepare", (block,) * 3, f, ez, xe, xee, tables)
    coef, send, *_ = local(
        levels_kernel,
        "levels",
        (SIDE * SIDE, devices, block, block, block),
        *(yup, ydown, before, after, th, tables, v, qa, qb),
        scalars=(spot,),
        scratch=(block,),
        aliases={7: 2, 8: 3, 9: 4},
    )
    send, spot, th = lax.optimization_barrier((send, spot, th))
    got = lax.all_to_all(send.reshape(devices, 1, LANES), ("gx", "gy", "gz"), 0, 0).reshape(devices, LANES)
    out, stats = pl.pallas_call(
        functools.partial(last_kernel, sizes=sizes, counts=counts),
        grid=(2,),
        in_specs=[
            here,
            pl.BlockSpec(memory_space=pltpu.SMEM),
            pl.BlockSpec((SIDE, LANES), lambda i: (16 * i, 0)),
            here,
        ],
        out_specs=[pl.BlockSpec((SIDE, LANES), lambda i: (16 * i, 0)), whole(2, 1, LEVELS)],
        out_shape=(shape(SIDE * SIDE, LANES), shape(2, 1, LEVELS)),
        scratch_shapes=[pltpu.VMEM((devices, LANES), F32)],
        input_output_aliases={2: 0},
        name="last",
    )(pinned(got), spot, coef, pinned(th))
    return out.reshape(fields.shape), stats


def solution(mesh):
    placed = (P(None, "gx", "gy", "gz"), P())
    return jax.shard_map(shards, mesh=mesh, in_specs=placed, out_specs=placed, check_vma=False)
```

```python
import functools

import jax
import jax.numpy as jnp
import numpy as np
from jax import lax
from jax.experimental import pallas as pl
from jax.experimental.pallas import tpu as pltpu
from jax.sharding import PartitionSpec as P

NEAR = 4
LEVELS = 5
LANES = 128
SIDE = 32
EXT = 2 * NEAR
PITCH = SIDE + EXT
F32 = jnp.float32


def cascade(cells, ahead, behind):
    details, firsts = [], []
    for level in range(NEAR):
        half = len(cells) // 2
        following = cells[2::2] + [ahead[level]]
        detail = [cells[2 * k + 1] - 0.5 * (cells[2 * k] + following[k]) for k in range(half)]
        details.append(detail[-1])
        firsts.append(cells[0])
        before = [behind[level]] + detail[:-1]
        cells = [cells[2 * k] + 0.25 * (before[k] + detail[k]) for k in range(half)]
    return details, firsts


def end_weights(length):
    none = [np.zeros(length)] * NEAR
    details, firsts = cascade(list(np.eye(length)), none, none)
    return np.stack(details + firsts)


def seam_weights():
    zero = [np.zeros(1)] * NEAR
    flat = [np.zeros(1)] * SIDE
    alpha = np.zeros((NEAR, NEAR))
    beta = np.zeros((NEAR, NEAR))
    for j in range(NEAR):
        unit = [np.ones(1) * (k == j) for k in range(NEAR)]
        alpha[:, j] = [d[0] for d in cascade(flat, unit, zero)[0]]
        beta[:, j] = [f[0] for f in cascade(flat, zero, unit)[1]]
    lasts, firsts = [], []
    for level in range(NEAR):
        first = np.eye(EXT)[NEAR + level]
        for j in range(level):
            first = first + beta[level, j] * lasts[j]
        firsts.append(first)
        last = np.eye(EXT)[level]
        for j in range(level + 1):
            last = last + alpha[level, j] * firsts[j]
        lasts.append(last)
    return np.stack(lasts), np.stack(firsts)


W = end_weights(SIDE)
WZ = end_weights(LANES)
LAST, FIRST = seam_weights()
GROUP = LANES // EXT


def constant_tables():
    left = np.zeros((EXT, EXT))
    right = np.zeros((EXT, EXT))
    left[:, :NEAR] = LAST.T
    right[:, NEAR:] = FIRST.T
    spread = np.zeros((2, EXT, EXT))
    for level in range(NEAR):
        spread[0, level, EXT - (1 << level)] = 1.0
        spread[1, NEAR + level, EXT - (1 << level)] = 1.0
    each = np.eye(GROUP)
    solve = [np.kron(each, left), np.kron(each, right)]
    corner = np.zeros((2, LANES, LANES))
    corner[:, : EXT * EXT, : EXT * EXT] = [np.kron(left, np.eye(EXT)), np.kron(right, np.eye(EXT))]
    ends = []
    for half in range(2):
        end = np.zeros((LANES, LANES))
        end[:, : EXT * EXT] = np.kron(W[:, half * GROUP : (half + 1) * GROUP].T, np.eye(EXT))
        ends += [side @ end for side in solve]
    tables = np.concatenate(solve + ends + list(corner) + [np.kron(each, part) for part in spread])
    return np.tile(WZ.T, (1, GROUP)).astype(np.float32), tables.astype(np.float32)


SOLVE, ENDS, CORNER, SPREAD = (pl.ds(LANES * i, LANES * n) for i, n in ((0, 2), (2, 4), (6, 2), (8, 2)))


def dot(a, b):
    return jnp.dot(a, b, precision=lax.Precision.HIGHEST, preferred_element_type=F32)


def lanes_of(rows):
    return lax.broadcasted_iota(jnp.int32, (rows, LANES), 1)


def rows_of(rows):
    return lax.broadcasted_iota(jnp.int32, (rows, LANES), 0)


def roll(v, shift):
    return pltpu.roll(v, shift % LANES, 1)


def weighted(rows, load):
    sums = [None] * EXT
    for i in range(SIDE):
        block = load(i)
        for g in range(EXT):
            if W[g, i] != 0.0:
                term = float(W[g, i]) * block
                sums[g] = term if sums[g] is None else sums[g] + term
    return sums


def mix(weights, blocks):
    total = None
    for w, block in zip(weights, blocks):
        if w != 0.0:
            term = float(w) * block
            total = term if total is None else total + term
    return total


def ends_kernel(f, table, pz):
    out = dot(f[...], table[...])
    group = lanes_of(SIDE) // EXT
    for half in range(2):
        packed = jnp.zeros((SIDE, LANES), F32)
        for j in range(GROUP):
            first = (half * GROUP + j) * SIDE
            packed = jnp.where(group == j, out[first : first + SIDE], packed)
        pz[pl.ds(half * SIDE, SIDE), :] = packed


def faces_kernel(f, fx, fy):
    for c in range(SIDE // 8):
        for g, block in enumerate(weighted(8, lambda x: f[pl.ds(x * SIDE + 8 * c, 8), :])):
            fx[pl.ds(g * SIDE + 8 * c, 8), :] = block
    for c in range(SIDE // 8):
        for g, block in enumerate(weighted(8, lambda y: f[pl.ds(8 * c * SIDE + y, 8, stride=SIDE), :])):
            fy[pl.ds(g * SIDE + 8 * c, 8), :] = block


def depth_kernel(pz, before, after, fx, tables, ez, up, down):
    near = lanes_of(2 * SIDE) % EXT < NEAR
    own = pz[...]
    sides = jnp.concatenate([jnp.where(near, before[...], own), jnp.where(near, own, after[...])], axis=1)
    fxe = dot(jnp.concatenate([sides[:SIDE], sides[SIDE:]], axis=1), tables[ENDS, :])
    ez[...] = dot(sides, tables[SOLVE, :])
    for g in range(NEAR):
        up[pl.ds(g * SIDE, SIDE), :] = fx[pl.ds(g * SIDE, SIDE), :]
        down[pl.ds(g * SIDE, SIDE), :] = fx[pl.ds((NEAR + g) * SIDE, SIDE), :]
    up[pl.ds(NEAR * SIDE, SIDE), :] = fxe
    down[pl.ds(NEAR * SIDE, SIDE), :] = fxe


def width_kernel(up, down, before, after, fy, ez, wy, tables, xe, xee, yup, ydown):
    for c in range(SIDE // 8):
        rows = [pl.ds(g * SIDE + 8 * c, 8) for g in range(NEAR)]
        own_last = [up[r, :] for r in rows]
        own_first = [down[r, :] for r in rows]
        seam_before = [before[r, :] for r in rows] + own_first
        seam_after = own_last + [after[r, :] for r in rows]
        for level in range(NEAR):
            xe[pl.ds(level * SIDE + 8 * c, 8), :] = mix(LAST[level], seam_before)
            xe[pl.ds((NEAR + level) * SIDE + 8 * c, 8), :] = mix(FIRST[level], seam_after)
    near = lanes_of(SIDE) // EXT < NEAR
    rows = pl.ds(NEAR * SIDE, SIDE)
    own = up[rows, :]
    sides = [jnp.where(near, before[rows, :], own), jnp.where(near, own, after[rows, :])]
    corner = dot(jnp.concatenate(sides, axis=1), tables[CORNER, :])
    xee[...] = corner
    sums = weighted(EXT, lambda y: xe[pl.ds(y, EXT, stride=SIDE), :])
    for g in range(EXT):
        target = yup if g < NEAR else ydown
        base = (g % NEAR) * PITCH
        target[pl.ds(base, SIDE), :] = fy[pl.ds(g * SIDE, SIDE), :]
        target[pl.ds(base + SIDE, EXT), :] = sums[g]
    for i, block in enumerate((ez[pl.ds(0, SIDE), :], ez[pl.ds(SIDE, SIDE), :], corner)):
        part = dot(wy[...], block)
        yup[pl.ds(NEAR * PITCH + i * EXT, EXT), :] = part
        ydown[pl.ds(NEAR * PITCH + i * EXT, EXT), :] = part


def lift_chunk(ref, at, level, masked):
    step = 1 << level
    pairs = SIDE // (2 * step)
    masked = masked and level > 0
    behind = ref[at(SIDE + level), :]
    even = ref[at(0), :]
    for k in range(pairs):
        odd = ref[at(step * (2 * k + 1)), :]
        ahead = ref[at(step * (2 * k + 2)), :] if k < pairs - 1 else ref[at(SIDE + NEAR + level), :]
        detail = odd - 0.5 * (even + ahead)
        smooth = even + 0.25 * (behind + detail)
        if masked:
            live = (lanes_of(odd.shape[0]) & (step - 1)) == 0
            detail, smooth = jnp.where(live, detail, odd), jnp.where(live, smooth, even)
        ref[at(step * (2 * k + 1)), :] = detail
        ref[at(2 * step * k), :] = smooth
        behind, even = detail, ahead


def chunks(level):
    step = 1 << level
    count = SIDE // step
    own = [(8 * step * c, min(8, count), step) for c in range(max(1, count // 8))]
    return own + ([(SIDE, EXT, 1)] if level < NEAR else [])


def lift_lanes(level, go, v, qa, qb, d, pieces):
    step = 1 << level
    rows = [
        (pl.ds(x * PITCH + first, count, stride=stride), count)
        for x in list(range(0, SIDE, step)) + (list(range(SIDE, PITCH)) if level < NEAR - 1 else [])
        for first, count, stride in pieces
    ]

    @pl.when(go)
    def _():
        for at, count in rows:
            cells = v[at, :]
            odd = roll(cells, -step)
            ahead = roll(jnp.where(lanes_of(count) == LANES - step, qb[at, :], odd), -step)
            d[at, :] = odd - 0.5 * (cells + ahead)

    @pl.when(go)
    def _():
        for at, count in rows:
            lane = lanes_of(count)
            cells, mid = v[at, :], d[at, :]
            odd = roll(mid, step)
            behind = roll(jnp.where(lane == LANES - step, qa[at, :], odd), step)
            even = cells + 0.25 * (mid + behind)
            place = lane & (2 * step - 1)
            v[at, :] = jnp.where(place == 0, even, jnp.where(place == step, odd, cells))


def lift_width(ref, level, masked, pieces):
    for first, count, stride in pieces:
        lift_chunk(ref, lambda i: pl.ds(i * PITCH + first, count, stride=stride), level, masked)


def prepare_kernel(spot, f, ez, xe, xee, tables, v, qa, qb, d):
    for x in range(SIDE):
        v[pl.ds(x * PITCH, SIDE), :] = f[pl.ds(x * SIDE, SIDE), :]
    for g in range(EXT):
        v[pl.ds((SIDE + g) * PITCH, SIDE), :] = xe[pl.ds(g * SIDE, SIDE), :]
    block = jnp.concatenate([ez[...], xee[...]], axis=0)
    for ref, k in ((qa, 0), (qb, 1)):
        spread_lanes(ref, 0, SIDE, block, tables, k)
    for ref in (v, qa, qb):
        lift_width(ref, 0, False, chunks(0)[:-1])
        for first, count, stride in chunks(0):

            def at(i):
                return pl.ds(first * PITCH + i, count, stride=stride * PITCH)

            even, behind = ref[at(0), :], None
            for k in range(SIDE // 2 - 1):
                ahead = ref[at(2 * k + 2), :]
                detail = ref[at(2 * k + 1), :] - 0.5 * (even + ahead)
                ref[at(2 * k + 1), :] = detail
                if k > 0:
                    ref[at(2 * k), :] = even + 0.25 * (behind + detail)
                even, behind = ahead, detail
    lift_lanes(0, spot[0] >= 0, v, qa, qb, d, chunks(0)[1:3])


def spread_lanes(ref, first, rows, block, tables, k):
    part = dot(block, tables[SPREAD, :][LANES * k : LANES * (k + 1)])
    for x in range(PITCH):
        group, j = x // GROUP, x % GROUP
        cells = part[group * rows : (group + 1) * rows]
        ref[pl.ds(x * PITCH + first, rows), :] = roll(cells, -EXT * (j + 1))


def close_height(ref):
    for first, count, stride in chunks(0):

        def at(i):
            return pl.ds(first * PITCH + i, count, stride=stride * PITCH)

        last, end = ref[at(SIDE - 2), :], ref[at(SIDE - 1), :]
        end = end - 0.5 * (last + ref[at(SIDE + NEAR), :])
        ref[at(SIDE - 1), :] = end
        ref[at(SIDE - 2), :] = last + 0.25 * (ref[at(SIDE - 3), :] + end)
        ref[at(0), :] = ref[at(0), :] + 0.25 * (ref[at(SIDE), :] + ref[at(1), :])


def levels_kernel(
    spot, yup, ydown, before, after, th, tables, v_in, qa_in, qb_in, coef, send, v, qa, qb, d
):
    del v_in, qa_in, qb_in
    go = spot[0] >= 0
    for c in range(PITCH // 8):
        rows = [pl.ds(g * PITCH + 8 * c, 8) for g in range(NEAR)]
        seam_before = [before[r, :] for r in rows] + [ydown[r, :] for r in rows]
        seam_after = [yup[r, :] for r in rows] + [after[r, :] for r in rows]
        for level in range(NEAR):
            v[pl.ds(8 * c * PITCH + SIDE + level, 8, stride=PITCH), :] = mix(LAST[level], seam_before)
            v[pl.ds(8 * c * PITCH + SIDE + NEAR + level, 8, stride=PITCH), :] = mix(FIRST[level], seam_after)
    row8 = rows_of(EXT)
    extras = []
    for i in range(3):
        first = NEAR * PITCH + i * EXT
        own = [yup[pl.ds(first + j, 1), :] for j in range(EXT)]
        seam_before = [before[pl.ds(first + j, 1), :] for j in range(NEAR)] + own[NEAR:]
        seam_after = own[:NEAR] + [after[pl.ds(first + NEAR + j, 1), :] for j in range(NEAR)]
        extra = jnp.zeros((EXT, LANES), F32)
        for level in range(NEAR):
            extra = jnp.where(row8 == level, mix(LAST[level], seam_before), extra)
            extra = jnp.where(row8 == NEAR + level, mix(FIRST[level], seam_after), extra)
        extras.append(extra)
    block = jnp.concatenate(extras, axis=0)
    for ref, k in ((qa, 0), (qb, 1)):
        spread_lanes(ref, SIDE, EXT, block, tables, k)

    for level in range(NEAR):
        pieces = chunks(level)
        for ref in (v, qa, qb):
            lift_width(ref, level, ref is v, pieces[-1:] if level == 0 else pieces)
            if level == 0:
                close_height(ref)
                continue
            for first, count, stride in pieces:
                lift_chunk(
                    ref,
                    lambda i: pl.ds(first * PITCH + i, count, stride=stride * PITCH),
                    level,
                    ref is v,
                )
        if level == 0:
            pieces = pieces[:1] + pieces[3:]
        elif level == NEAR - 1:
            pieces = pieces[:-1]
        lift_lanes(level, go, v, qa, qb, d, pieces)

    energy = [jnp.zeros((8, LANES), F32)] * NEAR
    kept = [jnp.zeros((8, LANES), F32)] * NEAR
    for c in range(SIDE // 8):
        bits = (rows_of(8) + 8 * c) | lanes_of(8)
        own = [(bits & ((2 << level) - 1)) == (1 << level) for level in range(NEAR)]
        rest = [(bits & ((1 << level) - 1)) == 0 for level in range(NEAR)]
        bounds = []
        for depth in range(NEAR + 1):
            bound = jnp.broadcast_to(th[pl.ds(min(depth, NEAR - 1), 1), :], (8, LANES))
            for level in range(min(depth, NEAR - 1) - 1, -1, -1):
                bound = jnp.where(own[level], th[pl.ds(level, 1), :], bound)
            bounds.append(bound)
        squares = [None] * (NEAR + 1)
        sizes = [None] * (NEAR + 1)
        for x in range(SIDE):
            depth = NEAR if x == 0 else min(NEAR, (x & -x).bit_length() - 1)
            cells = v[pl.ds(x * PITCH + 8 * c, 8), :]
            shrunk = cells - jnp.minimum(jnp.maximum(cells, -bounds[depth]), bounds[depth])
            coef[pl.ds(x * SIDE + 8 * c, 8), :] = shrunk
            square, size = cells * cells, jnp.abs(shrunk)
            squares[depth] = square if squares[depth] is None else squares[depth] + square
            sizes[depth] = size if sizes[depth] is None else sizes[depth] + size
        for sums, target in ((squares, energy), (sizes, kept)):
            for level in range(NEAR):
                deeper = functools.reduce(lambda a, b: a + b, sums[level + 1 :])
                part = jnp.where(rest[level], sums[level], 0.0) + jnp.where(own[level], deeper, 0.0)
                target[level] = target[level] + part

    lane8 = lanes_of(8)
    corners = [v[pl.ds(a * 16 * PITCH + b * 16, 1), :] for a in range(2) for b in range(2)]
    block = jnp.zeros((8, LANES), F32)
    for i, corner in enumerate(corners):
        block = jnp.where(row8 == i, corner, block)
    source, target = rows_of(LANES), lanes_of(LANES)
    pick = jnp.where((source == 16 * (target % 8)) & (target < 32), 1.0, 0.0).astype(F32)
    block = jnp.where(lane8 // 8 == row8, dot(block, pick), 0.0)
    for i, part in enumerate(energy + kept):
        block = jnp.where((lane8 == 32 + i) & (row8 == 0), jnp.sum(part), block)
    send[...] = jnp.broadcast_to(jnp.sum(block, axis=0, keepdims=True), send.shape)


def last_kernel(spot, got, coef, th, out, stats, grid, *, sizes, counts):
    nx, ny, nz = sizes
    plane = ny * nz
    lane, row = lanes_of(plane), rows_of(plane)
    v = [got[pl.ds(i * plane, plane), :] for i in range(nx)]
    sums = functools.reduce(lambda a, b: a + b, v)
    sums = jnp.sum(sums, axis=0, keepdims=True)

    def down(a, shift):
        return pltpu.roll(a, shift % plane, 0)

    odd = (lane & 16) != 0
    d = [v[i] - 0.5 * roll(v[i] + v[(i + 1) % nx], 16) for i in range(nx)]
    v = [jnp.where(odd, d[i], v[i] + 0.25 * roll(d[i] + d[i - 1], -16)) for i in range(nx)]
    odd = (lane & 8) != 0
    d = [a - 0.5 * roll(a + down(a, -nz), 8) for a in v]
    v = [jnp.where(odd, b, a + 0.25 * roll(b + down(b, nz), -8)) for a, b in zip(v, d)]
    odd = (lane & 1) != 0
    top, low = (lane & 7) == 7, (lane & 7) == 0
    far = row % nz == nz - 1
    near = row % nz == 0
    result = []
    for a in v:
        following = jnp.where(far, down(a, nz - 1), down(a, -1))
        d = a - 0.5 * (roll(a, 1) + jnp.where(top, roll(following, 7), roll(a, -1)))
        previous = jnp.where(near, down(d, 1 - nz), down(d, 1))
        s = a + 0.25 * (jnp.where(low, roll(previous, -7), roll(d, 1)) + roll(d, -1))
        result.append(jnp.where(odd, d, s))
    bound = th[pl.ds(LEVELS - 1, 1), :]
    detail = (lane < 32) & ((lane & 25) != 0)
    energy = kept = None
    for i, a in enumerate(result):
        shrunk = a - jnp.minimum(jnp.maximum(a, -bound), bound)
        grid[pl.ds(i * plane, plane), :] = jnp.where(detail, shrunk, a)
        square, size = jnp.where(detail, a * a, 0.0), jnp.where(detail, jnp.abs(shrunk), 0.0)
        energy = square if energy is None else energy + square
        kept = size if kept is None else kept + size
    lane1 = lanes_of(1)
    for i, (part, base) in enumerate(((energy, 32), (kept, 36))):
        totals = jnp.where(lane1 == NEAR, jnp.sum(part), roll(sums, -base))
        scale = jnp.zeros((1, LANES), F32)
        for level in range(LEVELS):
            scale = jnp.where(lane1 == level, 1.0 / counts[level], scale)
        stats[i] = (totals * scale)[:, :LEVELS]

    own = grid[pl.ds(spot[0], 1), :]
    row8, lane8 = rows_of(8), lanes_of(8)
    block = jnp.where((lane8 < 32) & (lane8 // 8 == row8), own, 0.0)
    source, target = rows_of(LANES), lanes_of(LANES)
    pick = jnp.where((target == 16 * (source % 8)) & (source < 32), 1.0, 0.0).astype(F32)
    block = dot(block, pick)
    start = (lane8[:1] % 16) == 0
    for i in range(4):
        at = pl.ds((i // 2 * SIDE + i % 2) * 16, 1)
        out[at, :] = jnp.where(start, block[i : i + 1, :], coef[at, :])


def shape(*dims):
    return jax.ShapeDtypeStruct(dims, F32)


def shards(fields, exponents):
    sizes = tuple(lax.axis_size(a) for a in ("gx", "gy", "gz"))
    devices = sizes[0] * sizes[1] * sizes[2]
    cells = fields.size * devices
    counts = [7.0 * cells / 8 ** (level + 1) for level in range(LEVELS)]
    f = fields.reshape(SIDE * SIDE, LANES)
    th = jnp.broadcast_to(jnp.pad(jnp.exp2(exponents.astype(F32)), (0, 3))[:, None], (8, LANES))
    table, tables = (jnp.asarray(t) for t in constant_tables())
    wy = jnp.asarray(W.astype(np.float32))

    def swap(up, down, axis):
        n = lax.axis_size(axis)
        before = lax.ppermute(up, axis, [(i, (i + 1) % n) for i in range(n)])
        after = lax.ppermute(down, axis, [((i + 1) % n, i) for i in range(n)])
        return before, after

    here = pl.BlockSpec(memory_space=pltpu.VMEM)

    def pinned(a):
        return pltpu.with_memory_space_constraint(a, pltpu.VMEM)

    def local(kernel, name, outs, *args, scalars=(), scratch=(), aliases={}):
        args = [pinned(a) for a in args]
        return pl.pallas_call(
            kernel,
            in_specs=[pl.BlockSpec(memory_space=pltpu.SMEM)] * len(scalars) + [here] * len(args),
            out_specs=[here] * len(outs),
            out_shape=[pltpu.VMEM((rows, LANES), F32) for rows in outs],
            scratch_shapes=[pltpu.VMEM((rows, LANES), F32) for rows in scratch],
            input_output_aliases=aliases,
            compiler_params=pltpu.CompilerParams(vmem_limit_bytes=8 << 20),
            name=name,
        )(*scalars, *args)

    spot = lax.axis_index(("gx", "gy", "gz")).astype(jnp.int32).reshape(1)
    pz = pl.pallas_call(
        ends_kernel, out_specs=here, out_shape=pltpu.VMEM((2 * SIDE, LANES), F32), name="ends"
    )(f, table)
    before, after = swap(pz, pz, "gz")
    fx, fy = local(faces_kernel, "faces", (EXT * SIDE, EXT * SIDE), f)
    message = (NEAR + 1) * SIDE
    ez, up, down = local(
        depth_kernel, "depth", (2 * SIDE, message, message), pz, before, after, fx, tables
    )
    before, after = swap(up, down, "gx")
    message = NEAR * PITCH + 3 * EXT
    xe, xee, yup, ydown = local(
        width_kernel, "width", (EXT * SIDE, SIDE, message, message), up, down, before, after, fy, ez, wy, tables
    )
    before, after = swap(yup, ydown, "gy")
    block = PITCH * PITCH
    v, qa, qb = local(
        prepare_kernel,
        "prepare",
        (block,) * 3,
        *(f, ez, xe, xee, tables),
        scalars=(spot,),
        scratch=(block,),
    )
    coef, send, *_ = local(
        levels_kernel,
        "levels",
        (SIDE * SIDE, devices, block, block, block),
        *(yup, ydown, before, after, th, tables, v, qa, qb),
        scalars=(spot,),
        scratch=(block,),
        aliases={7: 2, 8: 3, 9: 4},
    )
    send, spot, th = lax.optimization_barrier((send, spot, th))
    got = lax.all_to_all(send.reshape(devices, 1, LANES), ("gx", "gy", "gz"), 0, 0).reshape(devices, LANES)
    out, stats = pl.pallas_call(
        functools.partial(last_kernel, sizes=sizes, counts=counts),
        in_specs=[pl.BlockSpec(memory_space=pltpu.SMEM), here, here, here],
        out_specs=[here, here],
        out_shape=(pltpu.VMEM((SIDE * SIDE, LANES), F32), shape(2, 1, LEVELS)),
        scratch_shapes=[pltpu.VMEM((devices, LANES), F32)],
        input_output_aliases={2: 0},
        compiler_params=pltpu.CompilerParams(vmem_limit_bytes=8 << 20),
        name="last",
    )(spot, pinned(got), pinned(coef), pinned(th))
    return out.reshape(fields.shape), stats


def solution(mesh):
    placed = (P(None, "gx", "gy", "gz"), P())
    return jax.shard_map(shards, mesh=mesh, in_specs=placed, out_specs=placed, check_vma=False)
```

```python
import functools

import jax
import jax.numpy as jnp
import numpy as np
from jax import lax
from jax.experimental import pallas as pl
from jax.experimental.pallas import tpu as pltpu
from jax.sharding import PartitionSpec as P

NEAR = 4
LEVELS = 5
LANES = 128
SIDE = 32
EXT = 2 * NEAR
PITCH = SIDE + EXT
F32 = jnp.float32


def cascade(cells, ahead, behind):
    details, firsts = [], []
    for level in range(NEAR):
        half = len(cells) // 2
        following = cells[2::2] + [ahead[level]]
        detail = [cells[2 * k + 1] - 0.5 * (cells[2 * k] + following[k]) for k in range(half)]
        details.append(detail[-1])
        firsts.append(cells[0])
        before = [behind[level]] + detail[:-1]
        cells = [cells[2 * k] + 0.25 * (before[k] + detail[k]) for k in range(half)]
    return details, firsts


def end_weights(length):
    none = [np.zeros(length)] * NEAR
    details, firsts = cascade(list(np.eye(length)), none, none)
    return np.stack(details + firsts)


def seam_weights():
    zero = [np.zeros(1)] * NEAR
    flat = [np.zeros(1)] * SIDE
    alpha = np.zeros((NEAR, NEAR))
    beta = np.zeros((NEAR, NEAR))
    for j in range(NEAR):
        unit = [np.ones(1) * (k == j) for k in range(NEAR)]
        alpha[:, j] = [d[0] for d in cascade(flat, unit, zero)[0]]
        beta[:, j] = [f[0] for f in cascade(flat, zero, unit)[1]]
    lasts, firsts = [], []
    for level in range(NEAR):
        first = np.eye(EXT)[NEAR + level]
        for j in range(level):
            first = first + beta[level, j] * lasts[j]
        firsts.append(first)
        last = np.eye(EXT)[level]
        for j in range(level + 1):
            last = last + alpha[level, j] * firsts[j]
        lasts.append(last)
    return np.stack(lasts), np.stack(firsts)


W = end_weights(SIDE)
WZ = end_weights(LANES)
LAST, FIRST = seam_weights()
GROUP = LANES // EXT


def constant_tables():
    left = np.zeros((EXT, EXT))
    right = np.zeros((EXT, EXT))
    left[:, :NEAR] = LAST.T
    right[:, NEAR:] = FIRST.T
    spread = np.zeros((2, EXT, EXT))
    for level in range(NEAR):
        spread[0, level, EXT - (1 << level)] = 1.0
        spread[1, NEAR + level, EXT - (1 << level)] = 1.0
    each = np.eye(GROUP)
    solve = [np.kron(each, left), np.kron(each, right)]
    corner = np.zeros((2, LANES, LANES))
    corner[:, : EXT * EXT, : EXT * EXT] = [np.kron(left, np.eye(EXT)), np.kron(right, np.eye(EXT))]
    ends = []
    for half in range(2):
        end = np.zeros((LANES, LANES))
        end[:, : EXT * EXT] = np.kron(W[:, half * GROUP : (half + 1) * GROUP].T, np.eye(EXT))
        ends += [side @ end for side in solve]
    tables = np.concatenate(solve + ends + list(corner) + [np.kron(each, part) for part in spread])
    return np.tile(WZ.T, (1, GROUP)).astype(np.float32), tables.astype(np.float32)


SOLVE, ENDS, CORNER, SPREAD = (pl.ds(LANES * i, LANES * n) for i, n in ((0, 2), (2, 4), (6, 2), (8, 2)))


def dot(a, b):
    return jnp.dot(a, b, precision=lax.Precision.HIGHEST, preferred_element_type=F32)


def lanes_of(rows):
    return lax.broadcasted_iota(jnp.int32, (rows, LANES), 1)


def rows_of(rows):
    return lax.broadcasted_iota(jnp.int32, (rows, LANES), 0)


def roll(v, shift):
    return pltpu.roll(v, shift % LANES, 1)


def weighted(rows, load):
    sums = [None] * EXT
    for i in range(SIDE):
        block = load(i)
        for g in range(EXT):
            if W[g, i] != 0.0:
                term = float(W[g, i]) * block
                sums[g] = term if sums[g] is None else sums[g] + term
    return sums


def mix(weights, blocks):
    total = None
    for w, block in zip(weights, blocks):
        if w != 0.0:
            term = float(w) * block
            total = term if total is None else total + term
    return total


def ends_kernel(f, table, pz):
    out = dot(f[...], table[...])
    group = lanes_of(SIDE) // EXT
    for half in range(2):
        packed = jnp.zeros((SIDE, LANES), F32)
        for j in range(GROUP):
            first = (half * GROUP + j) * SIDE
            packed = jnp.where(group == j, out[first : first + SIDE], packed)
        pz[pl.ds(half * SIDE, SIDE), :] = packed


def faces_kernel(f, fx, fy):
    for c in range(SIDE // 8):
        for g, block in enumerate(weighted(8, lambda x: f[pl.ds(x * SIDE + 8 * c, 8), :])):
            fx[pl.ds(g * SIDE + 8 * c, 8), :] = block
    for c in range(SIDE // 8):
        for g, block in enumerate(weighted(8, lambda y: f[pl.ds(8 * c * SIDE + y, 8, stride=SIDE), :])):
            fy[pl.ds(g * SIDE + 8 * c, 8), :] = block


def depth_kernel(pz, before, after, fx, tables, ez, up, down):
    near = lanes_of(2 * SIDE) % EXT < NEAR
    own = pz[...]
    sides = jnp.concatenate([jnp.where(near, before[...], own), jnp.where(near, own, after[...])], axis=1)
    fxe = dot(jnp.concatenate([sides[:SIDE], sides[SIDE:]], axis=1), tables[ENDS, :])
    ez[...] = dot(sides, tables[SOLVE, :])
    for g in range(NEAR):
        up[pl.ds(g * SIDE, SIDE), :] = fx[pl.ds(g * SIDE, SIDE), :]
        down[pl.ds(g * SIDE, SIDE), :] = fx[pl.ds((NEAR + g) * SIDE, SIDE), :]
    up[pl.ds(NEAR * SIDE, SIDE), :] = fxe
    down[pl.ds(NEAR * SIDE, SIDE), :] = fxe


def width_kernel(up, down, before, after, fy, ez, wy, tables, xe, xee, yup, ydown):
    for c in range(SIDE // 8):
        rows = [pl.ds(g * SIDE + 8 * c, 8) for g in range(NEAR)]
        own_last = [up[r, :] for r in rows]
        own_first = [down[r, :] for r in rows]
        seam_before = [before[r, :] for r in rows] + own_first
        seam_after = own_last + [after[r, :] for r in rows]
        for level in range(NEAR):
            xe[pl.ds(level * SIDE + 8 * c, 8), :] = mix(LAST[level], seam_before)
            xe[pl.ds((NEAR + level) * SIDE + 8 * c, 8), :] = mix(FIRST[level], seam_after)
    near = lanes_of(SIDE) // EXT < NEAR
    rows = pl.ds(NEAR * SIDE, SIDE)
    own = up[rows, :]
    sides = [jnp.where(near, before[rows, :], own), jnp.where(near, own, after[rows, :])]
    corner = dot(jnp.concatenate(sides, axis=1), tables[CORNER, :])
    xee[...] = corner
    sums = weighted(EXT, lambda y: xe[pl.ds(y, EXT, stride=SIDE), :])
    for g in range(EXT):
        target = yup if g < NEAR else ydown
        base = (g % NEAR) * PITCH
        target[pl.ds(base, SIDE), :] = fy[pl.ds(g * SIDE, SIDE), :]
        target[pl.ds(base + SIDE, EXT), :] = sums[g]
    for i, block in enumerate((ez[pl.ds(0, SIDE), :], ez[pl.ds(SIDE, SIDE), :], corner)):
        part = dot(wy[...], block)
        yup[pl.ds(NEAR * PITCH + i * EXT, EXT), :] = part
        ydown[pl.ds(NEAR * PITCH + i * EXT, EXT), :] = part


def lift_chunk(ref, at, level, masked):
    step = 1 << level
    pairs = SIDE // (2 * step)
    masked = masked and level > 0
    behind = ref[at(SIDE + level), :]
    even = ref[at(0), :]
    for k in range(pairs):
        odd = ref[at(step * (2 * k + 1)), :]
        ahead = ref[at(step * (2 * k + 2)), :] if k < pairs - 1 else ref[at(SIDE + NEAR + level), :]
        detail = odd - 0.5 * (even + ahead)
        smooth = even + 0.25 * (behind + detail)
        if masked:
            live = (lanes_of(odd.shape[0]) & (step - 1)) == 0
            detail, smooth = jnp.where(live, detail, odd), jnp.where(live, smooth, even)
        ref[at(step * (2 * k + 1)), :] = detail
        ref[at(2 * step * k), :] = smooth
        behind, even = detail, ahead


def chunks(level):
    step = 1 << level
    count = SIDE // step
    own = [(8 * step * c, min(8, count), step) for c in range(max(1, count // 8))]
    return own + ([(SIDE, EXT, 1)] if level < NEAR else [])


def lift_lanes(level, spot, v, qa, qb, d, pieces):
    step = 1 << level
    rows = [
        (pl.ds(x * PITCH + first, count, stride=stride), count)
        for x in list(range(0, SIDE, step)) + (list(range(SIDE, PITCH)) if level < NEAR - 1 else [])
        for first, count, stride in pieces
    ]

    @pl.when(spot[0] > -1)
    def _():
        for at, count in rows:
            cells = v[at, :]
            odd = roll(cells, -step)
            ahead = roll(jnp.where(lanes_of(count) == LANES - step, qb[at, :], odd), -step)
            d[at, :] = odd - 0.5 * (cells + ahead)

    @pl.when(spot[0] > -2)
    def _():
        for at, count in rows:
            lane = lanes_of(count)
            cells, mid = v[at, :], d[at, :]
            odd = roll(mid, step)
            behind = roll(jnp.where(lane == LANES - step, qa[at, :], odd), step)
            even = cells + 0.25 * (mid + behind)
            place = lane & (2 * step - 1)
            v[at, :] = jnp.where(place == 0, even, jnp.where(place == step, odd, cells))


def lift_width(ref, level, masked, pieces):
    for first, count, stride in pieces:
        lift_chunk(ref, lambda i: pl.ds(i * PITCH + first, count, stride=stride), level, masked)


def prepare_kernel(spot, f, ez, xe, xee, tables, v, qa, qb, d):
    for x in range(SIDE):
        v[pl.ds(x * PITCH, SIDE), :] = f[pl.ds(x * SIDE, SIDE), :]
    for g in range(EXT):
        v[pl.ds((SIDE + g) * PITCH, SIDE), :] = xe[pl.ds(g * SIDE, SIDE), :]
    block = jnp.concatenate([ez[...], xee[...]], axis=0)
    for ref, k in ((qa, 0), (qb, 1)):
        spread_lanes(ref, 0, SIDE, block, tables, k)
    for ref in (v, qa, qb):
        lift_width(ref, 0, False, chunks(0)[:-1])
        for first, count, stride in chunks(0):

            def at(i):
                return pl.ds(first * PITCH + i, count, stride=stride * PITCH)

            even, behind = ref[at(0), :], None
            for k in range(SIDE // 2 - 1):
                ahead = ref[at(2 * k + 2), :]
                detail = ref[at(2 * k + 1), :] - 0.5 * (even + ahead)
                ref[at(2 * k + 1), :] = detail
                if k > 0:
                    ref[at(2 * k), :] = even + 0.25 * (behind + detail)
                even, behind = ahead, detail
    lift_lanes(0, spot, v, qa, qb, d, chunks(0)[1:3])


def spread_lanes(ref, first, rows, block, tables, k):
    part = dot(block, tables[SPREAD, :][LANES * k : LANES * (k + 1)])
    for x in range(PITCH):
        group, j = x // GROUP, x % GROUP
        cells = part[group * rows : (group + 1) * rows]
        ref[pl.ds(x * PITCH + first, rows), :] = roll(cells, -EXT * (j + 1))


def close_height(ref):
    for first, count, stride in chunks(0):

        def at(i):
            return pl.ds(first * PITCH + i, count, stride=stride * PITCH)

        last, end = ref[at(SIDE - 2), :], ref[at(SIDE - 1), :]
        end = end - 0.5 * (last + ref[at(SIDE + NEAR), :])
        ref[at(SIDE - 1), :] = end
        ref[at(SIDE - 2), :] = last + 0.25 * (ref[at(SIDE - 3), :] + end)
        ref[at(0), :] = ref[at(0), :] + 0.25 * (ref[at(SIDE), :] + ref[at(1), :])


def levels_kernel(
    spot, yup, ydown, before, after, th, tables, v_in, qa_in, qb_in, coef, send, v, qa, qb, d
):
    del v_in, qa_in, qb_in
    for c in range(PITCH // 8):
        rows = [pl.ds(g * PITCH + 8 * c, 8) for g in range(NEAR)]
        seam_before = [before[r, :] for r in rows] + [ydown[r, :] for r in rows]
        seam_after = [yup[r, :] for r in rows] + [after[r, :] for r in rows]
        for level in range(NEAR):
            v[pl.ds(8 * c * PITCH + SIDE + level, 8, stride=PITCH), :] = mix(LAST[level], seam_before)
            v[pl.ds(8 * c * PITCH + SIDE + NEAR + level, 8, stride=PITCH), :] = mix(FIRST[level], seam_after)
    row8 = rows_of(EXT)
    extras = []
    for i in range(3):
        first = NEAR * PITCH + i * EXT
        own = [yup[pl.ds(first + j, 1), :] for j in range(EXT)]
        seam_before = [before[pl.ds(first + j, 1), :] for j in range(NEAR)] + own[NEAR:]
        seam_after = own[:NEAR] + [after[pl.ds(first + NEAR + j, 1), :] for j in range(NEAR)]
        extra = jnp.zeros((EXT, LANES), F32)
        for level in range(NEAR):
            extra = jnp.where(row8 == level, mix(LAST[level], seam_before), extra)
            extra = jnp.where(row8 == NEAR + level, mix(FIRST[level], seam_after), extra)
        extras.append(extra)
    block = jnp.concatenate(extras, axis=0)
    for ref, k in ((qa, 0), (qb, 1)):
        spread_lanes(ref, SIDE, EXT, block, tables, k)

    for level in range(NEAR):
        pieces = chunks(level)
        for ref in (v, qa, qb):
            lift_width(ref, level, ref is v, pieces[-1:] if level == 0 else pieces)
            if level == 0:
                close_height(ref)
                continue
            for first, count, stride in pieces:
                lift_chunk(
                    ref,
                    lambda i: pl.ds(first * PITCH + i, count, stride=stride * PITCH),
                    level,
                    ref is v,
                )
        if level == 0:
            pieces = pieces[:1] + pieces[3:]
        elif level == NEAR - 1:
            pieces = pieces[:-1]
        lift_lanes(level, spot, v, qa, qb, d, pieces)

    energy = [jnp.zeros((8, LANES), F32)] * NEAR
    kept = [jnp.zeros((8, LANES), F32)] * NEAR
    for c in range(SIDE // 8):
        bits = (rows_of(8) + 8 * c) | lanes_of(8)
        own = [(bits & ((2 << level) - 1)) == (1 << level) for level in range(NEAR)]
        rest = [(bits & ((1 << level) - 1)) == 0 for level in range(NEAR)]
        bounds = []
        for depth in range(NEAR + 1):
            bound = jnp.broadcast_to(th[pl.ds(min(depth, NEAR - 1), 1), :], (8, LANES))
            for level in range(min(depth, NEAR - 1) - 1, -1, -1):
                bound = jnp.where(own[level], th[pl.ds(level, 1), :], bound)
            bounds.append(bound)
        squares = [None] * (NEAR + 1)
        sizes = [None] * (NEAR + 1)
        for x in range(SIDE):
            depth = NEAR if x == 0 else min(NEAR, (x & -x).bit_length() - 1)
            cells = v[pl.ds(x * PITCH + 8 * c, 8), :]
            shrunk = cells - jnp.minimum(jnp.maximum(cells, -bounds[depth]), bounds[depth])
            coef[pl.ds(x * SIDE + 8 * c, 8), :] = shrunk
            square, size = cells * cells, jnp.abs(shrunk)
            squares[depth] = square if squares[depth] is None else squares[depth] + square
            sizes[depth] = size if sizes[depth] is None else sizes[depth] + size
        for sums, target in ((squares, energy), (sizes, kept)):
            for level in range(NEAR):
                deeper = functools.reduce(lambda a, b: a + b, sums[level + 1 :])
                part = jnp.where(rest[level], sums[level], 0.0) + jnp.where(own[level], deeper, 0.0)
                target[level] = target[level] + part

    lane8 = lanes_of(8)
    corners = [v[pl.ds(a * 16 * PITCH + b * 16, 1), :] for a in range(2) for b in range(2)]
    block = jnp.zeros((8, LANES), F32)
    for i, corner in enumerate(corners):
        block = jnp.where(row8 == i, corner, block)
    source, target = rows_of(LANES), lanes_of(LANES)
    pick = jnp.where((source == 16 * (target % 8)) & (target < 32), 1.0, 0.0).astype(F32)
    block = jnp.where(lane8 // 8 == row8, dot(block, pick), 0.0)
    for i, part in enumerate(energy + kept):
        block = jnp.where((lane8 == 32 + i) & (row8 == 0), jnp.sum(part), block)
    send[...] = jnp.broadcast_to(jnp.sum(block, axis=0, keepdims=True), send.shape)


def last_kernel(spot, got, coef, th, out, stats, grid, planes, sums_out, sem, *, sizes, counts):
    half = SIDE // 2
    copies = []
    for a in range(2):
        at = pl.ds((a * half + 1) * SIDE, (half - 1) * SIDE)
        copies.append(pltpu.make_async_copy(coef.at[at], out.at[at], sem.at[a]))
        copies[a].start()
        planes[pl.ds(a * SIDE, SIDE), :] = coef[pl.ds(a * half * SIDE, SIDE), :]
    nx, ny, nz = sizes
    plane = ny * nz
    lane, row = lanes_of(plane), rows_of(plane)
    v = [got[pl.ds(i * plane, plane), :] for i in range(nx)]
    sums = functools.reduce(lambda a, b: a + b, v)
    sums = jnp.sum(sums, axis=0, keepdims=True)

    def down(a, shift):
        return pltpu.roll(a, shift % plane, 0)

    odd = (lane & 16) != 0
    d = [v[i] - 0.5 * roll(v[i] + v[(i + 1) % nx], 16) for i in range(nx)]
    v = [jnp.where(odd, d[i], v[i] + 0.25 * roll(d[i] + d[i - 1], -16)) for i in range(nx)]
    odd = (lane & 8) != 0
    d = [a - 0.5 * roll(a + down(a, -nz), 8) for a in v]
    v = [jnp.where(odd, b, a + 0.25 * roll(b + down(b, nz), -8)) for a, b in zip(v, d)]
    odd = (lane & 1) != 0
    top, low = (lane & 7) == 7, (lane & 7) == 0
    far = row % nz == nz - 1
    near = row % nz == 0
    result = []
    for a in v:
        following = jnp.where(far, down(a, nz - 1), down(a, -1))
        d = a - 0.5 * (roll(a, 1) + jnp.where(top, roll(following, 7), roll(a, -1)))
        previous = jnp.where(near, down(d, 1 - nz), down(d, 1))
        s = a + 0.25 * (jnp.where(low, roll(previous, -7), roll(d, 1)) + roll(d, -1))
        result.append(jnp.where(odd, d, s))
    bound = th[pl.ds(LEVELS - 1, 1), :]
    detail = (lane < 32) & ((lane & 25) != 0)
    energy = kept = None
    for i, a in enumerate(result):
        shrunk = a - jnp.minimum(jnp.maximum(a, -bound), bound)
        grid[pl.ds(i * plane, plane), :] = jnp.where(detail, shrunk, a)
        square, size = jnp.where(detail, a * a, 0.0), jnp.where(detail, jnp.abs(shrunk), 0.0)
        energy = square if energy is None else energy + square
        kept = size if kept is None else kept + size
    lane1 = lanes_of(1)
    for i, (part, base) in enumerate(((energy, 32), (kept, 36))):
        totals = jnp.where(lane1 == NEAR, jnp.sum(part), roll(sums, -base))
        scale = jnp.zeros((1, LANES), F32)
        for level in range(LEVELS):
            scale = jnp.where(lane1 == level, 1.0 / counts[level], scale)
        sums_out[i] = (totals * scale)[:, :LEVELS]

    own = grid[pl.ds(spot[0], 1), :]
    row8, lane8 = rows_of(8), lanes_of(8)
    block = jnp.where((lane8 < 32) & (lane8 // 8 == row8), own, 0.0)
    source, target = rows_of(LANES), lanes_of(LANES)
    pick = jnp.where((target == 16 * (source % 8)) & (source < 32), 1.0, 0.0).astype(F32)
    block = dot(block, pick)
    start = lane8[:1] % 16 == 0
    for i in range(4):
        at = pl.ds(i * half, 1)
        planes[at, :] = jnp.where(start, block[i : i + 1, :], planes[at, :])
    for a in range(2):
        target = out.at[pl.ds(a * half * SIDE, SIDE)]
        copies.append(pltpu.make_async_copy(planes.at[pl.ds(a * SIDE, SIDE)], target, sem.at[2 + a]))
    copies.append(pltpu.make_async_copy(sums_out, stats, sem.at[4]))
    for copy in copies[2:]:
        copy.start()
    for copy in copies:
        copy.wait()


def shape(*dims):
    return jax.ShapeDtypeStruct(dims, F32)


def shards(fields, exponents):
    sizes = tuple(lax.axis_size(a) for a in ("gx", "gy", "gz"))
    devices = sizes[0] * sizes[1] * sizes[2]
    cells = fields.size * devices
    counts = [7.0 * cells / 8 ** (level + 1) for level in range(LEVELS)]
    f = fields.reshape(SIDE * SIDE, LANES)
    th = jnp.broadcast_to(jnp.pad(jnp.exp2(exponents.astype(F32)), (0, 3))[:, None], (8, LANES))
    table, tables = (jnp.asarray(t) for t in constant_tables())
    wy = jnp.asarray(W.astype(np.float32))

    def swap(up, down, axis):
        n = lax.axis_size(axis)
        before = lax.ppermute(up, axis, [(i, (i + 1) % n) for i in range(n)])
        after = lax.ppermute(down, axis, [((i + 1) % n, i) for i in range(n)])
        return before, after

    here = pl.BlockSpec(memory_space=pltpu.VMEM)

    def pinned(a):
        return pltpu.with_memory_space_constraint(a, pltpu.VMEM)

    def local(kernel, name, outs, *args, scalars=(), scratch=(), aliases={}):
        args = [pinned(a) for a in args]
        return pl.pallas_call(
            kernel,
            in_specs=[pl.BlockSpec(memory_space=pltpu.SMEM)] * len(scalars) + [here] * len(args),
            out_specs=[here] * len(outs),
            out_shape=[pltpu.VMEM((rows, LANES), F32) for rows in outs],
            scratch_shapes=[pltpu.VMEM((rows, LANES), F32) for rows in scratch],
            input_output_aliases=aliases,
            compiler_params=pltpu.CompilerParams(vmem_limit_bytes=8 << 20),
            name=name,
        )(*scalars, *args)

    spot = lax.axis_index(("gx", "gy", "gz")).astype(jnp.int32).reshape(1)
    pz = pl.pallas_call(
        ends_kernel, out_specs=here, out_shape=pltpu.VMEM((2 * SIDE, LANES), F32), name="ends"
    )(f, table)
    before, after = swap(pz, pz, "gz")
    fx, fy = local(faces_kernel, "faces", (EXT * SIDE, EXT * SIDE), f)
    message = (NEAR + 1) * SIDE
    ez, up, down = local(
        depth_kernel, "depth", (2 * SIDE, message, message), pz, before, after, fx, tables
    )
    before, after = swap(up, down, "gx")
    message = NEAR * PITCH + 3 * EXT
    xe, xee, yup, ydown = local(
        width_kernel, "width", (EXT * SIDE, SIDE, message, message), up, down, before, after, fy, ez, wy, tables
    )
    before, after = swap(yup, ydown, "gy")
    block = PITCH * PITCH
    v, qa, qb = local(
        prepare_kernel,
        "prepare",
        (block,) * 3,
        *(f, ez, xe, xee, tables),
        scalars=(spot,),
        scratch=(block,),
    )
    coef, send, *_ = local(
        levels_kernel,
        "levels",
        (SIDE * SIDE, devices, block, block, block),
        *(yup, ydown, before, after, th, tables, v, qa, qb),
        scalars=(spot,),
        scratch=(block,),
        aliases={7: 2, 8: 3, 9: 4},
    )
    send, spot, th = lax.optimization_barrier((send, spot, th))
    got = lax.all_to_all(send.reshape(devices, 1, LANES), ("gx", "gy", "gz"), 0, 0).reshape(devices, LANES)
    there = pl.BlockSpec(memory_space=pltpu.HBM)
    out, stats = pl.pallas_call(
        functools.partial(last_kernel, sizes=sizes, counts=counts),
        in_specs=[pl.BlockSpec(memory_space=pltpu.SMEM), here, here, here],
        out_specs=[there, there],
        out_shape=(shape(SIDE * SIDE, LANES), shape(2, 1, LEVELS)),
        scratch_shapes=[
            pltpu.VMEM((devices, LANES), F32),
            pltpu.VMEM((2 * SIDE, LANES), F32),
            pltpu.VMEM((2, 1, LEVELS), F32),
            pltpu.SemaphoreType.DMA((5,)),
        ],
        compiler_params=pltpu.CompilerParams(vmem_limit_bytes=8 << 20),
        name="last",
    )(spot, pinned(got), pinned(coef), pinned(th))
    return out.reshape(fields.shape), stats


def solution(mesh):
    placed = (P(None, "gx", "gy", "gz"), P())
    return jax.shard_map(shards, mesh=mesh, in_specs=placed, out_specs=placed, check_vma=False)
```

```python
import functools

import jax
import jax.numpy as jnp
import numpy as np
from jax import lax
from jax.experimental import pallas as pl
from jax.experimental.pallas import tpu as pltpu
from jax.sharding import PartitionSpec as P

NEAR = 4
LEVELS = 5
LANES = 128
SIDE = 32
EXT = 2 * NEAR
PITCH = SIDE + EXT
F32 = jnp.float32


def cascade(cells, ahead, behind):
    details, firsts = [], []
    for level in range(NEAR):
        half = len(cells) // 2
        following = cells[2::2] + [ahead[level]]
        detail = [cells[2 * k + 1] - 0.5 * (cells[2 * k] + following[k]) for k in range(half)]
        details.append(detail[-1])
        firsts.append(cells[0])
        before = [behind[level]] + detail[:-1]
        cells = [cells[2 * k] + 0.25 * (before[k] + detail[k]) for k in range(half)]
    return details, firsts


def end_weights(length):
    none = [np.zeros(length)] * NEAR
    details, firsts = cascade(list(np.eye(length)), none, none)
    return np.stack(details + firsts)


def seam_weights():
    zero = [np.zeros(1)] * NEAR
    flat = [np.zeros(1)] * SIDE
    alpha = np.zeros((NEAR, NEAR))
    beta = np.zeros((NEAR, NEAR))
    for j in range(NEAR):
        unit = [np.ones(1) * (k == j) for k in range(NEAR)]
        alpha[:, j] = [d[0] for d in cascade(flat, unit, zero)[0]]
        beta[:, j] = [f[0] for f in cascade(flat, zero, unit)[1]]
    lasts, firsts = [], []
    for level in range(NEAR):
        first = np.eye(EXT)[NEAR + level]
        for j in range(level):
            first = first + beta[level, j] * lasts[j]
        firsts.append(first)
        last = np.eye(EXT)[level]
        for j in range(level + 1):
            last = last + alpha[level, j] * firsts[j]
        lasts.append(last)
    return np.stack(lasts), np.stack(firsts)


W = end_weights(SIDE)
WZ = end_weights(LANES)
LAST, FIRST = seam_weights()
GROUP = LANES // EXT


def constant_tables():
    left = np.zeros((EXT, EXT))
    right = np.zeros((EXT, EXT))
    left[:, :NEAR] = LAST.T
    right[:, NEAR:] = FIRST.T
    spread = np.zeros((2, EXT, EXT))
    for level in range(NEAR):
        spread[0, level, EXT - (1 << level)] = 1.0
        spread[1, NEAR + level, EXT - (1 << level)] = 1.0
    each = np.eye(GROUP)
    solve = [np.kron(each, left), np.kron(each, right)]
    corner = np.zeros((2, LANES, LANES))
    corner[:, : EXT * EXT, : EXT * EXT] = [np.kron(left, np.eye(EXT)), np.kron(right, np.eye(EXT))]
    ends = []
    for half in range(2):
        end = np.zeros((LANES, LANES))
        end[:, : EXT * EXT] = np.kron(W[:, half * GROUP : (half + 1) * GROUP].T, np.eye(EXT))
        ends += [side @ end for side in solve]
    tables = np.concatenate(solve + ends + list(corner))
    spread = np.concatenate([np.kron(each, part) for part in spread], axis=1)
    return [t.astype(np.float32) for t in (np.tile(WZ.T, (1, GROUP)), tables, spread)]


SOLVE, ENDS, CORNER = (pl.ds(LANES * i, LANES * n) for i, n in ((0, 2), (2, 4), (6, 2)))


def dot(a, b):
    return jnp.dot(a, b, precision=lax.Precision.HIGHEST, preferred_element_type=F32)


def lanes_of(rows):
    return lax.broadcasted_iota(jnp.int32, (rows, LANES), 1)


def rows_of(rows):
    return lax.broadcasted_iota(jnp.int32, (rows, LANES), 0)


def roll(v, shift):
    return pltpu.roll(v, shift % LANES, 1)


def weighted(rows, load):
    sums = [None] * EXT
    for i in range(SIDE):
        block = load(i)
        for g in range(EXT):
            if W[g, i] != 0.0:
                term = float(W[g, i]) * block
                sums[g] = term if sums[g] is None else sums[g] + term
    return sums


def mix(weights, blocks):
    total = None
    for w, block in zip(weights, blocks):
        if w != 0.0:
            term = float(w) * block
            total = term if total is None else total + term
    return total


def ends_kernel(f, table, pz, block, sem):
    copy = pltpu.make_async_copy(f, block, sem)
    copy.start()
    copy.wait()
    out = dot(block[...], table[...])
    group = lanes_of(SIDE) // EXT
    for half in range(2):
        packed = jnp.zeros((SIDE, LANES), F32)
        for j in range(GROUP):
            first = (half * GROUP + j) * SIDE
            packed = jnp.where(group == j, out[first : first + SIDE], packed)
        pz[pl.ds(half * SIDE, SIDE), :] = packed


def faces_kernel(f, fx, fy):
    for c in range(SIDE // 8):
        for g, block in enumerate(weighted(8, lambda x: f[pl.ds(x * SIDE + 8 * c, 8), :])):
            fx[pl.ds(g * SIDE + 8 * c, 8), :] = block
    for c in range(SIDE // 8):
        for g, block in enumerate(weighted(8, lambda y: f[pl.ds(8 * c * SIDE + y, 8, stride=SIDE), :])):
            fy[pl.ds(g * SIDE + 8 * c, 8), :] = block


def depth_kernel(pz, before, after, fx, tables, ez, up, down):
    near = lanes_of(2 * SIDE) % EXT < NEAR
    own = pz[...]
    sides = jnp.concatenate([jnp.where(near, before[...], own), jnp.where(near, own, after[...])], axis=1)
    fxe = dot(jnp.concatenate([sides[:SIDE], sides[SIDE:]], axis=1), tables[ENDS, :])
    ez[...] = dot(sides, tables[SOLVE, :])
    for g in range(NEAR):
        up[pl.ds(g * SIDE, SIDE), :] = fx[pl.ds(g * SIDE, SIDE), :]
        down[pl.ds(g * SIDE, SIDE), :] = fx[pl.ds((NEAR + g) * SIDE, SIDE), :]
    up[pl.ds(NEAR * SIDE, SIDE), :] = fxe
    down[pl.ds(NEAR * SIDE, SIDE), :] = fxe


def width_kernel(up, down, before, after, fy, ez, wy, tables, xe, xee, yup, ydown):
    for c in range(SIDE // 8):
        rows = [pl.ds(g * SIDE + 8 * c, 8) for g in range(NEAR)]
        own_last = [up[r, :] for r in rows]
        own_first = [down[r, :] for r in rows]
        seam_before = [before[r, :] for r in rows] + own_first
        seam_after = own_last + [after[r, :] for r in rows]
        for level in range(NEAR):
            xe[pl.ds(level * SIDE + 8 * c, 8), :] = mix(LAST[level], seam_before)
            xe[pl.ds((NEAR + level) * SIDE + 8 * c, 8), :] = mix(FIRST[level], seam_after)
    near = lanes_of(SIDE) // EXT < NEAR
    rows = pl.ds(NEAR * SIDE, SIDE)
    own = up[rows, :]
    sides = [jnp.where(near, before[rows, :], own), jnp.where(near, own, after[rows, :])]
    corner = dot(jnp.concatenate(sides, axis=1), tables[CORNER, :])
    xee[...] = corner
    sums = weighted(EXT, lambda y: xe[pl.ds(y, EXT, stride=SIDE), :])
    for g in range(EXT):
        target = yup if g < NEAR else ydown
        base = (g % NEAR) * PITCH
        target[pl.ds(base, SIDE), :] = fy[pl.ds(g * SIDE, SIDE), :]
        target[pl.ds(base + SIDE, EXT), :] = sums[g]
    for i, block in enumerate((ez[pl.ds(0, SIDE), :], ez[pl.ds(SIDE, SIDE), :], corner)):
        part = dot(wy[...], block)
        yup[pl.ds(NEAR * PITCH + i * EXT, EXT), :] = part
        ydown[pl.ds(NEAR * PITCH + i * EXT, EXT), :] = part


def lift_chunk(ref, at, level, masked):
    step = 1 << level
    pairs = SIDE // (2 * step)
    masked = masked and level > 0
    behind = ref[at(SIDE + level), :]
    even = ref[at(0), :]
    for k in range(pairs):
        odd = ref[at(step * (2 * k + 1)), :]
        ahead = ref[at(step * (2 * k + 2)), :] if k < pairs - 1 else ref[at(SIDE + NEAR + level), :]
        detail = odd - 0.5 * (even + ahead)
        smooth = even + 0.25 * (behind + detail)
        if masked:
            live = (lanes_of(odd.shape[0]) & (step - 1)) == 0
            detail, smooth = jnp.where(live, detail, odd), jnp.where(live, smooth, even)
        ref[at(step * (2 * k + 1)), :] = detail
        ref[at(2 * step * k), :] = smooth
        behind, even = detail, ahead


def chunks(level):
    step = 1 << level
    count = SIDE // step
    own = [(8 * step * c, min(8, count), step) for c in range(max(1, count // 8))]
    return own + ([(SIDE, EXT, 1)] if level < NEAR else [])


def lift_lanes(level, rows, v, qa, qb, keep=None):
    step = 1 << level
    lane = [lanes_of(count) for _, count in rows]
    last = [x == LANES - step for x in lane]
    cells = [v[at, :] for at, _ in rows]
    odd = [roll(c, -step) for c in cells]
    ahead = [roll(jnp.where(l, qb[at, :], o), -step) for (at, _), l, o in zip(rows, last, odd)]
    mid = [o - 0.5 * (c + a) for o, c, a in zip(odd, cells, ahead)]
    odd = [roll(m, step) for m in mid]
    behind = [roll(jnp.where(l, qa[at, :], o), step) for (at, _), l, o in zip(rows, last, odd)]
    for i, (at, _) in enumerate(rows):
        place = lane[i] & (2 * step - 1)
        smooth = cells[i] + 0.25 * (mid[i] + behind[i])
        lifted = jnp.where(place == 0, smooth, jnp.where(place == step, odd[i], cells[i]))
        mask = keep(i) if keep else None
        v[at, :] = lifted if mask is None else jnp.where(mask, cells[i], lifted)


def lane_rows(level, pieces):
    step = 1 << level
    planes = list(range(0, SIDE, step)) + (list(range(SIDE, PITCH)) if level < NEAR - 1 else [])
    return [
        (pl.ds(x * PITCH + first, count, stride=stride), count)
        for x in planes
        for first, count, stride in pieces
    ]


def lift_width(ref, level, masked, pieces):
    for first, count, stride in pieces:
        lift_chunk(ref, lambda i: pl.ds(i * PITCH + first, count, stride=stride), level, masked)


def prepare_kernel(f, ez, xe, xee, spread, v, qa, qb):
    for x in range(SIDE):
        v[pl.ds(x * PITCH, SIDE), :] = f[pl.ds(x * SIDE, SIDE), :]
    for g in range(EXT):
        v[pl.ds((SIDE + g) * PITCH, SIDE), :] = xe[pl.ds(g * SIDE, SIDE), :]
    block = jnp.concatenate([ez[...], xee[...]], axis=0)
    spread_lanes(qa, qb, 0, SIDE, block, spread)
    for ref in (v, qa, qb):
        lift_width(ref, 0, False, chunks(0)[:-1])
        for first, count, stride in chunks(0):

            def at(i):
                return pl.ds(first * PITCH + i, count, stride=stride * PITCH)

            even, behind = ref[at(0), :], None
            for k in range(SIDE // 2 - 1):
                ahead = ref[at(2 * k + 2), :]
                detail = ref[at(2 * k + 1), :] - 0.5 * (even + ahead)
                ref[at(2 * k + 1), :] = detail
                if k > 0:
                    ref[at(2 * k), :] = even + 0.25 * (behind + detail)
                even, behind = ahead, detail
    row8 = rows_of(8)
    waits = [row8 <= 1, None, None, row8 >= 5]
    lift_lanes(0, lane_rows(0, chunks(0)[:-1]), v, qa, qb, lambda i: waits[i % 4])


def spread_lanes(qa, qb, first, rows, block, spread):
    both = dot(block, spread[...])
    for x in range(PITCH):
        group, j = x // GROUP, x % GROUP
        for ref, part in ((qa, both[:, :LANES]), (qb, both[:, LANES:])):
            cells = part[group * rows : (group + 1) * rows]
            ref[pl.ds(x * PITCH + first, rows), :] = roll(cells, -EXT * (j + 1))


def stretch(v):
    lane = lanes_of(v.shape[0])
    for k in (2, 1, 0):
        spots = [16 * c - 15 * (c % (1 << k)) for c in range(8) if c >> k & 1]
        v = jnp.where(functools.reduce(jnp.logical_or, [lane == p for p in spots]), roll(v, 15 << k), v)
    return v


def close_height(ref):
    for first, count, stride in chunks(0):

        def at(i):
            return pl.ds(first * PITCH + i, count, stride=stride * PITCH)

        last, end = ref[at(SIDE - 2), :], ref[at(SIDE - 1), :]
        end = end - 0.5 * (last + ref[at(SIDE + NEAR), :])
        ref[at(SIDE - 1), :] = end
        ref[at(SIDE - 2), :] = last + 0.25 * (ref[at(SIDE - 3), :] + end)
        ref[at(0), :] = ref[at(0), :] + 0.25 * (ref[at(SIDE), :] + ref[at(1), :])


def levels_kernel(
    yup, ydown, before, after, th, spread, v_in, qa_in, qb_in, coef, send, v, qa, qb
):
    del v_in, qa_in, qb_in
    for c in range(PITCH // 8):
        rows = [pl.ds(g * PITCH + 8 * c, 8) for g in range(NEAR)]
        seam_before = [before[r, :] for r in rows] + [ydown[r, :] for r in rows]
        seam_after = [yup[r, :] for r in rows] + [after[r, :] for r in rows]
        for level in range(NEAR):
            v[pl.ds(8 * c * PITCH + SIDE + level, 8, stride=PITCH), :] = mix(LAST[level], seam_before)
            v[pl.ds(8 * c * PITCH + SIDE + NEAR + level, 8, stride=PITCH), :] = mix(FIRST[level], seam_after)
    row8 = rows_of(EXT)
    extras = []
    for i in range(3):
        first = NEAR * PITCH + i * EXT
        own = [yup[pl.ds(first + j, 1), :] for j in range(EXT)]
        seam_before = [before[pl.ds(first + j, 1), :] for j in range(NEAR)] + own[NEAR:]
        seam_after = own[:NEAR] + [after[pl.ds(first + NEAR + j, 1), :] for j in range(NEAR)]
        extra = jnp.zeros((EXT, LANES), F32)
        for level in range(NEAR):
            extra = jnp.where(row8 == level, mix(LAST[level], seam_before), extra)
            extra = jnp.where(row8 == NEAR + level, mix(FIRST[level], seam_after), extra)
        extras.append(extra)
    block = jnp.concatenate(extras, axis=0)
    spread_lanes(qa, qb, SIDE, EXT, block, spread)

    for level in range(NEAR):
        pieces = chunks(level)
        for ref in (v, qa, qb):
            lift_width(ref, level, ref is v, pieces[-1:] if level == 0 else pieces)
            if level == 0:
                close_height(ref)
                continue
            for first, count, stride in pieces:
                lift_chunk(
                    ref,
                    lambda i: pl.ds(first * PITCH + i, count, stride=stride * PITCH),
                    level,
                    ref is v,
                )
        if level == 0:
            rows = lane_rows(0, pieces[-1:])
            for y in (0, 1, SIDE - 3, SIDE - 2, SIDE - 1):
                rows += [(pl.ds(8 * c * PITCH + y, 8, stride=PITCH), 8) for c in range(PITCH // 8)]
        else:
            rows = lane_rows(level, pieces[: len(pieces) - (level == NEAR - 1)])
        lift_lanes(level, rows, v, qa, qb)

    energy = [jnp.zeros((8, LANES), F32)] * NEAR
    kept = [jnp.zeros((8, LANES), F32)] * NEAR
    for c in range(SIDE // 8):
        bits = (rows_of(8) + 8 * c) | lanes_of(8)
        own = [(bits & ((2 << level) - 1)) == (1 << level) for level in range(NEAR)]
        rest = [(bits & ((1 << level) - 1)) == 0 for level in range(NEAR)]
        bounds = []
        for depth in range(NEAR + 1):
            bound = jnp.broadcast_to(th[pl.ds(min(depth, NEAR - 1), 1), :], (8, LANES))
            for level in range(min(depth, NEAR - 1) - 1, -1, -1):
                bound = jnp.where(own[level], th[pl.ds(level, 1), :], bound)
            bounds.append(bound)
        squares = [None] * (NEAR + 1)
        sizes = [None] * (NEAR + 1)
        for x in range(SIDE):
            depth = NEAR if x == 0 else min(NEAR, (x & -x).bit_length() - 1)
            cells = v[pl.ds(x * PITCH + 8 * c, 8), :]
            shrunk = cells - jnp.minimum(jnp.maximum(cells, -bounds[depth]), bounds[depth])
            coef[pl.ds(x * SIDE + 8 * c, 8), :] = shrunk
            square, size = cells * cells, jnp.abs(shrunk)
            squares[depth] = square if squares[depth] is None else squares[depth] + square
            sizes[depth] = size if sizes[depth] is None else sizes[depth] + size
        for sums, target in ((squares, energy), (sizes, kept)):
            for level in range(NEAR):
                deeper = functools.reduce(lambda a, b: a + b, sums[level + 1 :])
                part = jnp.where(rest[level], sums[level], 0.0) + jnp.where(own[level], deeper, 0.0)
                target[level] = target[level] + part

    lane8 = lanes_of(8)
    block = jnp.zeros((8, LANES), F32)
    for i in range(4):
        block = jnp.where(row8 == i, v[pl.ds((i // 2 * PITCH + i % 2) * 16, 1), :], block)
    source, target = rows_of(LANES), lanes_of(LANES)
    pick = jnp.where((source == 16 * (target % 8)) & (target < 32), 1.0, 0.0).astype(F32)
    block = jnp.where(lane8 // 8 == row8, dot(block, pick), 0.0)
    for i, part in enumerate(energy + kept):
        block = jnp.where((lane8 == 32 + i) & (row8 == 0), jnp.sum(part), block)
    send[...] = jnp.broadcast_to(jnp.sum(block, axis=0, keepdims=True), send.shape)


def last_kernel(spot, got, coef, th, out, stats, grid, planes, sums_out, sem, *, sizes, counts):
    half = SIDE // 2
    copies = []
    for a in range(2):
        at = pl.ds((a * half + 1) * SIDE, (half - 1) * SIDE)
        copies.append(pltpu.make_async_copy(coef.at[at], out.at[at], sem.at[a]))
        copies[a].start()
        planes[pl.ds(a * SIDE, SIDE), :] = coef[pl.ds(a * half * SIDE, SIDE), :]
    nx, ny, nz = sizes
    plane = ny * nz
    lane, row = lanes_of(plane), rows_of(plane)
    v = [got[pl.ds(i * plane, plane), :] for i in range(nx)]
    sums = functools.reduce(lambda a, b: a + b, v)
    sums = jnp.sum(sums, axis=0, keepdims=True)

    def down(a, shift):
        return pltpu.roll(a, shift % plane, 0)

    odd = (lane & 16) != 0
    d = [v[i] - 0.5 * roll(v[i] + v[(i + 1) % nx], 16) for i in range(nx)]
    v = [jnp.where(odd, d[i], v[i] + 0.25 * roll(d[i] + d[i - 1], -16)) for i in range(nx)]
    odd = (lane & 8) != 0
    d = [a - 0.5 * roll(a + down(a, -nz), 8) for a in v]
    v = [jnp.where(odd, b, a + 0.25 * roll(b + down(b, nz), -8)) for a, b in zip(v, d)]
    odd = (lane & 1) != 0
    top, low = (lane & 7) == 7, (lane & 7) == 0
    far = row % nz == nz - 1
    near = row % nz == 0
    result = []
    for a in v:
        following = jnp.where(far, down(a, nz - 1), down(a, -1))
        d = a - 0.5 * (roll(a, 1) + jnp.where(top, roll(following, 7), roll(a, -1)))
        previous = jnp.where(near, down(d, 1 - nz), down(d, 1))
        s = a + 0.25 * (jnp.where(low, roll(previous, -7), roll(d, 1)) + roll(d, -1))
        result.append(jnp.where(odd, d, s))
    bound = th[pl.ds(LEVELS - 1, 1), :]
    detail = (lane < 32) & ((lane & 25) != 0)
    energy = kept = None
    for i, a in enumerate(result):
        shrunk = a - jnp.minimum(jnp.maximum(a, -bound), bound)
        grid[pl.ds(i * plane, plane), :] = jnp.where(detail, shrunk, a)
        square, size = jnp.where(detail, a * a, 0.0), jnp.where(detail, jnp.abs(shrunk), 0.0)
        energy = square if energy is None else energy + square
        kept = size if kept is None else kept + size
    lane1 = lanes_of(1)
    for i, (part, base) in enumerate(((energy, 32), (kept, 36))):
        totals = jnp.where(lane1 == NEAR, jnp.sum(part), roll(sums, -base))
        scale = jnp.zeros((1, LANES), F32)
        for level in range(LEVELS):
            scale = jnp.where(lane1 == level, 1.0 / counts[level], scale)
        sums_out[i] = (totals * scale)[:, :LEVELS]

    own = grid[pl.ds(spot[0], 1), :]
    start = lanes_of(1) % 16 == 0
    for i in range(4):
        at = pl.ds(i * half, 1)
        planes[at, :] = jnp.where(start, stretch(roll(own, -8 * i)), planes[at, :])
    for a in range(2):
        target = out.at[pl.ds(a * half * SIDE, SIDE)]
        copies.append(pltpu.make_async_copy(planes.at[pl.ds(a * SIDE, SIDE)], target, sem.at[2 + a]))
    copies.append(pltpu.make_async_copy(sums_out, stats, sem.at[4]))
    for copy in copies[2:]:
        copy.start()
    for copy in copies:
        copy.wait()


def shape(*dims):
    return jax.ShapeDtypeStruct(dims, F32)


def shards(fields, exponents):
    sizes = tuple(lax.axis_size(a) for a in ("gx", "gy", "gz"))
    devices = sizes[0] * sizes[1] * sizes[2]
    cells = fields.size * devices
    counts = [7.0 * cells / 8 ** (level + 1) for level in range(LEVELS)]
    f = fields.reshape(SIDE * SIDE, LANES)
    th = jnp.broadcast_to(jnp.pad(jnp.exp2(exponents.astype(F32)), (0, 3))[:, None], (8, LANES))
    table, tables, spread = (jnp.asarray(t) for t in constant_tables())
    wy = jnp.asarray(W.astype(np.float32))

    def swap(up, down, axis):
        n = lax.axis_size(axis)
        before = lax.ppermute(up, axis, [(i, (i + 1) % n) for i in range(n)])
        after = lax.ppermute(down, axis, [((i + 1) % n, i) for i in range(n)])
        return before, after

    here = pl.BlockSpec(memory_space=pltpu.VMEM)
    there = pl.BlockSpec(memory_space=pltpu.HBM)

    def pinned(a):
        return pltpu.with_memory_space_constraint(a, pltpu.VMEM)

    def local(kernel, name, outs, *args, aliases={}):
        args = [pinned(a) for a in args]
        return pl.pallas_call(
            kernel,
            in_specs=[here] * len(args),
            out_specs=[here] * len(outs),
            out_shape=[pltpu.VMEM((rows, LANES), F32) for rows in outs],
            input_output_aliases=aliases,
            compiler_params=pltpu.CompilerParams(vmem_limit_bytes=8 << 20),
            name=name,
        )(*args)

    spot = lax.axis_index(("gx", "gy", "gz")).astype(jnp.int32).reshape(1)
    pz = pl.pallas_call(
        ends_kernel,
        in_specs=[there, here],
        out_specs=here,
        out_shape=pltpu.VMEM((2 * SIDE, LANES), F32),
        scratch_shapes=[pltpu.VMEM((SIDE * SIDE, LANES), F32), pltpu.SemaphoreType.DMA(())],
        compiler_params=pltpu.CompilerParams(vmem_limit_bytes=8 << 20),
        name="ends",
    )(f, table)
    before, after = swap(pz, pz, "gz")
    fx, fy = local(faces_kernel, "faces", (EXT * SIDE, EXT * SIDE), f)
    message = (NEAR + 1) * SIDE
    ez, up, down = local(
        depth_kernel, "depth", (2 * SIDE, message, message), pz, before, after, fx, tables
    )
    before, after = swap(up, down, "gx")
    message = NEAR * PITCH + 3 * EXT
    xe, xee, yup, ydown = local(
        width_kernel, "width", (EXT * SIDE, SIDE, message, message), up, down, before, after, fy, ez, wy, tables
    )
    before, after = swap(yup, ydown, "gy")
    block = PITCH * PITCH
    v, qa, qb = local(
        prepare_kernel,
        "prepare",
        (block,) * 3,
        *(f, ez, xe, xee, spread),
    )
    coef, send, *_ = local(
        levels_kernel,
        "levels",
        (SIDE * SIDE, devices, block, block, block),
        *(yup, ydown, before, after, th, spread, v, qa, qb),
        aliases={6: 2, 7: 3, 8: 4},
    )
    send, spot, th = lax.optimization_barrier((send, spot, th))
    got = lax.all_to_all(send.reshape(devices, 1, LANES), ("gx", "gy", "gz"), 0, 0).reshape(devices, LANES)
    out, stats = pl.pallas_call(
        functools.partial(last_kernel, sizes=sizes, counts=counts),
        in_specs=[pl.BlockSpec(memory_space=pltpu.SMEM), here, here, here],
        out_specs=[there, there],
        out_shape=(shape(SIDE * SIDE, LANES), shape(2, 1, LEVELS)),
        scratch_shapes=[
            pltpu.VMEM((devices, LANES), F32),
            pltpu.VMEM((2 * SIDE, LANES), F32),
            pltpu.VMEM((2, 1, LEVELS), F32),
            pltpu.SemaphoreType.DMA((5,)),
        ],
        compiler_params=pltpu.CompilerParams(vmem_limit_bytes=8 << 20),
        name="last",
    )(spot, pinned(got), pinned(coef), pinned(th))
    return out.reshape(fields.shape), stats


def solution(mesh):
    placed = (P(None, "gx", "gy", "gz"), P())
    return jax.shard_map(shards, mesh=mesh, in_specs=placed, out_specs=placed, check_vma=False)
```

```python
import functools

import jax
import jax.numpy as jnp
import numpy as np
from jax import lax
from jax.experimental import pallas as pl
from jax.experimental.pallas import tpu as pltpu
from jax.sharding import PartitionSpec as P

NEAR = 4
LEVELS = 5
LANES = 128
SIDE = 32
EXT = 2 * NEAR
PITCH = SIDE + EXT
F32 = jnp.float32


def cascade(cells, ahead, behind):
    details, firsts = [], []
    for level in range(NEAR):
        half = len(cells) // 2
        following = cells[2::2] + [ahead[level]]
        detail = [cells[2 * k + 1] - 0.5 * (cells[2 * k] + following[k]) for k in range(half)]
        details.append(detail[-1])
        firsts.append(cells[0])
        before = [behind[level]] + detail[:-1]
        cells = [cells[2 * k] + 0.25 * (before[k] + detail[k]) for k in range(half)]
    return details, firsts


def end_weights(length):
    none = [np.zeros(length)] * NEAR
    details, firsts = cascade(list(np.eye(length)), none, none)
    return np.stack(details + firsts)


def seam_weights():
    zero = [np.zeros(1)] * NEAR
    flat = [np.zeros(1)] * SIDE
    alpha = np.zeros((NEAR, NEAR))
    beta = np.zeros((NEAR, NEAR))
    for j in range(NEAR):
        unit = [np.ones(1) * (k == j) for k in range(NEAR)]
        alpha[:, j] = [d[0] for d in cascade(flat, unit, zero)[0]]
        beta[:, j] = [f[0] for f in cascade(flat, zero, unit)[1]]
    lasts, firsts = [], []
    for level in range(NEAR):
        first = np.eye(EXT)[NEAR + level]
        for j in range(level):
            first = first + beta[level, j] * lasts[j]
        firsts.append(first)
        last = np.eye(EXT)[level]
        for j in range(level + 1):
            last = last + alpha[level, j] * firsts[j]
        lasts.append(last)
    return np.stack(lasts), np.stack(firsts)


W = end_weights(SIDE)
WZ = end_weights(LANES)
LAST, FIRST = seam_weights()
GROUP = LANES // EXT


def constant_tables():
    left = np.zeros((EXT, EXT))
    right = np.zeros((EXT, EXT))
    left[:, :NEAR] = LAST.T
    right[:, NEAR:] = FIRST.T
    spread = np.zeros((2, EXT, EXT))
    for level in range(NEAR):
        spread[0, level, EXT - (1 << level)] = 1.0
        spread[1, NEAR + level, EXT - (1 << level)] = 1.0
    each = np.eye(GROUP)
    solve = [np.kron(each, left), np.kron(each, right)]
    corner = np.zeros((2, LANES, LANES))
    corner[:, : EXT * EXT, : EXT * EXT] = [np.kron(left, np.eye(EXT)), np.kron(right, np.eye(EXT))]
    ends = []
    for half in range(2):
        end = np.zeros((LANES, LANES))
        end[:, : EXT * EXT] = np.kron(W[:, half * GROUP : (half + 1) * GROUP].T, np.eye(EXT))
        ends += [side @ end for side in solve]
    tables = np.concatenate(solve + ends + list(corner))
    spread = np.concatenate([np.kron(each, part) for part in spread], axis=1)
    return [t.astype(np.float32) for t in (np.tile(WZ.T, (1, GROUP)), tables, spread)]


SOLVE, ENDS, CORNER = (pl.ds(LANES * i, LANES * n) for i, n in ((0, 2), (2, 4), (6, 2)))


def dot(a, b):
    return jnp.dot(a, b, precision=lax.Precision.HIGHEST, preferred_element_type=F32)


def lanes_of(rows):
    return lax.broadcasted_iota(jnp.int32, (rows, LANES), 1)


def rows_of(rows):
    return lax.broadcasted_iota(jnp.int32, (rows, LANES), 0)


def roll(v, shift):
    return pltpu.roll(v, shift % LANES, 1)


def weighted(rows, load):
    sums = [None] * EXT
    for i in range(SIDE):
        block = load(i)
        for g in range(EXT):
            if W[g, i] != 0.0:
                term = float(W[g, i]) * block
                sums[g] = term if sums[g] is None else sums[g] + term
    return sums


def mix(weights, blocks):
    total = None
    for w, block in zip(weights, blocks):
        if w != 0.0:
            term = float(w) * block
            total = term if total is None else total + term
    return total


def ends_kernel(f, table, pz, block, weights, sem):
    copies = [pltpu.make_async_copy(f, block, sem.at[0]), pltpu.make_async_copy(table, weights, sem.at[1])]
    for copy in copies:
        copy.start()
    for copy in copies:
        copy.wait()
    out = dot(block[...], weights[...])
    group = lanes_of(SIDE) // EXT
    for half in range(2):
        packed = jnp.zeros((SIDE, LANES), F32)
        for j in range(GROUP):
            first = (half * GROUP + j) * SIDE
            packed = jnp.where(group == j, out[first : first + SIDE], packed)
        pz[pl.ds(half * SIDE, SIDE), :] = packed


def faces_kernel(f, fx, fy):
    for c in range(SIDE // 8):
        for g, block in enumerate(weighted(8, lambda x: f[pl.ds(x * SIDE + 8 * c, 8), :])):
            fx[pl.ds(g * SIDE + 8 * c, 8), :] = block
    for c in range(SIDE // 8):
        for g, block in enumerate(weighted(8, lambda y: f[pl.ds(8 * c * SIDE + y, 8, stride=SIDE), :])):
            fy[pl.ds(g * SIDE + 8 * c, 8), :] = block


def depth_kernel(pz, before, after, fx, tables, ez, up, down):
    near = lanes_of(2 * SIDE) % EXT < NEAR
    own = pz[...]
    sides = jnp.concatenate([jnp.where(near, before[...], own), jnp.where(near, own, after[...])], axis=1)
    fxe = dot(jnp.concatenate([sides[:SIDE], sides[SIDE:]], axis=1), tables[ENDS, :])
    ez[...] = dot(sides, tables[SOLVE, :])
    for g in range(NEAR):
        up[pl.ds(g * SIDE, SIDE), :] = fx[pl.ds(g * SIDE, SIDE), :]
        down[pl.ds(g * SIDE, SIDE), :] = fx[pl.ds((NEAR + g) * SIDE, SIDE), :]
    up[pl.ds(NEAR * SIDE, SIDE), :] = fxe
    down[pl.ds(NEAR * SIDE, SIDE), :] = fxe


def width_kernel(up, down, before, after, fy, ez, wy, tables, xe, xee, yup, ydown):
    for c in range(SIDE // 8):
        rows = [pl.ds(g * SIDE + 8 * c, 8) for g in range(NEAR)]
        own_last = [up[r, :] for r in rows]
        own_first = [down[r, :] for r in rows]
        seam_before = [before[r, :] for r in rows] + own_first
        seam_after = own_last + [after[r, :] for r in rows]
        for level in range(NEAR):
            xe[pl.ds(level * SIDE + 8 * c, 8), :] = mix(LAST[level], seam_before)
            xe[pl.ds((NEAR + level) * SIDE + 8 * c, 8), :] = mix(FIRST[level], seam_after)
    near = lanes_of(SIDE) // EXT < NEAR
    rows = pl.ds(NEAR * SIDE, SIDE)
    own = up[rows, :]
    sides = [jnp.where(near, before[rows, :], own), jnp.where(near, own, after[rows, :])]
    corner = dot(jnp.concatenate(sides, axis=1), tables[CORNER, :])
    xee[...] = corner
    sums = weighted(EXT, lambda y: xe[pl.ds(y, EXT, stride=SIDE), :])
    for g in range(EXT):
        target = yup if g < NEAR else ydown
        base = (g % NEAR) * PITCH
        target[pl.ds(base, SIDE), :] = fy[pl.ds(g * SIDE, SIDE), :]
        target[pl.ds(base + SIDE, EXT), :] = sums[g]
    for i, block in enumerate((ez[pl.ds(0, SIDE), :], ez[pl.ds(SIDE, SIDE), :], corner)):
        part = dot(wy[...], block)
        yup[pl.ds(NEAR * PITCH + i * EXT, EXT), :] = part
        ydown[pl.ds(NEAR * PITCH + i * EXT, EXT), :] = part


def lift_chunk(ref, at, level, masked):
    step = 1 << level
    pairs = SIDE // (2 * step)
    masked = masked and level > 0
    behind = ref[at(SIDE + level), :]
    even = ref[at(0), :]
    for k in range(pairs):
        odd = ref[at(step * (2 * k + 1)), :]
        ahead = ref[at(step * (2 * k + 2)), :] if k < pairs - 1 else ref[at(SIDE + NEAR + level), :]
        detail = odd - 0.5 * (even + ahead)
        smooth = even + 0.25 * (behind + detail)
        if masked:
            live = (lanes_of(odd.shape[0]) & (step - 1)) == 0
            detail, smooth = jnp.where(live, detail, odd), jnp.where(live, smooth, even)
        ref[at(step * (2 * k + 1)), :] = detail
        ref[at(2 * step * k), :] = smooth
        behind, even = detail, ahead


def chunks(level):
    step = 1 << level
    count = SIDE // step
    own = [(8 * step * c, min(8, count), step) for c in range(max(1, count // 8))]
    return own + ([(SIDE, EXT, 1)] if level < NEAR else [])


def lift_lanes(level, rows, v, qa, qb, keep=None):
    step = 1 << level
    lane = [lanes_of(count) for _, count in rows]
    last = [x == LANES - step for x in lane]
    cells = [v[at, :] for at, _ in rows]
    odd = [roll(c, -step) for c in cells]
    ahead = [roll(jnp.where(l, qb[at, :], o), -step) for (at, _), l, o in zip(rows, last, odd)]
    mid = [o - 0.5 * (c + a) for o, c, a in zip(odd, cells, ahead)]
    odd = [roll(m, step) for m in mid]
    behind = [roll(jnp.where(l, qa[at, :], o), step) for (at, _), l, o in zip(rows, last, odd)]
    for i, (at, _) in enumerate(rows):
        place = lane[i] & (2 * step - 1)
        smooth = cells[i] + 0.25 * (mid[i] + behind[i])
        lifted = jnp.where(place == 0, smooth, jnp.where(place == step, odd[i], cells[i]))
        mask = keep(i) if keep else None
        v[at, :] = lifted if mask is None else jnp.where(mask, cells[i], lifted)


def lane_rows(level, pieces):
    step = 1 << level
    planes = list(range(0, SIDE, step)) + (list(range(SIDE, PITCH)) if level < NEAR - 1 else [])
    return [
        (pl.ds(x * PITCH + first, count, stride=stride), count)
        for x in planes
        for first, count, stride in pieces
    ]


def lift_width(ref, level, masked, pieces):
    for first, count, stride in pieces:
        lift_chunk(ref, lambda i: pl.ds(i * PITCH + first, count, stride=stride), level, masked)


def prepare_kernel(f, ez, xe, xee, spread, v, qa, qb):
    for x in range(SIDE):
        v[pl.ds(x * PITCH, SIDE), :] = f[pl.ds(x * SIDE, SIDE), :]
    for g in range(EXT):
        v[pl.ds((SIDE + g) * PITCH, SIDE), :] = xe[pl.ds(g * SIDE, SIDE), :]
    block = jnp.concatenate([ez[...], xee[...]], axis=0)
    spread_lanes(qa, qb, 0, SIDE, block, spread)
    for ref in (v, qa, qb):
        lift_width(ref, 0, False, chunks(0)[:-1])
        for first, count, stride in chunks(0):

            def at(i):
                return pl.ds(first * PITCH + i, count, stride=stride * PITCH)

            even, behind = ref[at(0), :], None
            for k in range(SIDE // 2 - 1):
                ahead = ref[at(2 * k + 2), :]
                detail = ref[at(2 * k + 1), :] - 0.5 * (even + ahead)
                ref[at(2 * k + 1), :] = detail
                if k > 0:
                    ref[at(2 * k), :] = even + 0.25 * (behind + detail)
                even, behind = ahead, detail
    row8 = rows_of(8)
    waits = [row8 <= 1, None, None, row8 >= 5]
    lift_lanes(0, lane_rows(0, chunks(0)[:-1]), v, qa, qb, lambda i: waits[i % 4])


def spread_lanes(qa, qb, first, rows, block, spread):
    both = dot(block, spread[...])
    for x in range(PITCH):
        group, j = x // GROUP, x % GROUP
        for ref, part in ((qa, both[:, :LANES]), (qb, both[:, LANES:])):
            cells = part[group * rows : (group + 1) * rows]
            ref[pl.ds(x * PITCH + first, rows), :] = roll(cells, -EXT * (j + 1))


def stretch(v):
    lane = lanes_of(v.shape[0])
    for k in (2, 1, 0):
        spots = [16 * c - 15 * (c % (1 << k)) for c in range(8) if c >> k & 1]
        v = jnp.where(functools.reduce(jnp.logical_or, [lane == p for p in spots]), roll(v, 15 << k), v)
    return v


def close_height(ref):
    for first, count, stride in chunks(0):

        def at(i):
            return pl.ds(first * PITCH + i, count, stride=stride * PITCH)

        last, end = ref[at(SIDE - 2), :], ref[at(SIDE - 1), :]
        end = end - 0.5 * (last + ref[at(SIDE + NEAR), :])
        ref[at(SIDE - 1), :] = end
        ref[at(SIDE - 2), :] = last + 0.25 * (ref[at(SIDE - 3), :] + end)
        ref[at(0), :] = ref[at(0), :] + 0.25 * (ref[at(SIDE), :] + ref[at(1), :])


def levels_kernel(
    yup, ydown, before, after, th, spread, v_in, qa_in, qb_in, coef, send, v, qa, qb
):
    del v_in, qa_in, qb_in
    for c in range(PITCH // 8):
        rows = [pl.ds(g * PITCH + 8 * c, 8) for g in range(NEAR)]
        seam_before = [before[r, :] for r in rows] + [ydown[r, :] for r in rows]
        seam_after = [yup[r, :] for r in rows] + [after[r, :] for r in rows]
        for level in range(NEAR):
            v[pl.ds(8 * c * PITCH + SIDE + level, 8, stride=PITCH), :] = mix(LAST[level], seam_before)
            v[pl.ds(8 * c * PITCH + SIDE + NEAR + level, 8, stride=PITCH), :] = mix(FIRST[level], seam_after)
    row8 = rows_of(EXT)
    extras = []
    for i in range(3):
        first = NEAR * PITCH + i * EXT
        own = [yup[pl.ds(first + j, 1), :] for j in range(EXT)]
        seam_before = [before[pl.ds(first + j, 1), :] for j in range(NEAR)] + own[NEAR:]
        seam_after = own[:NEAR] + [after[pl.ds(first + NEAR + j, 1), :] for j in range(NEAR)]
        extra = jnp.zeros((EXT, LANES), F32)
        for level in range(NEAR):
            extra = jnp.where(row8 == level, mix(LAST[level], seam_before), extra)
            extra = jnp.where(row8 == NEAR + level, mix(FIRST[level], seam_after), extra)
        extras.append(extra)
    block = jnp.concatenate(extras, axis=0)
    spread_lanes(qa, qb, SIDE, EXT, block, spread)

    for level in range(NEAR):
        pieces = chunks(level)
        for ref in (v, qa, qb):
            lift_width(ref, level, ref is v, pieces[-1:] if level == 0 else pieces)
            if level == 0:
                close_height(ref)
                continue
            for first, count, stride in pieces:
                lift_chunk(
                    ref,
                    lambda i: pl.ds(first * PITCH + i, count, stride=stride * PITCH),
                    level,
                    ref is v,
                )
        if level == 0:
            rows = lane_rows(0, pieces[-1:])
            for y in (0, 1, SIDE - 3, SIDE - 2, SIDE - 1):
                rows += [(pl.ds(8 * c * PITCH + y, 8, stride=PITCH), 8) for c in range(PITCH // 8)]
        else:
            rows = lane_rows(level, pieces[: len(pieces) - (level == NEAR - 1)])
        lift_lanes(level, rows, v, qa, qb)

    energy = [jnp.zeros((8, LANES), F32)] * NEAR
    kept = [jnp.zeros((8, LANES), F32)] * NEAR
    for c in range(SIDE // 8):
        bits = (rows_of(8) + 8 * c) | lanes_of(8)
        own = [(bits & ((2 << level) - 1)) == (1 << level) for level in range(NEAR)]
        rest = [(bits & ((1 << level) - 1)) == 0 for level in range(NEAR)]
        bounds = []
        for depth in range(NEAR + 1):
            bound = jnp.broadcast_to(th[pl.ds(min(depth, NEAR - 1), 1), :], (8, LANES))
            for level in range(min(depth, NEAR - 1) - 1, -1, -1):
                bound = jnp.where(own[level], th[pl.ds(level, 1), :], bound)
            bounds.append(bound)
        squares = [None] * (NEAR + 1)
        sizes = [None] * (NEAR + 1)
        for x in range(SIDE):
            depth = NEAR if x == 0 else min(NEAR, (x & -x).bit_length() - 1)
            cells = v[pl.ds(x * PITCH + 8 * c, 8), :]
            shrunk = cells - jnp.minimum(jnp.maximum(cells, -bounds[depth]), bounds[depth])
            coef[pl.ds(x * SIDE + 8 * c, 8), :] = shrunk
            square, size = cells * cells, jnp.abs(shrunk)
            squares[depth] = square if squares[depth] is None else squares[depth] + square
            sizes[depth] = size if sizes[depth] is None else sizes[depth] + size
        for sums, target in ((squares, energy), (sizes, kept)):
            for level in range(NEAR):
                deeper = functools.reduce(lambda a, b: a + b, sums[level + 1 :])
                part = jnp.where(rest[level], sums[level], 0.0) + jnp.where(own[level], deeper, 0.0)
                target[level] = target[level] + part

    lane8 = lanes_of(8)
    block = jnp.zeros((8, LANES), F32)
    for i in range(4):
        block = jnp.where(row8 == i, v[pl.ds((i // 2 * PITCH + i % 2) * 16, 1), :], block)
    source, target = rows_of(LANES), lanes_of(LANES)
    pick = jnp.where((source == 16 * (target % 8)) & (target < 32), 1.0, 0.0).astype(F32)
    block = jnp.where(lane8 // 8 == row8, dot(block, pick), 0.0)
    for i, part in enumerate(energy + kept):
        block = jnp.where((lane8 == 32 + i) & (row8 == 0), jnp.sum(part), block)
    send[...] = jnp.broadcast_to(jnp.sum(block, axis=0, keepdims=True), send.shape)


def last_kernel(spot, got, coef, th, out, stats, grid, planes, sums_out, sem, *, sizes, counts):
    half = SIDE // 2
    copies = []
    for a in range(2):
        at = pl.ds((a * half + 1) * SIDE, (half - 1) * SIDE)
        copies.append(pltpu.make_async_copy(coef.at[at], out.at[at], sem.at[a]))
        copies[a].start()
        planes[pl.ds(a * SIDE, SIDE), :] = coef[pl.ds(a * half * SIDE, SIDE), :]
    nx, ny, nz = sizes
    plane = ny * nz
    lane, row = lanes_of(plane), rows_of(plane)
    v = [got[pl.ds(i * plane, plane), :] for i in range(nx)]
    sums = functools.reduce(lambda a, b: a + b, v)
    sums = jnp.sum(sums, axis=0, keepdims=True)

    def down(a, shift):
        return pltpu.roll(a, shift % plane, 0)

    odd = (lane & 16) != 0
    d = [v[i] - 0.5 * roll(v[i] + v[(i + 1) % nx], 16) for i in range(nx)]
    v = [jnp.where(odd, d[i], v[i] + 0.25 * roll(d[i] + d[i - 1], -16)) for i in range(nx)]
    odd = (lane & 8) != 0
    d = [a - 0.5 * roll(a + down(a, -nz), 8) for a in v]
    v = [jnp.where(odd, b, a + 0.25 * roll(b + down(b, nz), -8)) for a, b in zip(v, d)]
    odd = (lane & 1) != 0
    top, low = (lane & 7) == 7, (lane & 7) == 0
    far = row % nz == nz - 1
    near = row % nz == 0
    result = []
    for a in v:
        following = jnp.where(far, down(a, nz - 1), down(a, -1))
        d = a - 0.5 * (roll(a, 1) + jnp.where(top, roll(following, 7), roll(a, -1)))
        previous = jnp.where(near, down(d, 1 - nz), down(d, 1))
        s = a + 0.25 * (jnp.where(low, roll(previous, -7), roll(d, 1)) + roll(d, -1))
        result.append(jnp.where(odd, d, s))
    bound = th[pl.ds(LEVELS - 1, 1), :]
    detail = (lane < 32) & ((lane & 25) != 0)
    energy = kept = None
    for i, a in enumerate(result):
        shrunk = a - jnp.minimum(jnp.maximum(a, -bound), bound)
        grid[pl.ds(i * plane, plane), :] = jnp.where(detail, shrunk, a)
        square, size = jnp.where(detail, a * a, 0.0), jnp.where(detail, jnp.abs(shrunk), 0.0)
        energy = square if energy is None else energy + square
        kept = size if kept is None else kept + size
    lane1 = lanes_of(1)
    for i, (part, base) in enumerate(((energy, 32), (kept, 36))):
        totals = jnp.where(lane1 == NEAR, jnp.sum(part), roll(sums, -base))
        scale = jnp.zeros((1, LANES), F32)
        for level in range(LEVELS):
            scale = jnp.where(lane1 == level, 1.0 / counts[level], scale)
        sums_out[i] = (totals * scale)[:, :LEVELS]

    own = grid[pl.ds(spot[0], 1), :]
    start = lanes_of(1) % 16 == 0
    for i in range(4):
        at = pl.ds(i * half, 1)
        planes[at, :] = jnp.where(start, stretch(roll(own, -8 * i)), planes[at, :])
    for a in range(2):
        target = out.at[pl.ds(a * half * SIDE, SIDE)]
        copies.append(pltpu.make_async_copy(planes.at[pl.ds(a * SIDE, SIDE)], target, sem.at[2 + a]))
    copies.append(pltpu.make_async_copy(sums_out, stats, sem.at[4]))
    for copy in copies[2:]:
        copy.start()
    for copy in copies:
        copy.wait()


def shape(*dims):
    return jax.ShapeDtypeStruct(dims, F32)


def shards(fields, exponents):
    sizes = tuple(lax.axis_size(a) for a in ("gx", "gy", "gz"))
    devices = sizes[0] * sizes[1] * sizes[2]
    cells = fields.size * devices
    counts = [7.0 * cells / 8 ** (level + 1) for level in range(LEVELS)]
    f = fields.reshape(SIDE * SIDE, LANES)
    th = jnp.broadcast_to(jnp.pad(jnp.exp2(exponents.astype(F32)), (0, 3))[:, None], (8, LANES))
    table, tables, spread = (jnp.asarray(t) for t in constant_tables())
    wy = jnp.asarray(W.astype(np.float32))

    def swap(up, down, axis):
        n = lax.axis_size(axis)
        before = lax.ppermute(up, axis, [(i, (i + 1) % n) for i in range(n)])
        after = lax.ppermute(down, axis, [((i + 1) % n, i) for i in range(n)])
        return before, after

    here = pl.BlockSpec(memory_space=pltpu.VMEM)
    there = pl.BlockSpec(memory_space=pltpu.HBM)

    def pinned(a):
        return pltpu.with_memory_space_constraint(a, pltpu.VMEM)

    def local(kernel, name, outs, *args, aliases={}):
        args = [pinned(a) for a in args]
        return pl.pallas_call(
            kernel,
            in_specs=[here] * len(args),
            out_specs=[here] * len(outs),
            out_shape=[pltpu.VMEM((rows, LANES), F32) for rows in outs],
            input_output_aliases=aliases,
            compiler_params=pltpu.CompilerParams(vmem_limit_bytes=8 << 20),
            name=name,
        )(*args)

    spot = lax.axis_index(("gx", "gy", "gz")).astype(jnp.int32).reshape(1)
    pz, f = pl.pallas_call(
        ends_kernel,
        in_specs=[there] * 2,
        out_specs=[here] * 2,
        out_shape=[pltpu.VMEM((2 * SIDE, LANES), F32), pltpu.VMEM((SIDE * SIDE, LANES), F32)],
        scratch_shapes=[pltpu.VMEM((LANES, LANES), F32), pltpu.SemaphoreType.DMA((2,))],
        compiler_params=pltpu.CompilerParams(vmem_limit_bytes=8 << 20),
        name="ends",
    )(*(pltpu.with_memory_space_constraint(a, pltpu.HBM) for a in (f, table)))
    before, after = swap(pz, pz, "gz")
    fx, fy = local(faces_kernel, "faces", (EXT * SIDE, EXT * SIDE), f)
    message = (NEAR + 1) * SIDE
    ez, up, down = local(
        depth_kernel, "depth", (2 * SIDE, message, message), pz, before, after, fx, tables
    )
    before, after = swap(up, down, "gx")
    message = NEAR * PITCH + 3 * EXT
    xe, xee, yup, ydown = local(
        width_kernel, "width", (EXT * SIDE, SIDE, message, message), up, down, before, after, fy, ez, wy, tables
    )
    before, after = swap(yup, ydown, "gy")
    block = PITCH * PITCH
    v, qa, qb = local(
        prepare_kernel,
        "prepare",
        (block,) * 3,
        *(f, ez, xe, xee, spread),
    )
    coef, send, *_ = local(
        levels_kernel,
        "levels",
        (SIDE * SIDE, devices, block, block, block),
        *(yup, ydown, before, after, th, spread, v, qa, qb),
        aliases={6: 2, 7: 3, 8: 4},
    )
    send, spot, th = lax.optimization_barrier((send, spot, th))
    got = lax.all_to_all(send.reshape(devices, 1, LANES), ("gx", "gy", "gz"), 0, 0).reshape(devices, LANES)
    out, stats = pl.pallas_call(
        functools.partial(last_kernel, sizes=sizes, counts=counts),
        in_specs=[pl.BlockSpec(memory_space=pltpu.SMEM), here, here, here],
        out_specs=[there, there],
        out_shape=(shape(SIDE * SIDE, LANES), shape(2, 1, LEVELS)),
        scratch_shapes=[
            pltpu.VMEM((devices, LANES), F32),
            pltpu.VMEM((2 * SIDE, LANES), F32),
            pltpu.VMEM((2, 1, LEVELS), F32),
            pltpu.SemaphoreType.DMA((5,)),
        ],
        compiler_params=pltpu.CompilerParams(vmem_limit_bytes=8 << 20),
        name="last",
    )(spot, pinned(got), pinned(coef), pinned(th))
    return out.reshape(fields.shape), stats


def solution(mesh):
    placed = (P(None, "gx", "gy", "gz"), P())
    return jax.shard_map(shards, mesh=mesh, in_specs=placed, out_specs=placed, check_vma=False)
```

```python
import functools

import jax
import jax.numpy as jnp
import numpy as np
from jax import lax
from jax.experimental import pallas as pl
from jax.experimental.pallas import tpu as pltpu
from jax.sharding import PartitionSpec as P

NEAR = 4
LEVELS = 5
LANES = 128
SIDE = 32
EXT = 2 * NEAR
PITCH = SIDE + EXT
F32 = jnp.float32


def cascade(cells, ahead, behind):
    details, firsts = [], []
    for level in range(NEAR):
        half = len(cells) // 2
        following = cells[2::2] + [ahead[level]]
        detail = [cells[2 * k + 1] - 0.5 * (cells[2 * k] + following[k]) for k in range(half)]
        details.append(detail[-1])
        firsts.append(cells[0])
        before = [behind[level]] + detail[:-1]
        cells = [cells[2 * k] + 0.25 * (before[k] + detail[k]) for k in range(half)]
    return details, firsts


def end_weights(length):
    none = [np.zeros(length)] * NEAR
    details, firsts = cascade(list(np.eye(length)), none, none)
    return np.stack(details + firsts)


def seam_weights():
    zero = [np.zeros(1)] * NEAR
    flat = [np.zeros(1)] * SIDE
    alpha = np.zeros((NEAR, NEAR))
    beta = np.zeros((NEAR, NEAR))
    for j in range(NEAR):
        unit = [np.ones(1) * (k == j) for k in range(NEAR)]
        alpha[:, j] = [d[0] for d in cascade(flat, unit, zero)[0]]
        beta[:, j] = [f[0] for f in cascade(flat, zero, unit)[1]]
    lasts, firsts = [], []
    for level in range(NEAR):
        first = np.eye(EXT)[NEAR + level]
        for j in range(level):
            first = first + beta[level, j] * lasts[j]
        firsts.append(first)
        last = np.eye(EXT)[level]
        for j in range(level + 1):
            last = last + alpha[level, j] * firsts[j]
        lasts.append(last)
    return np.stack(lasts), np.stack(firsts)


W = end_weights(SIDE)
WZ = end_weights(LANES)
LAST, FIRST = seam_weights()
GROUP = LANES // EXT


def constant_tables():
    left = np.zeros((EXT, EXT))
    right = np.zeros((EXT, EXT))
    left[:, :NEAR] = LAST.T
    right[:, NEAR:] = FIRST.T
    spread = np.zeros((2, EXT, EXT))
    for level in range(NEAR):
        spread[0, level, EXT - (1 << level)] = 1.0
        spread[1, NEAR + level, EXT - (1 << level)] = 1.0
    each = np.eye(GROUP)
    solve = [np.kron(each, left), np.kron(each, right)]
    corner = np.zeros((2, LANES, LANES))
    corner[:, : EXT * EXT, : EXT * EXT] = [np.kron(left, np.eye(EXT)), np.kron(right, np.eye(EXT))]
    ends = []
    for half in range(2):
        end = np.zeros((LANES, LANES))
        end[:, : EXT * EXT] = np.kron(W[:, half * GROUP : (half + 1) * GROUP].T, np.eye(EXT))
        ends += [side @ end for side in solve]
    tables = np.concatenate(solve + ends + list(corner))
    spread = np.concatenate([np.kron(each, part) for part in spread], axis=1)
    return [t.astype(np.float32) for t in (np.tile(WZ.T, (1, GROUP)), tables, spread)]


SOLVE, ENDS, CORNER = (pl.ds(LANES * i, LANES * n) for i, n in ((0, 2), (2, 4), (6, 2)))


def dot(a, b):
    return jnp.dot(a, b, precision=lax.Precision.HIGHEST, preferred_element_type=F32)


def lanes_of(rows):
    return lax.broadcasted_iota(jnp.int32, (rows, LANES), 1)


def rows_of(rows):
    return lax.broadcasted_iota(jnp.int32, (rows, LANES), 0)


def roll(v, shift):
    return pltpu.roll(v, shift % LANES, 1)


def weighted(rows, load):
    sums = [None] * EXT
    for i in range(SIDE):
        block = load(i)
        for g in range(EXT):
            if W[g, i] != 0.0:
                term = float(W[g, i]) * block
                sums[g] = term if sums[g] is None else sums[g] + term
    return sums


def mix(weights, blocks):
    total = None
    for w, block in zip(weights, blocks):
        if w != 0.0:
            term = float(w) * block
            total = term if total is None else total + term
    return total


def ends_kernel(f, table, pz, block, weights, sem):
    copies = [pltpu.make_async_copy(f, block, sem.at[0]), pltpu.make_async_copy(table, weights, sem.at[1])]
    for copy in copies:
        copy.start()
    for copy in copies:
        copy.wait()
    out = dot(block[...], weights[...])
    group = lanes_of(SIDE) // EXT
    for half in range(2):
        packed = jnp.zeros((SIDE, LANES), F32)
        for j in range(GROUP):
            first = (half * GROUP + j) * SIDE
            packed = jnp.where(group == j, out[first : first + SIDE], packed)
        pz[pl.ds(half * SIDE, SIDE), :] = packed


def faces_kernel(f, fx, fy):
    for c in range(SIDE // 8):
        for g, block in enumerate(weighted(8, lambda x: f[pl.ds(x * SIDE + 8 * c, 8), :])):
            fx[pl.ds(g * SIDE + 8 * c, 8), :] = block
    for c in range(SIDE // 8):
        for g, block in enumerate(weighted(8, lambda y: f[pl.ds(8 * c * SIDE + y, 8, stride=SIDE), :])):
            fy[pl.ds(g * SIDE + 8 * c, 8), :] = block


def depth_kernel(pz, before, after, fx, tables, ez, up, down):
    near = lanes_of(2 * SIDE) % EXT < NEAR
    own = pz[...]
    sides = jnp.concatenate([jnp.where(near, before[...], own), jnp.where(near, own, after[...])], axis=1)
    fxe = dot(jnp.concatenate([sides[:SIDE], sides[SIDE:]], axis=1), tables[ENDS, :])
    ez[...] = dot(sides, tables[SOLVE, :])
    for g in range(NEAR):
        up[pl.ds(g * SIDE, SIDE), :] = fx[pl.ds(g * SIDE, SIDE), :]
        down[pl.ds(g * SIDE, SIDE), :] = fx[pl.ds((NEAR + g) * SIDE, SIDE), :]
    up[pl.ds(NEAR * SIDE, SIDE), :] = fxe
    down[pl.ds(NEAR * SIDE, SIDE), :] = fxe


def width_kernel(up, down, before, after, fy, ez, wy, tables, xe, xee, yup, ydown):
    for c in range(SIDE // 8):
        rows = [pl.ds(g * SIDE + 8 * c, 8) for g in range(NEAR)]
        own_last = [up[r, :] for r in rows]
        own_first = [down[r, :] for r in rows]
        seam_before = [before[r, :] for r in rows] + own_first
        seam_after = own_last + [after[r, :] for r in rows]
        for level in range(NEAR):
            xe[pl.ds(level * SIDE + 8 * c, 8), :] = mix(LAST[level], seam_before)
            xe[pl.ds((NEAR + level) * SIDE + 8 * c, 8), :] = mix(FIRST[level], seam_after)
    near = lanes_of(SIDE) // EXT < NEAR
    rows = pl.ds(NEAR * SIDE, SIDE)
    own = up[rows, :]
    sides = [jnp.where(near, before[rows, :], own), jnp.where(near, own, after[rows, :])]
    corner = dot(jnp.concatenate(sides, axis=1), tables[CORNER, :])
    xee[...] = corner
    sums = weighted(EXT, lambda y: xe[pl.ds(y, EXT, stride=SIDE), :])
    for g in range(EXT):
        target = yup if g < NEAR else ydown
        base = (g % NEAR) * PITCH
        target[pl.ds(base, SIDE), :] = fy[pl.ds(g * SIDE, SIDE), :]
        target[pl.ds(base + SIDE, EXT), :] = sums[g]
    for i, block in enumerate((ez[pl.ds(0, SIDE), :], ez[pl.ds(SIDE, SIDE), :], corner)):
        part = dot(wy[...], block)
        yup[pl.ds(NEAR * PITCH + i * EXT, EXT), :] = part
        ydown[pl.ds(NEAR * PITCH + i * EXT, EXT), :] = part


def lift_chunk(ref, at, level, masked):
    step = 1 << level
    pairs = SIDE // (2 * step)
    masked = masked and level > 0
    behind = ref[at(SIDE + level), :]
    even = ref[at(0), :]
    for k in range(pairs):
        odd = ref[at(step * (2 * k + 1)), :]
        ahead = ref[at(step * (2 * k + 2)), :] if k < pairs - 1 else ref[at(SIDE + NEAR + level), :]
        detail = odd - 0.5 * (even + ahead)
        smooth = even + 0.25 * (behind + detail)
        if masked:
            live = (lanes_of(odd.shape[0]) & (step - 1)) == 0
            detail, smooth = jnp.where(live, detail, odd), jnp.where(live, smooth, even)
        ref[at(step * (2 * k + 1)), :] = detail
        ref[at(2 * step * k), :] = smooth
        behind, even = detail, ahead


def chunks(level):
    step = 1 << level
    count = SIDE // step
    own = [(8 * step * c, min(8, count), step) for c in range(max(1, count // 8))]
    return own + ([(SIDE, EXT, 1)] if level < NEAR else [])


def lift_lanes(level, rows, v, qa, qb, keep=None):
    step = 1 << level
    lane = [lanes_of(count) for _, count in rows]
    last = [x == LANES - step for x in lane]
    cells = [v[at, :] for at, _ in rows]
    odd = [roll(c, -step) for c in cells]
    ahead = [roll(jnp.where(l, qb[at, :], o), -step) for (at, _), l, o in zip(rows, last, odd)]
    mid = [o - 0.5 * (c + a) for o, c, a in zip(odd, cells, ahead)]
    odd = [roll(m, step) for m in mid]
    behind = [roll(jnp.where(l, qa[at, :], o), step) for (at, _), l, o in zip(rows, last, odd)]
    for i, (at, _) in enumerate(rows):
        place = lane[i] & (2 * step - 1)
        smooth = cells[i] + 0.25 * (mid[i] + behind[i])
        lifted = jnp.where(place == 0, smooth, jnp.where(place == step, odd[i], cells[i]))
        mask = keep(i) if keep else None
        v[at, :] = lifted if mask is None else jnp.where(mask, cells[i], lifted)


def lane_rows(level, pieces):
    step = 1 << level
    planes = list(range(0, SIDE, step)) + (list(range(SIDE, PITCH)) if level < NEAR - 1 else [])
    return [
        (pl.ds(x * PITCH + first, count, stride=stride), count)
        for x in planes
        for first, count, stride in pieces
    ]


def lift_width(ref, level, masked, pieces):
    for first, count, stride in pieces:
        lift_chunk(ref, lambda i: pl.ds(i * PITCH + first, count, stride=stride), level, masked)


def prepare_kernel(f, ez, xe, xee, spread, v, qa, qb):
    for x in range(SIDE):
        v[pl.ds(x * PITCH, SIDE), :] = f[pl.ds(x * SIDE, SIDE), :]
    for g in range(EXT):
        v[pl.ds((SIDE + g) * PITCH, SIDE), :] = xe[pl.ds(g * SIDE, SIDE), :]
    block = jnp.concatenate([ez[...], xee[...]], axis=0)
    spread_lanes(qa, qb, 0, SIDE, block, spread)
    for ref in (v, qa, qb):
        lift_width(ref, 0, False, chunks(0)[:-1])
        for first, count, stride in chunks(0):

            def at(i):
                return pl.ds(first * PITCH + i, count, stride=stride * PITCH)

            even, behind = ref[at(0), :], None
            for k in range(SIDE // 2 - 1):
                ahead = ref[at(2 * k + 2), :]
                detail = ref[at(2 * k + 1), :] - 0.5 * (even + ahead)
                ref[at(2 * k + 1), :] = detail
                if k > 0:
                    ref[at(2 * k), :] = even + 0.25 * (behind + detail)
                even, behind = ahead, detail
    row8 = rows_of(8)
    waits = [row8 <= 1, None, None, row8 >= 5]
    lift_lanes(0, lane_rows(0, chunks(0)[:-1]), v, qa, qb, lambda i: waits[i % 4])


def spread_lanes(qa, qb, first, rows, block, spread):
    both = dot(block, spread[...])
    for x in range(PITCH):
        group, j = x // GROUP, x % GROUP
        for ref, part in ((qa, both[:, :LANES]), (qb, both[:, LANES:])):
            cells = part[group * rows : (group + 1) * rows]
            ref[pl.ds(x * PITCH + first, rows), :] = roll(cells, -EXT * (j + 1))


def stretch(v):
    lane = lanes_of(v.shape[0])
    for k in (2, 1, 0):
        spots = [16 * c - 15 * (c % (1 << k)) for c in range(8) if c >> k & 1]
        v = jnp.where(functools.reduce(jnp.logical_or, [lane == p for p in spots]), roll(v, 15 << k), v)
    return v


def close_height(ref):
    for first, count, stride in chunks(0):

        def at(i):
            return pl.ds(first * PITCH + i, count, stride=stride * PITCH)

        last, end = ref[at(SIDE - 2), :], ref[at(SIDE - 1), :]
        end = end - 0.5 * (last + ref[at(SIDE + NEAR), :])
        ref[at(SIDE - 1), :] = end
        ref[at(SIDE - 2), :] = last + 0.25 * (ref[at(SIDE - 3), :] + end)
        ref[at(0), :] = ref[at(0), :] + 0.25 * (ref[at(SIDE), :] + ref[at(1), :])


def levels_kernel(
    yup, ydown, before, after, th, spread, v_in, qa_in, qb_in, coef, send, v, qa, qb
):
    del v_in, qa_in, qb_in
    for c in range(PITCH // 8):
        rows = [pl.ds(g * PITCH + 8 * c, 8) for g in range(NEAR)]
        seam_before = [before[r, :] for r in rows] + [ydown[r, :] for r in rows]
        seam_after = [yup[r, :] for r in rows] + [after[r, :] for r in rows]
        for level in range(NEAR):
            v[pl.ds(8 * c * PITCH + SIDE + level, 8, stride=PITCH), :] = mix(LAST[level], seam_before)
            v[pl.ds(8 * c * PITCH + SIDE + NEAR + level, 8, stride=PITCH), :] = mix(FIRST[level], seam_after)
    row8 = rows_of(EXT)
    extras = []
    for i in range(3):
        first = NEAR * PITCH + i * EXT
        own = [yup[pl.ds(first + j, 1), :] for j in range(EXT)]
        seam_before = [before[pl.ds(first + j, 1), :] for j in range(NEAR)] + own[NEAR:]
        seam_after = own[:NEAR] + [after[pl.ds(first + NEAR + j, 1), :] for j in range(NEAR)]
        extra = jnp.zeros((EXT, LANES), F32)
        for level in range(NEAR):
            extra = jnp.where(row8 == level, mix(LAST[level], seam_before), extra)
            extra = jnp.where(row8 == NEAR + level, mix(FIRST[level], seam_after), extra)
        extras.append(extra)
    block = jnp.concatenate(extras, axis=0)
    spread_lanes(qa, qb, SIDE, EXT, block, spread)

    for level in range(NEAR):
        pieces = chunks(level)
        for ref in (v, qa, qb):
            lift_width(ref, level, ref is v, pieces[-1:] if level == 0 else pieces)
            if level == 0:
                close_height(ref)
                continue
            for first, count, stride in pieces:
                lift_chunk(
                    ref,
                    lambda i: pl.ds(first * PITCH + i, count, stride=stride * PITCH),
                    level,
                    ref is v,
                )
        if level == 0:
            rows = lane_rows(0, pieces[-1:])
            for y in (0, 1, SIDE - 3, SIDE - 2, SIDE - 1):
                rows += [(pl.ds(8 * c * PITCH + y, 8, stride=PITCH), 8) for c in range(PITCH // 8)]
        else:
            rows = lane_rows(level, pieces[: len(pieces) - (level == NEAR - 1)])
        lift_lanes(level, rows, v, qa, qb)

    energy = [jnp.zeros((8, LANES), F32)] * NEAR
    kept = [jnp.zeros((8, LANES), F32)] * NEAR
    for c in range(SIDE // 8):
        bits = (rows_of(8) + 8 * c) | lanes_of(8)
        own = [(bits & ((2 << level) - 1)) == (1 << level) for level in range(NEAR)]
        rest = [(bits & ((1 << level) - 1)) == 0 for level in range(NEAR)]
        bounds = []
        for depth in range(NEAR + 1):
            bound = jnp.broadcast_to(th[pl.ds(min(depth, NEAR - 1), 1), :], (8, LANES))
            for level in range(min(depth, NEAR - 1) - 1, -1, -1):
                bound = jnp.where(own[level], th[pl.ds(level, 1), :], bound)
            bounds.append(bound)
        squares = [None] * (NEAR + 1)
        sizes = [None] * (NEAR + 1)
        for x in range(SIDE):
            depth = NEAR if x == 0 else min(NEAR, (x & -x).bit_length() - 1)
            cells = v[pl.ds(x * PITCH + 8 * c, 8), :]
            shrunk = cells - jnp.minimum(jnp.maximum(cells, -bounds[depth]), bounds[depth])
            coef[pl.ds(x * SIDE + 8 * c, 8), :] = shrunk
            square, size = cells * cells, jnp.abs(shrunk)
            squares[depth] = square if squares[depth] is None else squares[depth] + square
            sizes[depth] = size if sizes[depth] is None else sizes[depth] + size
        for sums, target in ((squares, energy), (sizes, kept)):
            for level in range(NEAR):
                deeper = functools.reduce(lambda a, b: a + b, sums[level + 1 :])
                part = jnp.where(rest[level], sums[level], 0.0) + jnp.where(own[level], deeper, 0.0)
                target[level] = target[level] + part

    lane8 = lanes_of(8)
    block = jnp.zeros((8, LANES), F32)
    for i in range(4):
        block = jnp.where(row8 == i, v[pl.ds((i // 2 * PITCH + i % 2) * 16, 1), :], block)
    source, target = rows_of(LANES), lanes_of(LANES)
    pick = jnp.where((source == 16 * (target % 8)) & (target < 32), 1.0, 0.0).astype(F32)
    block = jnp.where(lane8 // 8 == row8, dot(block, pick), 0.0)
    for i, part in enumerate(energy + kept):
        block = jnp.where((lane8 == 32 + i) & (row8 == 0), jnp.sum(part), block)
    send[...] = jnp.broadcast_to(jnp.sum(block, axis=0, keepdims=True), send.shape)


def last_kernel(spot, got, coef, th, out, stats, grid, planes, sums_out, sem, *, sizes, counts):
    half = SIDE // 2
    copies = []
    for a in range(2):
        at = pl.ds((a * half + 1) * SIDE, (half - 1) * SIDE)
        copies.append(pltpu.make_async_copy(coef.at[at], out.at[at], sem.at[a]))
        copies[a].start()
        planes[pl.ds(a * SIDE, SIDE), :] = coef[pl.ds(a * half * SIDE, SIDE), :]
    nx, ny, nz = sizes
    plane = ny * nz
    lane, row = lanes_of(plane), rows_of(plane)
    v = [got[pl.ds(i * plane, plane), :] for i in range(nx)]
    sums = functools.reduce(lambda a, b: a + b, v)
    sums = jnp.sum(sums, axis=0, keepdims=True)

    def down(a, shift):
        return pltpu.roll(a, shift % plane, 0)

    odd = (lane & 16) != 0
    d = [v[i] - 0.5 * roll(v[i] + v[(i + 1) % nx], 16) for i in range(nx)]
    v = [jnp.where(odd, d[i], v[i] + 0.25 * roll(d[i] + d[i - 1], -16)) for i in range(nx)]
    odd = (lane & 8) != 0
    d = [a - 0.5 * roll(a + down(a, -nz), 8) for a in v]
    v = [jnp.where(odd, b, a + 0.25 * roll(b + down(b, nz), -8)) for a, b in zip(v, d)]
    odd = (lane & 1) != 0
    top, low = (lane & 7) == 7, (lane & 7) == 0
    far = row % nz == nz - 1
    near = row % nz == 0
    result = []
    for a in v:
        following = jnp.where(far, down(a, nz - 1), down(a, -1))
        d = a - 0.5 * (roll(a, 1) + jnp.where(top, roll(following, 7), roll(a, -1)))
        previous = jnp.where(near, down(d, 1 - nz), down(d, 1))
        s = a + 0.25 * (jnp.where(low, roll(previous, -7), roll(d, 1)) + roll(d, -1))
        result.append(jnp.where(odd, d, s))
    bound = th[pl.ds(LEVELS - 1, 1), :]
    detail = (lane < 32) & ((lane & 25) != 0)
    energy = kept = None
    for i, a in enumerate(result):
        shrunk = a - jnp.minimum(jnp.maximum(a, -bound), bound)
        grid[pl.ds(i * plane, plane), :] = jnp.where(detail, shrunk, a)
        square, size = jnp.where(detail, a * a, 0.0), jnp.where(detail, jnp.abs(shrunk), 0.0)
        energy = square if energy is None else energy + square
        kept = size if kept is None else kept + size
    own = grid[pl.ds(spot[0], 1), :]
    start = lanes_of(1) % 16 == 0
    for i in range(4):
        at = pl.ds(i * half, 1)
        planes[at, :] = jnp.where(start, stretch(roll(own, -8 * i)), planes[at, :])
    for a in range(2):
        target = out.at[pl.ds(a * half * SIDE, SIDE)]
        copies.append(pltpu.make_async_copy(planes.at[pl.ds(a * SIDE, SIDE)], target, sem.at[2 + a]))
        copies[2 + a].start()
    lane1 = lanes_of(1)
    for i, (part, base) in enumerate(((energy, 32), (kept, 36))):
        totals = jnp.where(lane1 == NEAR, jnp.sum(part), roll(sums, -base))
        scale = jnp.zeros((1, LANES), F32)
        for level in range(LEVELS):
            scale = jnp.where(lane1 == level, 1.0 / counts[level], scale)
        sums_out[i] = (totals * scale)[:, :LEVELS]
    copies.append(pltpu.make_async_copy(sums_out, stats, sem.at[4]))
    copies[4].start()
    for copy in copies:
        copy.wait()


def shape(*dims):
    return jax.ShapeDtypeStruct(dims, F32)


def shards(fields, exponents):
    sizes = tuple(lax.axis_size(a) for a in ("gx", "gy", "gz"))
    devices = sizes[0] * sizes[1] * sizes[2]
    cells = fields.size * devices
    counts = [7.0 * cells / 8 ** (level + 1) for level in range(LEVELS)]
    f = fields.reshape(SIDE * SIDE, LANES)
    th = jnp.broadcast_to(jnp.pad(jnp.exp2(exponents.astype(F32)), (0, 3))[:, None], (8, LANES))
    table, tables, spread = (jnp.asarray(t) for t in constant_tables())
    wy = jnp.asarray(W.astype(np.float32))

    def swap(up, down, axis):
        n = lax.axis_size(axis)
        before = lax.ppermute(up, axis, [(i, (i + 1) % n) for i in range(n)])
        after = lax.ppermute(down, axis, [((i + 1) % n, i) for i in range(n)])
        return before, after

    here = pl.BlockSpec(memory_space=pltpu.VMEM)
    there = pl.BlockSpec(memory_space=pltpu.HBM)

    def pinned(a):
        return pltpu.with_memory_space_constraint(a, pltpu.VMEM)

    def local(kernel, name, outs, *args, aliases={}):
        args = [pinned(a) for a in args]
        return pl.pallas_call(
            kernel,
            in_specs=[here] * len(args),
            out_specs=[here] * len(outs),
            out_shape=[pltpu.VMEM((rows, LANES), F32) for rows in outs],
            input_output_aliases=aliases,
            compiler_params=pltpu.CompilerParams(vmem_limit_bytes=8 << 20),
            name=name,
        )(*args)

    spot = lax.axis_index(("gx", "gy", "gz")).astype(jnp.int32).reshape(1)
    pz, f = pl.pallas_call(
        ends_kernel,
        in_specs=[there] * 2,
        out_specs=[here] * 2,
        out_shape=[pltpu.VMEM((2 * SIDE, LANES), F32), pltpu.VMEM((SIDE * SIDE, LANES), F32)],
        scratch_shapes=[pltpu.VMEM((LANES, LANES), F32), pltpu.SemaphoreType.DMA((2,))],
        compiler_params=pltpu.CompilerParams(vmem_limit_bytes=8 << 20),
        name="ends",
    )(*(pltpu.with_memory_space_constraint(a, pltpu.HBM) for a in (f, table)))
    before, after = swap(pz, pz, "gz")
    fx, fy = local(faces_kernel, "faces", (EXT * SIDE, EXT * SIDE), f)
    message = (NEAR + 1) * SIDE
    ez, up, down = local(
        depth_kernel, "depth", (2 * SIDE, message, message), pz, before, after, fx, tables
    )
    before, after = swap(up, down, "gx")
    message = NEAR * PITCH + 3 * EXT
    xe, xee, yup, ydown = local(
        width_kernel, "width", (EXT * SIDE, SIDE, message, message), up, down, before, after, fy, ez, wy, tables
    )
    before, after = swap(yup, ydown, "gy")
    block = PITCH * PITCH
    v, qa, qb = local(
        prepare_kernel,
        "prepare",
        (block,) * 3,
        *(f, ez, xe, xee, spread),
    )
    coef, send, *_ = local(
        levels_kernel,
        "levels",
        (SIDE * SIDE, devices, block, block, block),
        *(yup, ydown, before, after, th, spread, v, qa, qb),
        aliases={6: 2, 7: 3, 8: 4},
    )
    send, spot, th = lax.optimization_barrier((send, spot, th))
    got = lax.all_to_all(send.reshape(devices, 1, LANES), ("gx", "gy", "gz"), 0, 0).reshape(devices, LANES)
    out, stats = pl.pallas_call(
        functools.partial(last_kernel, sizes=sizes, counts=counts),
        in_specs=[pl.BlockSpec(memory_space=pltpu.SMEM), here, here, here],
        out_specs=[there, there],
        out_shape=(shape(SIDE * SIDE, LANES), shape(2, 1, LEVELS)),
        scratch_shapes=[
            pltpu.VMEM((devices, LANES), F32),
            pltpu.VMEM((2 * SIDE, LANES), F32),
            pltpu.VMEM((2, 1, LEVELS), F32),
            pltpu.SemaphoreType.DMA((5,)),
        ],
        compiler_params=pltpu.CompilerParams(vmem_limit_bytes=8 << 20),
        name="last",
    )(spot, pinned(got), pinned(coef), pinned(th))
    return out.reshape(fields.shape), stats


def solution(mesh):
    placed = (P(None, "gx", "gy", "gz"), P())
    return jax.shard_map(shards, mesh=mesh, in_specs=placed, out_specs=placed, check_vma=False)
```

```python
import functools

import jax
import jax.numpy as jnp
import numpy as np
from jax import lax
from jax.experimental import pallas as pl
from jax.experimental.pallas import tpu as pltpu
from jax.sharding import PartitionSpec as P

NEAR = 4
LEVELS = 5
LANES = 128
SIDE = 32
EXT = 2 * NEAR
PITCH = SIDE + EXT
F32 = jnp.float32


def cascade(cells, ahead, behind):
    details, firsts = [], []
    for level in range(NEAR):
        half = len(cells) // 2
        following = cells[2::2] + [ahead[level]]
        detail = [cells[2 * k + 1] - 0.5 * (cells[2 * k] + following[k]) for k in range(half)]
        details.append(detail[-1])
        firsts.append(cells[0])
        before = [behind[level]] + detail[:-1]
        cells = [cells[2 * k] + 0.25 * (before[k] + detail[k]) for k in range(half)]
    return details, firsts


def end_weights(length):
    none = [np.zeros(length)] * NEAR
    details, firsts = cascade(list(np.eye(length)), none, none)
    return np.stack(details + firsts)


def seam_weights():
    zero = [np.zeros(1)] * NEAR
    flat = [np.zeros(1)] * SIDE
    alpha = np.zeros((NEAR, NEAR))
    beta = np.zeros((NEAR, NEAR))
    for j in range(NEAR):
        unit = [np.ones(1) * (k == j) for k in range(NEAR)]
        alpha[:, j] = [d[0] for d in cascade(flat, unit, zero)[0]]
        beta[:, j] = [f[0] for f in cascade(flat, zero, unit)[1]]
    lasts, firsts = [], []
    for level in range(NEAR):
        first = np.eye(EXT)[NEAR + level]
        for j in range(level):
            first = first + beta[level, j] * lasts[j]
        firsts.append(first)
        last = np.eye(EXT)[level]
        for j in range(level + 1):
            last = last + alpha[level, j] * firsts[j]
        lasts.append(last)
    return np.stack(lasts), np.stack(firsts)


W = end_weights(SIDE)
WZ = end_weights(LANES)
LAST, FIRST = seam_weights()
GROUP = LANES // EXT


def constant_tables():
    left = np.zeros((EXT, EXT))
    right = np.zeros((EXT, EXT))
    left[:, :NEAR] = LAST.T
    right[:, NEAR:] = FIRST.T
    spread = np.zeros((2, EXT, EXT))
    for level in range(NEAR):
        spread[0, level, EXT - (1 << level)] = 1.0
        spread[1, NEAR + level, EXT - (1 << level)] = 1.0
    each = np.eye(GROUP)
    solve = [np.kron(each, left), np.kron(each, right)]
    corner = np.zeros((2, LANES, LANES))
    corner[:, : EXT * EXT, : EXT * EXT] = [np.kron(left, np.eye(EXT)), np.kron(right, np.eye(EXT))]
    ends = []
    for half in range(2):
        end = np.zeros((LANES, LANES))
        end[:, : EXT * EXT] = np.kron(W[:, half * GROUP : (half + 1) * GROUP].T, np.eye(EXT))
        ends += [side @ end for side in solve]
    tables = np.concatenate(solve + ends + list(corner))
    spread = np.concatenate([np.kron(each, part) for part in spread], axis=1)
    return [t.astype(np.float32) for t in (np.tile(WZ.T, (1, GROUP)), tables, spread)]


SOLVE, ENDS, CORNER = (pl.ds(LANES * i, LANES * n) for i, n in ((0, 2), (2, 4), (6, 2)))


def dot(a, b):
    return jnp.dot(a, b, precision=lax.Precision.HIGHEST, preferred_element_type=F32)


def lanes_of(rows):
    return lax.broadcasted_iota(jnp.int32, (rows, LANES), 1)


def rows_of(rows):
    return lax.broadcasted_iota(jnp.int32, (rows, LANES), 0)


def roll(v, shift):
    return pltpu.roll(v, shift % LANES, 1)


def weighted(rows, load):
    sums = [None] * EXT
    for i in range(SIDE):
        block = load(i)
        for g in range(EXT):
            if W[g, i] != 0.0:
                term = float(W[g, i]) * block
                sums[g] = term if sums[g] is None else sums[g] + term
    return sums


def mix(weights, blocks):
    total = None
    for w, block in zip(weights, blocks):
        if w != 0.0:
            term = float(w) * block
            total = term if total is None else total + term
    return total


def ends_kernel(f, table, pz, block, weights, sem):
    copies = [pltpu.make_async_copy(f, block, sem.at[0]), pltpu.make_async_copy(table, weights, sem.at[1])]
    for copy in copies:
        copy.start()
    for copy in copies:
        copy.wait()
    out = dot(block[...], weights[...])
    group = lanes_of(SIDE) // EXT
    for half in range(2):
        packed = jnp.zeros((SIDE, LANES), F32)
        for j in range(GROUP):
            first = (half * GROUP + j) * SIDE
            packed = jnp.where(group == j, out[first : first + SIDE], packed)
        pz[pl.ds(half * SIDE, SIDE), :] = packed


def faces_kernel(f, fx, fy):
    for c in range(SIDE // 8):
        for g, block in enumerate(weighted(8, lambda x: f[pl.ds(x * SIDE + 8 * c, 8), :])):
            fx[pl.ds(g * SIDE + 8 * c, 8), :] = block
    for c in range(SIDE // 8):
        for g, block in enumerate(weighted(8, lambda y: f[pl.ds(8 * c * SIDE + y, 8, stride=SIDE), :])):
            fy[pl.ds(g * SIDE + 8 * c, 8), :] = block


def depth_kernel(pz, before, after, fx, tables, ez, up, down):
    near = lanes_of(2 * SIDE) % EXT < NEAR
    own = pz[...]
    sides = jnp.concatenate([jnp.where(near, before[...], own), jnp.where(near, own, after[...])], axis=1)
    fxe = dot(jnp.concatenate([sides[:SIDE], sides[SIDE:]], axis=1), tables[ENDS, :])
    ez[...] = dot(sides, tables[SOLVE, :])
    for g in range(NEAR):
        up[pl.ds(g * SIDE, SIDE), :] = fx[pl.ds(g * SIDE, SIDE), :]
        down[pl.ds(g * SIDE, SIDE), :] = fx[pl.ds((NEAR + g) * SIDE, SIDE), :]
    up[pl.ds(NEAR * SIDE, SIDE), :] = fxe
    down[pl.ds(NEAR * SIDE, SIDE), :] = fxe


def width_kernel(up, down, before, after, fy, ez, wy, tables, xe, xee, yup, ydown):
    for c in range(SIDE // 8):
        rows = [pl.ds(g * SIDE + 8 * c, 8) for g in range(NEAR)]
        own_last = [up[r, :] for r in rows]
        own_first = [down[r, :] for r in rows]
        seam_before = [before[r, :] for r in rows] + own_first
        seam_after = own_last + [after[r, :] for r in rows]
        for level in range(NEAR):
            xe[pl.ds(level * SIDE + 8 * c, 8), :] = mix(LAST[level], seam_before)
            xe[pl.ds((NEAR + level) * SIDE + 8 * c, 8), :] = mix(FIRST[level], seam_after)
    near = lanes_of(SIDE) // EXT < NEAR
    rows = pl.ds(NEAR * SIDE, SIDE)
    own = up[rows, :]
    sides = [jnp.where(near, before[rows, :], own), jnp.where(near, own, after[rows, :])]
    corner = dot(jnp.concatenate(sides, axis=1), tables[CORNER, :])
    xee[...] = corner
    sums = weighted(EXT, lambda y: xe[pl.ds(y, EXT, stride=SIDE), :])
    for g in range(EXT):
        target = yup if g < NEAR else ydown
        base = (g % NEAR) * PITCH
        target[pl.ds(base, SIDE), :] = fy[pl.ds(g * SIDE, SIDE), :]
        target[pl.ds(base + SIDE, EXT), :] = sums[g]
    for i, block in enumerate((ez[pl.ds(0, SIDE), :], ez[pl.ds(SIDE, SIDE), :], corner)):
        part = dot(wy[...], block)
        yup[pl.ds(NEAR * PITCH + i * EXT, EXT), :] = part
        ydown[pl.ds(NEAR * PITCH + i * EXT, EXT), :] = part


def lift_chunk(ref, at, level, masked):
    step = 1 << level
    pairs = SIDE // (2 * step)
    masked = masked and level > 0
    behind = ref[at(SIDE + level), :]
    even = ref[at(0), :]
    for k in range(pairs):
        odd = ref[at(step * (2 * k + 1)), :]
        ahead = ref[at(step * (2 * k + 2)), :] if k < pairs - 1 else ref[at(SIDE + NEAR + level), :]
        detail = odd - 0.5 * (even + ahead)
        smooth = even + 0.25 * (behind + detail)
        if masked:
            live = (lanes_of(odd.shape[0]) & (step - 1)) == 0
            detail, smooth = jnp.where(live, detail, odd), jnp.where(live, smooth, even)
        ref[at(step * (2 * k + 1)), :] = detail
        ref[at(2 * step * k), :] = smooth
        behind, even = detail, ahead


def chunks(level):
    step = 1 << level
    count = SIDE // step
    own = [(8 * step * c, min(8, count), step) for c in range(max(1, count // 8))]
    return own + ([(SIDE, EXT, 1)] if level < NEAR else [])


def lift_lanes(level, rows, v, qa, qb, keep=None):
    step = 1 << level
    lane = [lanes_of(count) for _, count in rows]
    last = [x == LANES - step for x in lane]
    cells = [v[at, :] for at, _ in rows]
    odd = [roll(c, -step) for c in cells]
    ahead = [roll(jnp.where(l, qb[at, :], o), -step) for (at, _), l, o in zip(rows, last, odd)]
    mid = [o - 0.5 * (c + a) for o, c, a in zip(odd, cells, ahead)]
    odd = [roll(m, step) for m in mid]
    behind = [roll(jnp.where(l, qa[at, :], o), step) for (at, _), l, o in zip(rows, last, odd)]
    for i, (at, _) in enumerate(rows):
        place = lane[i] & (2 * step - 1)
        smooth = cells[i] + 0.25 * (mid[i] + behind[i])
        lifted = jnp.where(place == 0, smooth, jnp.where(place == step, odd[i], cells[i]))
        mask = keep(i) if keep else None
        v[at, :] = lifted if mask is None else jnp.where(mask, cells[i], lifted)


def lane_rows(level, pieces):
    step = 1 << level
    planes = list(range(0, SIDE, step)) + (list(range(SIDE, PITCH)) if level < NEAR - 1 else [])
    return [
        (pl.ds(x * PITCH + first, count, stride=stride), count)
        for x in planes
        for first, count, stride in pieces
    ]


def lift_width(ref, level, masked, pieces):
    for first, count, stride in pieces:
        lift_chunk(ref, lambda i: pl.ds(i * PITCH + first, count, stride=stride), level, masked)


def prepare_kernel(f, ez, xe, xee, spread, v, qa, qb):
    for x in range(SIDE):
        v[pl.ds(x * PITCH, SIDE), :] = f[pl.ds(x * SIDE, SIDE), :]
    for g in range(EXT):
        v[pl.ds((SIDE + g) * PITCH, SIDE), :] = xe[pl.ds(g * SIDE, SIDE), :]
    block = jnp.concatenate([ez[...], xee[...]], axis=0)
    spread_lanes(qa, qb, 0, SIDE, block, spread)
    for ref in (v, qa, qb):
        lift_width(ref, 0, False, chunks(0)[:-1])
        for first, count, stride in chunks(0):

            def at(i):
                return pl.ds(first * PITCH + i, count, stride=stride * PITCH)

            even, behind = ref[at(0), :], None
            for k in range(SIDE // 2 - 1):
                ahead = ref[at(2 * k + 2), :]
                detail = ref[at(2 * k + 1), :] - 0.5 * (even + ahead)
                ref[at(2 * k + 1), :] = detail
                if k > 0:
                    ref[at(2 * k), :] = even + 0.25 * (behind + detail)
                even, behind = ahead, detail
    row8 = rows_of(8)
    waits = [row8 <= 1, None, None, row8 >= 5]
    lift_lanes(0, lane_rows(0, chunks(0)[:-1]), v, qa, qb, lambda i: waits[i % 4])


def spread_lanes(qa, qb, first, rows, block, spread):
    both = dot(block, spread[...])
    for x in range(PITCH):
        group, j = x // GROUP, x % GROUP
        for ref, part in ((qa, both[:, :LANES]), (qb, both[:, LANES:])):
            cells = part[group * rows : (group + 1) * rows]
            ref[pl.ds(x * PITCH + first, rows), :] = roll(cells, -EXT * (j + 1))


def stretch(v):
    lane = lanes_of(v.shape[0])
    for k in (2, 1, 0):
        spots = [16 * c - 15 * (c % (1 << k)) for c in range(8) if c >> k & 1]
        v = jnp.where(functools.reduce(jnp.logical_or, [lane == p for p in spots]), roll(v, 15 << k), v)
    return v


def close_height(ref):
    for first, count, stride in chunks(0):

        def at(i):
            return pl.ds(first * PITCH + i, count, stride=stride * PITCH)

        last, end = ref[at(SIDE - 2), :], ref[at(SIDE - 1), :]
        end = end - 0.5 * (last + ref[at(SIDE + NEAR), :])
        ref[at(SIDE - 1), :] = end
        ref[at(SIDE - 2), :] = last + 0.25 * (ref[at(SIDE - 3), :] + end)
        ref[at(0), :] = ref[at(0), :] + 0.25 * (ref[at(SIDE), :] + ref[at(1), :])


def levels_kernel(
    yup, ydown, before, after, th, spread, v_in, qa_in, qb_in, coef, send, v, qa, qb
):
    del v_in, qa_in, qb_in
    for c in range(PITCH // 8):
        rows = [pl.ds(g * PITCH + 8 * c, 8) for g in range(NEAR)]
        seam_before = [before[r, :] for r in rows] + [ydown[r, :] for r in rows]
        seam_after = [yup[r, :] for r in rows] + [after[r, :] for r in rows]
        for level in range(NEAR):
            v[pl.ds(8 * c * PITCH + SIDE + level, 8, stride=PITCH), :] = mix(LAST[level], seam_before)
            v[pl.ds(8 * c * PITCH + SIDE + NEAR + level, 8, stride=PITCH), :] = mix(FIRST[level], seam_after)
    row8 = rows_of(EXT)
    extras = []
    for i in range(3):
        first = NEAR * PITCH + i * EXT
        own = [yup[pl.ds(first + j, 1), :] for j in range(EXT)]
        seam_before = [before[pl.ds(first + j, 1), :] for j in range(NEAR)] + own[NEAR:]
        seam_after = own[:NEAR] + [after[pl.ds(first + NEAR + j, 1), :] for j in range(NEAR)]
        extra = jnp.zeros((EXT, LANES), F32)
        for level in range(NEAR):
            extra = jnp.where(row8 == level, mix(LAST[level], seam_before), extra)
            extra = jnp.where(row8 == NEAR + level, mix(FIRST[level], seam_after), extra)
        extras.append(extra)
    block = jnp.concatenate(extras, axis=0)
    spread_lanes(qa, qb, SIDE, EXT, block, spread)

    for level in range(NEAR):
        pieces = chunks(level)
        for ref in (v, qa, qb):
            lift_width(ref, level, ref is v, pieces[-1:] if level == 0 else pieces)
            if level == 0:
                close_height(ref)
                continue
            for first, count, stride in pieces:
                lift_chunk(
                    ref,
                    lambda i: pl.ds(first * PITCH + i, count, stride=stride * PITCH),
                    level,
                    ref is v,
                )
        if level == 0:
            rows = lane_rows(0, pieces[-1:])
            for y in (0, 1, SIDE - 3, SIDE - 2, SIDE - 1):
                rows += [(pl.ds(8 * c * PITCH + y, 8, stride=PITCH), 8) for c in range(PITCH // 8)]
        else:
            rows = lane_rows(level, pieces[: len(pieces) - (level == NEAR - 1)])
        lift_lanes(level, rows, v, qa, qb)

    energy = [jnp.zeros((8, LANES), F32)] * NEAR
    kept = [jnp.zeros((8, LANES), F32)] * NEAR
    for c in range(SIDE // 8):
        bits = (rows_of(8) + 8 * c) | lanes_of(8)
        own = [(bits & ((2 << level) - 1)) == (1 << level) for level in range(NEAR)]
        rest = [(bits & ((1 << level) - 1)) == 0 for level in range(NEAR)]
        bounds = []
        for depth in range(NEAR + 1):
            bound = jnp.broadcast_to(th[pl.ds(min(depth, NEAR - 1), 1), :], (8, LANES))
            for level in range(min(depth, NEAR - 1) - 1, -1, -1):
                bound = jnp.where(own[level], th[pl.ds(level, 1), :], bound)
            bounds.append(bound)
        squares = [None] * (NEAR + 1)
        sizes = [None] * (NEAR + 1)
        for x in range(SIDE):
            depth = NEAR if x == 0 else min(NEAR, (x & -x).bit_length() - 1)
            cells = v[pl.ds(x * PITCH + 8 * c, 8), :]
            shrunk = cells - jnp.minimum(jnp.maximum(cells, -bounds[depth]), bounds[depth])
            coef[pl.ds(x * SIDE + 8 * c, 8), :] = shrunk
            square, size = cells * cells, jnp.abs(shrunk)
            squares[depth] = square if squares[depth] is None else squares[depth] + square
            sizes[depth] = size if sizes[depth] is None else sizes[depth] + size
        for sums, target in ((squares, energy), (sizes, kept)):
            for level in range(NEAR):
                deeper = functools.reduce(lambda a, b: a + b, sums[level + 1 :])
                part = jnp.where(rest[level], sums[level], 0.0) + jnp.where(own[level], deeper, 0.0)
                target[level] = target[level] + part

    lane8 = lanes_of(8)
    block = jnp.zeros((8, LANES), F32)
    for i in range(4):
        block = jnp.where(row8 == i, v[pl.ds((i // 2 * PITCH + i % 2) * 16, 1), :], block)
    source, target = rows_of(LANES), lanes_of(LANES)
    pick = jnp.where((source == 16 * (target % 8)) & (target < 32), 1.0, 0.0).astype(F32)
    block = jnp.where(lane8 // 8 == row8, dot(block, pick), 0.0)
    for i, part in enumerate(energy + kept):
        block = jnp.where((lane8 == 32 + i) & (row8 == 0), jnp.sum(part), block)
    send[...] = jnp.broadcast_to(jnp.sum(block, axis=0, keepdims=True), send.shape)


def last_kernel(spot, got, coef, th, out, stats, grid, planes, sums_out, sem, *, sizes, counts):
    half = SIDE // 2
    copies = []
    for a in range(2):
        at = pl.ds((a * half + 1) * SIDE, (half - 1) * SIDE)
        copies.append(pltpu.make_async_copy(coef.at[at], out.at[at], sem.at[a]))
        copies[a].start()
        planes[pl.ds(a * SIDE, SIDE), :] = coef[pl.ds(a * half * SIDE, SIDE), :]
    nx, ny, nz = sizes
    plane = ny * nz
    lane, row = lanes_of(plane), rows_of(plane)
    v = [got[pl.ds(i * plane, plane), :] for i in range(nx)]
    sums = functools.reduce(lambda a, b: a + b, v)
    sums = jnp.sum(sums, axis=0, keepdims=True)

    def down(a, shift):
        return pltpu.roll(a, shift % plane, 0)

    odd = (lane & 16) != 0
    d = [v[i] - 0.5 * roll(v[i] + v[(i + 1) % nx], 16) for i in range(nx)]
    v = [jnp.where(odd, d[i], v[i] + 0.25 * roll(d[i] + d[i - 1], -16)) for i in range(nx)]
    odd = (lane & 8) != 0
    d = [a - 0.5 * roll(a + down(a, -nz), 8) for a in v]
    v = [jnp.where(odd, b, a + 0.25 * roll(b + down(b, nz), -8)) for a, b in zip(v, d)]
    odd = (lane & 1) != 0
    top, low = (lane & 7) == 7, (lane & 7) == 0
    far = row % nz == nz - 1
    near = row % nz == 0
    left = [roll(a, 1) for a in v]
    right = [roll(a, -1) for a in v]
    wrap = [roll(jnp.where(far, down(a, nz - 1), down(a, -1)), 7) for a in v]
    d = [a - 0.5 * (x + jnp.where(top, w, y)) for a, x, y, w in zip(v, left, right, wrap)]
    right = [roll(a, -1) for a in d]
    left = [roll(a, 1) for a in d]
    wrap = [roll(jnp.where(near, down(a, 1 - nz), down(a, 1)), -7) for a in d]
    result = [
        jnp.where(odd, b, a + 0.25 * (jnp.where(low, w, x) + y))
        for a, b, x, y, w in zip(v, d, left, right, wrap)
    ]
    bound = th[pl.ds(LEVELS - 1, 1), :]
    detail = (lane < 32) & ((lane & 25) != 0)
    energy = kept = None
    for i, a in enumerate(result):
        shrunk = a - jnp.minimum(jnp.maximum(a, -bound), bound)
        grid[pl.ds(i * plane, plane), :] = jnp.where(detail, shrunk, a)
        square, size = jnp.where(detail, a * a, 0.0), jnp.where(detail, jnp.abs(shrunk), 0.0)
        energy = square if energy is None else energy + square
        kept = size if kept is None else kept + size
    own = grid[pl.ds(spot[0], 1), :]
    start = lanes_of(1) % 16 == 0
    for i in range(4):
        at = pl.ds(i * half, 1)
        planes[at, :] = jnp.where(start, stretch(roll(own, -8 * i)), planes[at, :])
    for a in range(2):
        target = out.at[pl.ds(a * half * SIDE, SIDE)]
        copies.append(pltpu.make_async_copy(planes.at[pl.ds(a * SIDE, SIDE)], target, sem.at[2 + a]))
        copies[2 + a].start()
    lane1 = lanes_of(1)
    for i, (part, base) in enumerate(((energy, 32), (kept, 36))):
        totals = jnp.where(lane1 == NEAR, jnp.sum(part), roll(sums, -base))
        scale = jnp.zeros((1, LANES), F32)
        for level in range(LEVELS):
            scale = jnp.where(lane1 == level, 1.0 / counts[level], scale)
        sums_out[i] = (totals * scale)[:, :LEVELS]
    copies.append(pltpu.make_async_copy(sums_out, stats, sem.at[4]))
    copies[4].start()
    for copy in copies:
        copy.wait()


def shape(*dims):
    return jax.ShapeDtypeStruct(dims, F32)


def shards(fields, exponents):
    sizes = tuple(lax.axis_size(a) for a in ("gx", "gy", "gz"))
    devices = sizes[0] * sizes[1] * sizes[2]
    cells = fields.size * devices
    counts = [7.0 * cells / 8 ** (level + 1) for level in range(LEVELS)]
    f = fields.reshape(SIDE * SIDE, LANES)
    th = jnp.broadcast_to(jnp.pad(jnp.exp2(exponents.astype(F32)), (0, 3))[:, None], (8, LANES))
    table, tables, spread = (jnp.asarray(t) for t in constant_tables())
    wy = jnp.asarray(W.astype(np.float32))

    def swap(up, down, axis):
        n = lax.axis_size(axis)
        before = lax.ppermute(up, axis, [(i, (i + 1) % n) for i in range(n)])
        after = lax.ppermute(down, axis, [((i + 1) % n, i) for i in range(n)])
        return before, after

    here = pl.BlockSpec(memory_space=pltpu.VMEM)
    there = pl.BlockSpec(memory_space=pltpu.HBM)

    def pinned(a):
        return pltpu.with_memory_space_constraint(a, pltpu.VMEM)

    def local(kernel, name, outs, *args, aliases={}):
        args = [pinned(a) for a in args]
        return pl.pallas_call(
            kernel,
            in_specs=[here] * len(args),
            out_specs=[here] * len(outs),
            out_shape=[pltpu.VMEM((rows, LANES), F32) for rows in outs],
            input_output_aliases=aliases,
            compiler_params=pltpu.CompilerParams(vmem_limit_bytes=8 << 20),
            name=name,
        )(*args)

    spot = lax.axis_index(("gx", "gy", "gz")).astype(jnp.int32).reshape(1)
    pz, f = pl.pallas_call(
        ends_kernel,
        in_specs=[there] * 2,
        out_specs=[here] * 2,
        out_shape=[pltpu.VMEM((2 * SIDE, LANES), F32), pltpu.VMEM((SIDE * SIDE, LANES), F32)],
        scratch_shapes=[pltpu.VMEM((LANES, LANES), F32), pltpu.SemaphoreType.DMA((2,))],
        compiler_params=pltpu.CompilerParams(vmem_limit_bytes=8 << 20),
        name="ends",
    )(*(pltpu.with_memory_space_constraint(a, pltpu.HBM) for a in (f, table)))
    before, after = swap(pz, pz, "gz")
    fx, fy = local(faces_kernel, "faces", (EXT * SIDE, EXT * SIDE), f)
    message = (NEAR + 1) * SIDE
    ez, up, down = local(
        depth_kernel, "depth", (2 * SIDE, message, message), pz, before, after, fx, tables
    )
    before, after = swap(up, down, "gx")
    message = NEAR * PITCH + 3 * EXT
    xe, xee, yup, ydown = local(
        width_kernel, "width", (EXT * SIDE, SIDE, message, message), up, down, before, after, fy, ez, wy, tables
    )
    before, after = swap(yup, ydown, "gy")
    block = PITCH * PITCH
    v, qa, qb = local(
        prepare_kernel,
        "prepare",
        (block,) * 3,
        *(f, ez, xe, xee, spread),
    )
    coef, send, *_ = local(
        levels_kernel,
        "levels",
        (SIDE * SIDE, devices, block, block, block),
        *(yup, ydown, before, after, th, spread, v, qa, qb),
        aliases={6: 2, 7: 3, 8: 4},
    )
    send, spot, th = lax.optimization_barrier((send, spot, th))
    got = lax.all_to_all(send.reshape(devices, 1, LANES), ("gx", "gy", "gz"), 0, 0).reshape(devices, LANES)
    out, stats = pl.pallas_call(
        functools.partial(last_kernel, sizes=sizes, counts=counts),
        in_specs=[pl.BlockSpec(memory_space=pltpu.SMEM), here, here, here],
        out_specs=[there, there],
        out_shape=(shape(SIDE * SIDE, LANES), shape(2, 1, LEVELS)),
        scratch_shapes=[
            pltpu.VMEM((devices, LANES), F32),
            pltpu.VMEM((2 * SIDE, LANES), F32),
            pltpu.VMEM((2, 1, LEVELS), F32),
            pltpu.SemaphoreType.DMA((5,)),
        ],
        compiler_params=pltpu.CompilerParams(vmem_limit_bytes=8 << 20),
        name="last",
    )(spot, pinned(got), pinned(coef), pinned(th))
    return out.reshape(fields.shape), stats


def solution(mesh):
    placed = (P(None, "gx", "gy", "gz"), P())
    return jax.shard_map(shards, mesh=mesh, in_specs=placed, out_specs=placed, check_vma=False)
```

```python
import functools

import jax
import jax.numpy as jnp
import numpy as np
from jax import lax
from jax.experimental import pallas as pl
from jax.experimental.pallas import tpu as pltpu
from jax.sharding import PartitionSpec as P

NEAR = 4
LEVELS = 5
LANES = 128
SIDE = 32
EXT = 2 * NEAR
PITCH = SIDE + EXT
F32 = jnp.float32


def cascade(cells, ahead, behind):
    details, firsts = [], []
    for level in range(NEAR):
        half = len(cells) // 2
        following = cells[2::2] + [ahead[level]]
        detail = [cells[2 * k + 1] - 0.5 * (cells[2 * k] + following[k]) for k in range(half)]
        details.append(detail[-1])
        firsts.append(cells[0])
        before = [behind[level]] + detail[:-1]
        cells = [cells[2 * k] + 0.25 * (before[k] + detail[k]) for k in range(half)]
    return details, firsts


def end_weights(length):
    none = [np.zeros(length)] * NEAR
    details, firsts = cascade(list(np.eye(length)), none, none)
    return np.stack(details + firsts)


def seam_weights():
    zero = [np.zeros(1)] * NEAR
    flat = [np.zeros(1)] * SIDE
    alpha = np.zeros((NEAR, NEAR))
    beta = np.zeros((NEAR, NEAR))
    for j in range(NEAR):
        unit = [np.ones(1) * (k == j) for k in range(NEAR)]
        alpha[:, j] = [d[0] for d in cascade(flat, unit, zero)[0]]
        beta[:, j] = [f[0] for f in cascade(flat, zero, unit)[1]]
    lasts, firsts = [], []
    for level in range(NEAR):
        first = np.eye(EXT)[NEAR + level]
        for j in range(level):
            first = first + beta[level, j] * lasts[j]
        firsts.append(first)
        last = np.eye(EXT)[level]
        for j in range(level + 1):
            last = last + alpha[level, j] * firsts[j]
        lasts.append(last)
    return np.stack(lasts), np.stack(firsts)


W = end_weights(SIDE)
WZ = end_weights(LANES)
LAST, FIRST = seam_weights()
GROUP = LANES // EXT


def constant_tables():
    left = np.zeros((EXT, EXT))
    right = np.zeros((EXT, EXT))
    left[:, :NEAR] = LAST.T
    right[:, NEAR:] = FIRST.T
    spread = np.zeros((2, EXT, EXT))
    for level in range(NEAR):
        spread[0, level, EXT - (1 << level)] = 1.0
        spread[1, NEAR + level, EXT - (1 << level)] = 1.0
    each = np.eye(GROUP)
    solve = [np.kron(each, left), np.kron(each, right)]
    corner = np.zeros((2, LANES, LANES))
    corner[:, : EXT * EXT, : EXT * EXT] = [np.kron(left, np.eye(EXT)), np.kron(right, np.eye(EXT))]
    ends = []
    for half in range(2):
        end = np.zeros((LANES, LANES))
        end[:, : EXT * EXT] = np.kron(W[:, half * GROUP : (half + 1) * GROUP].T, np.eye(EXT))
        ends += [side @ end for side in solve]
    tables = np.concatenate(solve + ends + list(corner))
    spread = np.concatenate([np.kron(each, part) for part in spread], axis=1)
    return [t.astype(np.float32) for t in (np.tile(WZ.T, (1, GROUP)), tables, spread)]


SOLVE, ENDS, CORNER = (pl.ds(LANES * i, LANES * n) for i, n in ((0, 2), (2, 4), (6, 2)))


def dot(a, b):
    return jnp.dot(a, b, precision=lax.Precision.HIGHEST, preferred_element_type=F32)


def lanes_of(rows):
    return lax.broadcasted_iota(jnp.int32, (rows, LANES), 1)


def rows_of(rows):
    return lax.broadcasted_iota(jnp.int32, (rows, LANES), 0)


def roll(v, shift):
    return pltpu.roll(v, shift % LANES, 1)


def weighted(rows, load):
    sums = [None] * EXT
    for i in range(SIDE):
        block = load(i)
        for g in range(EXT):
            if W[g, i] != 0.0:
                term = float(W[g, i]) * block
                sums[g] = term if sums[g] is None else sums[g] + term
    return sums


def mix(weights, blocks):
    total = None
    for w, block in zip(weights, blocks):
        if w != 0.0:
            term = float(w) * block
            total = term if total is None else total + term
    return total


def ends_kernel(f, table, pz, block, weights, sem):
    copies = [pltpu.make_async_copy(f, block, sem.at[0]), pltpu.make_async_copy(table, weights, sem.at[1])]
    for copy in copies:
        copy.start()
    for copy in copies:
        copy.wait()
    out = dot(block[...], weights[...])
    group = lanes_of(SIDE) // EXT
    for half in range(2):
        packed = jnp.zeros((SIDE, LANES), F32)
        for j in range(GROUP):
            first = (half * GROUP + j) * SIDE
            packed = jnp.where(group == j, out[first : first + SIDE], packed)
        pz[pl.ds(half * SIDE, SIDE), :] = packed


def faces_kernel(f, fx, fy):
    for c in range(SIDE // 8):
        for g, block in enumerate(weighted(8, lambda x: f[pl.ds(x * SIDE + 8 * c, 8), :])):
            fx[pl.ds(g * SIDE + 8 * c, 8), :] = block
    for c in range(SIDE // 8):
        for g, block in enumerate(weighted(8, lambda y: f[pl.ds(8 * c * SIDE + y, 8, stride=SIDE), :])):
            fy[pl.ds(g * SIDE + 8 * c, 8), :] = block


def depth_kernel(pz, before, after, fx, tables, ez, up, down):
    near = lanes_of(2 * SIDE) % EXT < NEAR
    own = pz[...]
    sides = jnp.concatenate([jnp.where(near, before[...], own), jnp.where(near, own, after[...])], axis=1)
    fxe = dot(jnp.concatenate([sides[:SIDE], sides[SIDE:]], axis=1), tables[ENDS, :])
    ez[...] = dot(sides, tables[SOLVE, :])
    for g in range(NEAR):
        up[pl.ds(g * SIDE, SIDE), :] = fx[pl.ds(g * SIDE, SIDE), :]
        down[pl.ds(g * SIDE, SIDE), :] = fx[pl.ds((NEAR + g) * SIDE, SIDE), :]
    up[pl.ds(NEAR * SIDE, SIDE), :] = fxe
    down[pl.ds(NEAR * SIDE, SIDE), :] = fxe


def width_kernel(up, down, before, after, fy, ez, wy, tables, xe, xee, yup, ydown):
    for c in range(SIDE // 8):
        rows = [pl.ds(g * SIDE + 8 * c, 8) for g in range(NEAR)]
        own_last = [up[r, :] for r in rows]
        own_first = [down[r, :] for r in rows]
        seam_before = [before[r, :] for r in rows] + own_first
        seam_after = own_last + [after[r, :] for r in rows]
        for level in range(NEAR):
            xe[pl.ds(level * SIDE + 8 * c, 8), :] = mix(LAST[level], seam_before)
            xe[pl.ds((NEAR + level) * SIDE + 8 * c, 8), :] = mix(FIRST[level], seam_after)
    near = lanes_of(SIDE) // EXT < NEAR
    rows = pl.ds(NEAR * SIDE, SIDE)
    own = up[rows, :]
    sides = [jnp.where(near, before[rows, :], own), jnp.where(near, own, after[rows, :])]
    corner = dot(jnp.concatenate(sides, axis=1), tables[CORNER, :])
    xee[...] = corner
    sums = weighted(EXT, lambda y: xe[pl.ds(y, EXT, stride=SIDE), :])
    for g in range(EXT):
        target = yup if g < NEAR else ydown
        base = (g % NEAR) * PITCH
        target[pl.ds(base, SIDE), :] = fy[pl.ds(g * SIDE, SIDE), :]
        target[pl.ds(base + SIDE, EXT), :] = sums[g]
    for i, block in enumerate((ez[pl.ds(0, SIDE), :], ez[pl.ds(SIDE, SIDE), :], corner)):
        part = dot(wy[...], block)
        yup[pl.ds(NEAR * PITCH + i * EXT, EXT), :] = part
        ydown[pl.ds(NEAR * PITCH + i * EXT, EXT), :] = part


def lift_chunk(ref, at, level, masked):
    step = 1 << level
    pairs = SIDE // (2 * step)
    masked = masked and level > 0
    behind = ref[at(SIDE + level), :]
    even = ref[at(0), :]
    for k in range(pairs):
        odd = ref[at(step * (2 * k + 1)), :]
        ahead = ref[at(step * (2 * k + 2)), :] if k < pairs - 1 else ref[at(SIDE + NEAR + level), :]
        detail = odd - 0.5 * (even + ahead)
        smooth = even + 0.25 * (behind + detail)
        if masked:
            live = (lanes_of(odd.shape[0]) & (step - 1)) == 0
            detail, smooth = jnp.where(live, detail, odd), jnp.where(live, smooth, even)
        ref[at(step * (2 * k + 1)), :] = detail
        ref[at(2 * step * k), :] = smooth
        behind, even = detail, ahead


def chunks(level):
    step = 1 << level
    count = SIDE // step
    own = [(8 * step * c, min(8, count), step) for c in range(max(1, count // 8))]
    return own + ([(SIDE, EXT, 1)] if level < NEAR else [])


def lift_lanes(level, rows, v, qa, qb, keep=None):
    step = 1 << level
    lane = [lanes_of(count) for _, count in rows]
    last = [x == LANES - step for x in lane]
    cells = [v[at, :] for at, _ in rows]
    odd = [roll(c, -step) for c in cells]
    ahead = [roll(jnp.where(l, qb[at, :], o), -step) for (at, _), l, o in zip(rows, last, odd)]
    mid = [o - 0.5 * (c + a) for o, c, a in zip(odd, cells, ahead)]
    odd = [roll(m, step) for m in mid]
    behind = [roll(jnp.where(l, qa[at, :], o), step) for (at, _), l, o in zip(rows, last, odd)]
    for i, (at, _) in enumerate(rows):
        place = lane[i] & (2 * step - 1)
        smooth = cells[i] + 0.25 * (mid[i] + behind[i])
        lifted = jnp.where(place == 0, smooth, jnp.where(place == step, odd[i], cells[i]))
        mask = keep(i) if keep else None
        v[at, :] = lifted if mask is None else jnp.where(mask, cells[i], lifted)


def lane_rows(level, pieces):
    step = 1 << level
    planes = list(range(0, SIDE, step)) + [SIDE + g for g in range(EXT) if g % NEAR > level]
    return [
        (pl.ds(x * PITCH + first, count, stride=stride), count)
        for x in planes
        for first, count, stride in pieces
    ]


def lift_width(ref, level, masked, pieces):
    for first, count, stride in pieces:
        lift_chunk(ref, lambda i: pl.ds(i * PITCH + first, count, stride=stride), level, masked)


def prepare_kernel(f, ez, xe, xee, spread, v, qa, qb):
    for x in range(SIDE):
        v[pl.ds(x * PITCH, SIDE), :] = f[pl.ds(x * SIDE, SIDE), :]
    for g in range(EXT):
        v[pl.ds((SIDE + g) * PITCH, SIDE), :] = xe[pl.ds(g * SIDE, SIDE), :]
    block = jnp.concatenate([ez[...], xee[...]], axis=0)
    spread_lanes(qa, qb, 0, SIDE, block, spread)
    for ref in (v, qa, qb):
        lift_width(ref, 0, False, chunks(0)[:-1])
        for first, count, stride in chunks(0):

            def at(i):
                return pl.ds(first * PITCH + i, count, stride=stride * PITCH)

            even, behind = ref[at(0), :], None
            for k in range(SIDE // 2 - 1):
                ahead = ref[at(2 * k + 2), :]
                detail = ref[at(2 * k + 1), :] - 0.5 * (even + ahead)
                ref[at(2 * k + 1), :] = detail
                if k > 0:
                    ref[at(2 * k), :] = even + 0.25 * (behind + detail)
                even, behind = ahead, detail
    row8 = rows_of(8)
    waits = [row8 <= 1, None, None, row8 >= 5]
    lift_lanes(0, lane_rows(0, chunks(0)[:-1]), v, qa, qb, lambda i: waits[i % 4])


def spread_lanes(qa, qb, first, rows, block, spread):
    both = dot(block, spread[...])
    for x in range(PITCH):
        group, j = x // GROUP, x % GROUP
        for ref, part in ((qa, both[:, :LANES]), (qb, both[:, LANES:])):
            cells = part[group * rows : (group + 1) * rows]
            ref[pl.ds(x * PITCH + first, rows), :] = roll(cells, -EXT * (j + 1))


def stretch(v):
    lane = lanes_of(v.shape[0])
    for k in (2, 1, 0):
        spots = [16 * c - 15 * (c % (1 << k)) for c in range(8) if c >> k & 1]
        v = jnp.where(functools.reduce(jnp.logical_or, [lane == p for p in spots]), roll(v, 15 << k), v)
    return v


def close_height(ref):
    for first, count, stride in chunks(0):

        def at(i):
            return pl.ds(first * PITCH + i, count, stride=stride * PITCH)

        last, end = ref[at(SIDE - 2), :], ref[at(SIDE - 1), :]
        end = end - 0.5 * (last + ref[at(SIDE + NEAR), :])
        ref[at(SIDE - 1), :] = end
        ref[at(SIDE - 2), :] = last + 0.25 * (ref[at(SIDE - 3), :] + end)
        ref[at(0), :] = ref[at(0), :] + 0.25 * (ref[at(SIDE), :] + ref[at(1), :])


def levels_kernel(
    yup, ydown, before, after, th, spread, v_in, qa_in, qb_in, coef, send, v, qa, qb
):
    del v_in, qa_in, qb_in
    for c in range(PITCH // 8):
        rows = [pl.ds(g * PITCH + 8 * c, 8) for g in range(NEAR)]
        seam_before = [before[r, :] for r in rows] + [ydown[r, :] for r in rows]
        seam_after = [yup[r, :] for r in rows] + [after[r, :] for r in rows]
        for level in range(NEAR):
            v[pl.ds(8 * c * PITCH + SIDE + level, 8, stride=PITCH), :] = mix(LAST[level], seam_before)
            v[pl.ds(8 * c * PITCH + SIDE + NEAR + level, 8, stride=PITCH), :] = mix(FIRST[level], seam_after)
    row8 = rows_of(EXT)
    extras = []
    for i in range(3):
        first = NEAR * PITCH + i * EXT
        own = [yup[pl.ds(first + j, 1), :] for j in range(EXT)]
        seam_before = [before[pl.ds(first + j, 1), :] for j in range(NEAR)] + own[NEAR:]
        seam_after = own[:NEAR] + [after[pl.ds(first + NEAR + j, 1), :] for j in range(NEAR)]
        extra = jnp.zeros((EXT, LANES), F32)
        for level in range(NEAR):
            extra = jnp.where(row8 == level, mix(LAST[level], seam_before), extra)
            extra = jnp.where(row8 == NEAR + level, mix(FIRST[level], seam_after), extra)
        extras.append(extra)
    block = jnp.concatenate(extras, axis=0)
    spread_lanes(qa, qb, SIDE, EXT, block, spread)

    for level in range(NEAR):
        pieces = chunks(level)
        for ref in (v, qa, qb):
            lift_width(ref, level, ref is v, pieces[-1:] if level == 0 else pieces)
            if level == 0:
                close_height(ref)
                continue
            for first, count, stride in pieces:
                lift_chunk(
                    ref,
                    lambda i: pl.ds(first * PITCH + i, count, stride=stride * PITCH),
                    level,
                    ref is v,
                )
        if level == 0:
            rows = lane_rows(0, pieces[-1:])
            for y in (0, 1, SIDE - 3, SIDE - 2, SIDE - 1):
                rows += [(pl.ds(8 * c * PITCH + y, 8, stride=PITCH), 8) for c in range(PITCH // 8)]
        else:
            rows = lane_rows(level, pieces[: len(pieces) - (level == NEAR - 1)])
        lift_lanes(level, rows, v, qa, qb)

    energy = [jnp.zeros((8, LANES), F32)] * NEAR
    kept = [jnp.zeros((8, LANES), F32)] * NEAR
    for c in range(SIDE // 8):
        bits = (rows_of(8) + 8 * c) | lanes_of(8)
        own = [(bits & ((2 << level) - 1)) == (1 << level) for level in range(NEAR)]
        rest = [(bits & ((1 << level) - 1)) == 0 for level in range(NEAR)]
        bounds = []
        for depth in range(NEAR + 1):
            bound = jnp.broadcast_to(th[pl.ds(min(depth, NEAR - 1), 1), :], (8, LANES))
            for level in range(min(depth, NEAR - 1) - 1, -1, -1):
                bound = jnp.where(own[level], th[pl.ds(level, 1), :], bound)
            bounds.append(bound)
        squares = [None] * (NEAR + 1)
        sizes = [None] * (NEAR + 1)
        for x in range(SIDE):
            depth = NEAR if x == 0 else min(NEAR, (x & -x).bit_length() - 1)
            cells = v[pl.ds(x * PITCH + 8 * c, 8), :]
            shrunk = cells - jnp.minimum(jnp.maximum(cells, -bounds[depth]), bounds[depth])
            coef[pl.ds(x * SIDE + 8 * c, 8), :] = shrunk
            square, size = cells * cells, jnp.abs(shrunk)
            squares[depth] = square if squares[depth] is None else squares[depth] + square
            sizes[depth] = size if sizes[depth] is None else sizes[depth] + size
        for sums, target in ((squares, energy), (sizes, kept)):
            for level in range(NEAR):
                deeper = functools.reduce(lambda a, b: a + b, sums[level + 1 :])
                part = jnp.where(rest[level], sums[level], 0.0) + jnp.where(own[level], deeper, 0.0)
                target[level] = target[level] + part

    lane8 = lanes_of(8)
    block = jnp.zeros((8, LANES), F32)
    for i in range(4):
        block = jnp.where(row8 == i, v[pl.ds((i // 2 * PITCH + i % 2) * 16, 1), :], block)
    source, target = rows_of(LANES), lanes_of(LANES)
    pick = jnp.where((source == 16 * (target % 8)) & (target < 32), 1.0, 0.0).astype(F32)
    block = jnp.where(lane8 // 8 == row8, dot(block, pick), 0.0)
    for i, part in enumerate(energy + kept):
        block = jnp.where((lane8 == 32 + i) & (row8 == 0), jnp.sum(part), block)
    send[...] = jnp.broadcast_to(jnp.sum(block, axis=0, keepdims=True), send.shape)


def last_kernel(spot, got, coef, th, out, stats, grid, planes, sums_out, sem, *, sizes, counts):
    half = SIDE // 2
    copies = []
    for a in range(2):
        at = pl.ds((a * half + 1) * SIDE, (half - 1) * SIDE)
        copies.append(pltpu.make_async_copy(coef.at[at], out.at[at], sem.at[a]))
        copies[a].start()
        planes[pl.ds(a * SIDE, SIDE), :] = coef[pl.ds(a * half * SIDE, SIDE), :]
    nx, ny, nz = sizes
    plane = ny * nz
    lane, row = lanes_of(plane), rows_of(plane)
    v = [got[pl.ds(i * plane, plane), :] for i in range(nx)]
    sums = functools.reduce(lambda a, b: a + b, v)
    sums = jnp.sum(sums, axis=0, keepdims=True)

    def down(a, shift):
        return pltpu.roll(a, shift % plane, 0)

    odd = (lane & 16) != 0
    d = [v[i] - 0.5 * roll(v[i] + v[(i + 1) % nx], 16) for i in range(nx)]
    v = [jnp.where(odd, d[i], v[i] + 0.25 * roll(d[i] + d[i - 1], -16)) for i in range(nx)]
    odd = (lane & 8) != 0
    d = [a - 0.5 * roll(a + down(a, -nz), 8) for a in v]
    v = [jnp.where(odd, b, a + 0.25 * roll(b + down(b, nz), -8)) for a, b in zip(v, d)]
    odd = (lane & 1) != 0
    top, low = (lane & 7) == 7, (lane & 7) == 0
    far = row % nz == nz - 1
    near = row % nz == 0
    result = []
    for a in v:
        following = jnp.where(far, down(a, nz - 1), down(a, -1))
        d = a - 0.5 * (roll(a, 1) + jnp.where(top, roll(following, 7), roll(a, -1)))
        previous = jnp.where(near, down(d, 1 - nz), down(d, 1))
        s = a + 0.25 * (jnp.where(low, roll(previous, -7), roll(d, 1)) + roll(d, -1))
        result.append(jnp.where(odd, d, s))
    bound = th[pl.ds(LEVELS - 1, 1), :]
    detail = (lane < 32) & ((lane & 25) != 0)
    energy = kept = None
    for i, a in enumerate(result):
        shrunk = a - jnp.minimum(jnp.maximum(a, -bound), bound)
        grid[pl.ds(i * plane, plane), :] = jnp.where(detail, shrunk, a)
        square, size = jnp.where(detail, a * a, 0.0), jnp.where(detail, jnp.abs(shrunk), 0.0)
        energy = square if energy is None else energy + square
        kept = size if kept is None else kept + size
    lane1 = lanes_of(1)
    for i, (part, base) in enumerate(((energy, 32), (kept, 36))):
        totals = jnp.where(lane1 == NEAR, jnp.sum(part), roll(sums, -base))
        scale = jnp.zeros((1, LANES), F32)
        for level in range(LEVELS):
            scale = jnp.where(lane1 == level, 1.0 / counts[level], scale)
        sums_out[i] = (totals * scale)[:, :LEVELS]

    own = grid[pl.ds(spot[0], 1), :]
    start = lanes_of(1) % 16 == 0
    for i in range(4):
        at = pl.ds(i * half, 1)
        planes[at, :] = jnp.where(start, stretch(roll(own, -8 * i)), planes[at, :])
    for a in range(2):
        target = out.at[pl.ds(a * half * SIDE, SIDE)]
        copies.append(pltpu.make_async_copy(planes.at[pl.ds(a * SIDE, SIDE)], target, sem.at[2 + a]))
    copies.append(pltpu.make_async_copy(sums_out, stats, sem.at[4]))
    for copy in copies[2:]:
        copy.start()
    for copy in copies:
        copy.wait()


def shape(*dims):
    return jax.ShapeDtypeStruct(dims, F32)


def shards(fields, exponents):
    sizes = tuple(lax.axis_size(a) for a in ("gx", "gy", "gz"))
    devices = sizes[0] * sizes[1] * sizes[2]
    cells = fields.size * devices
    counts = [7.0 * cells / 8 ** (level + 1) for level in range(LEVELS)]
    f = fields.reshape(SIDE * SIDE, LANES)
    th = jnp.broadcast_to(jnp.pad(jnp.exp2(exponents.astype(F32)), (0, 3))[:, None], (8, LANES))
    table, tables, spread = (jnp.asarray(t) for t in constant_tables())
    wy = jnp.asarray(W.astype(np.float32))

    def swap(up, down, axis):
        n = lax.axis_size(axis)
        before = lax.ppermute(up, axis, [(i, (i + 1) % n) for i in range(n)])
        after = lax.ppermute(down, axis, [((i + 1) % n, i) for i in range(n)])
        return before, after

    here = pl.BlockSpec(memory_space=pltpu.VMEM)
    there = pl.BlockSpec(memory_space=pltpu.HBM)

    def pinned(a):
        return pltpu.with_memory_space_constraint(a, pltpu.VMEM)

    def local(kernel, name, outs, *args, aliases={}):
        args = [pinned(a) for a in args]
        return pl.pallas_call(
            kernel,
            in_specs=[here] * len(args),
            out_specs=[here] * len(outs),
            out_shape=[pltpu.VMEM((rows, LANES), F32) for rows in outs],
            input_output_aliases=aliases,
            compiler_params=pltpu.CompilerParams(vmem_limit_bytes=8 << 20),
            name=name,
        )(*args)

    spot = lax.axis_index(("gx", "gy", "gz")).astype(jnp.int32).reshape(1)
    pz, f = pl.pallas_call(
        ends_kernel,
        in_specs=[there] * 2,
        out_specs=[here] * 2,
        out_shape=[pltpu.VMEM((2 * SIDE, LANES), F32), pltpu.VMEM((SIDE * SIDE, LANES), F32)],
        scratch_shapes=[pltpu.VMEM((LANES, LANES), F32), pltpu.SemaphoreType.DMA((2,))],
        compiler_params=pltpu.CompilerParams(vmem_limit_bytes=8 << 20),
        name="ends",
    )(*(pltpu.with_memory_space_constraint(a, pltpu.HBM) for a in (f, table)))
    before, after = swap(pz, pz, "gz")
    fx, fy = local(faces_kernel, "faces", (EXT * SIDE, EXT * SIDE), f)
    message = (NEAR + 1) * SIDE
    ez, up, down = local(
        depth_kernel, "depth", (2 * SIDE, message, message), pz, before, after, fx, tables
    )
    before, after = swap(up, down, "gx")
    message = NEAR * PITCH + 3 * EXT
    xe, xee, yup, ydown = local(
        width_kernel, "width", (EXT * SIDE, SIDE, message, message), up, down, before, after, fy, ez, wy, tables
    )
    before, after = swap(yup, ydown, "gy")
    block = PITCH * PITCH
    v, qa, qb = local(
        prepare_kernel,
        "prepare",
        (block,) * 3,
        *(f, ez, xe, xee, spread),
    )
    coef, send, *_ = local(
        levels_kernel,
        "levels",
        (SIDE * SIDE, devices, block, block, block),
        *(yup, ydown, before, after, th, spread, v, qa, qb),
        aliases={6: 2, 7: 3, 8: 4},
    )
    send, spot, th = lax.optimization_barrier((send, spot, th))
    got = lax.all_to_all(send.reshape(devices, 1, LANES), ("gx", "gy", "gz"), 0, 0).reshape(devices, LANES)
    out, stats = pl.pallas_call(
        functools.partial(last_kernel, sizes=sizes, counts=counts),
        in_specs=[pl.BlockSpec(memory_space=pltpu.SMEM), here, here, here],
        out_specs=[there, there],
        out_shape=(shape(SIDE * SIDE, LANES), shape(2, 1, LEVELS)),
        scratch_shapes=[
            pltpu.VMEM((devices, LANES), F32),
            pltpu.VMEM((2 * SIDE, LANES), F32),
            pltpu.VMEM((2, 1, LEVELS), F32),
            pltpu.SemaphoreType.DMA((5,)),
        ],
        compiler_params=pltpu.CompilerParams(vmem_limit_bytes=8 << 20),
        name="last",
    )(spot, pinned(got), pinned(coef), pinned(th))
    return out.reshape(fields.shape), stats


def solution(mesh):
    placed = (P(None, "gx", "gy", "gz"), P())
    return jax.shard_map(shards, mesh=mesh, in_specs=placed, out_specs=placed, check_vma=False)
```
